32 devices in a mesh: blk: 32 (over z, y, x, core).
Axes of the slice: x: 2, y: 2, z: 4, core: 2. Of those that a mesh axis runs over, the one named last changes fastest.
Arguments:
- fields: float32 [256, 4, 16, 256], P('blk'), may hold values from -1 to 2, as said below
- guidance: float32 [256, 4, 16, 256], P('blk'), may hold values from -6 to 6
- levels: int32 [256], P('blk'), may hold values from -1 to 2, as said below
- send_faces: int32 [32, 32, 6], P('blk'), may hold values from -1 to 7, as said below
- ghost_peer: int32 [256, 6, 4], P('blk'), may hold values from -1 to 31, as said below
- ghost_code: int32 [256, 6, 4], P('blk'), may hold values from 0 to 24, as said below
- child_send: int32 [32, 32], P('blk'), may hold values from -1 to 7, as said below
- parent_peer: int32 [256, 8], P('blk'), may hold values from -1 to 31, as said below
Outputs:
- final_fields: float32 [256, 4, 16, 256], P('blk')
- gradient: float32 [256, 4, 16, 256], P('blk')
The draws below stay inside these ranges and needn't reach their ends.
Inputs may be any that keep to these rules, and one draw needn't show every extreme that they name: `fields`: channel 0 is a density between 0.5 and 2; channels 1 to 3 are that density times velocities of magnitude at most 0.5. `levels`: on each device the occupied slots come first and the rest are -1; a device has 8, 4, 2 or 1 occupied slots, device 0 all of them and device 1 an eighth. `send_faces`: entry [p, d, j] is an occupied local slot of device p, or -1 where p sends no face of type j to d; device (d + 1) mod 32 sends every face type to device d. `ghost_peer`: rows of empty slots are -1. For each occupied slot and face the entries in use come first: one, or four for a face next to finer blocks; each names a device p with send_faces[p, d, f xor 1] >= 0 for the slot's device d and face f; unused entries are -1. `ghost_code`: 0 for a single same-level entry and for unused entries; a and b in 1, 2 for a single entry from a coarser block; the four pairs of 3, 4 over the four entries of a face next to finer blocks. `child_send`: entry [c, d] is an occupied slot of device c that is not a covered parent, exactly where device d names c in parent_peer, else -1. `parent_peer`: A covered parent's row holds eight devices, and all devices named on one device are distinct; other rows are -1. Covered parents are the last occupied slots of a device, at most 4 of them and at most half of its occupied slots.
All inputs are finite; a program needn't handle non-finite values.
Results may differ from the reference program's by a relative error of at most 0.0003.
Values sent between devices are 32-bit elements; how exact they have to be, the bound alone decides.
No kernel may reach another device: no remote copies, remote signals or barrier semaphores. Data moves between devices by JAX's collectives and lax.ppermute only.
A program may use at most 128 MiB of HBM per device.

```python
import jax
import jax.numpy as jnp
from jax import lax

BLOCK_EDGE_CELLS = 16
SLOTS = 8
BLOCK_SLOT_TOTAL = 256
N_BLK = 32


def layout(key):
    devices = N_BLK
    slot_total = SLOTS
    subkeys = jax.random.split(jax.random.fold_in(key, 7301), 10)
    shrink_draw = jax.random.randint(subkeys[0], (devices,), 0, 8)
    shrink = jnp.maximum(shrink_draw - 4, 0)
    live_total = jnp.right_shift(jnp.full((devices,), slot_total, jnp.int32), shrink)
    live_total = live_total.at[0].set(slot_total).at[1].set(slot_total // 8)
    slot_ids = jnp.arange(slot_total, dtype=jnp.int32)
    occupied = slot_ids[None, :] < live_total[:, None]
    levels = jnp.where(occupied, jax.random.randint(subkeys[1], (devices, slot_total), 0, 3), -1).astype(jnp.int32)
    wanted = jax.random.randint(subkeys[2], (devices,), 1, devices // 8 + 1)
    parent_total = jnp.minimum(wanted, live_total // 2)
    orders = jax.vmap(lambda subkey: jax.random.permutation(subkey, devices))(jax.random.split(subkeys[3], devices)).astype(jnp.int32)
    parent_index = slot_ids[None, :] - (live_total - parent_total)[:, None]
    is_parent = (parent_index >= 0) & occupied
    positions = jnp.minimum(jnp.maximum(parent_index, 0)[:, :, None] * 8 + jnp.arange(8, dtype=jnp.int32), devices - 1)
    named = jax.vmap(lambda ordering, spots: ordering[spots])(orders, positions)
    parent_peer = jnp.where(is_parent[:, :, None], named, -1).astype(jnp.int32)
    inverse = jnp.argsort(orders, axis=1).astype(jnp.int32)
    wanted_child = inverse.T < (parent_total * 8)[None, :]
    child_pick = jax.random.randint(subkeys[4], (devices, devices), 0, (live_total - parent_total)[:, None])
    child_send = jnp.where(wanted_child, child_pick, -1).astype(jnp.int32)
    device_ids = jnp.arange(devices, dtype=jnp.int32)
    entry_ids = jnp.arange(4, dtype=jnp.int32)
    relation = jnp.minimum(jax.random.randint(subkeys[8], (devices, slot_total, 6), 0, 6), 3)
    entry_total = jnp.where(relation == 3, 4, 1)
    in_use = (entry_ids[None, None, None, :] < entry_total[:, :, :, None]) & occupied[:, :, None, None]
    use_flat = in_use.transpose(0, 2, 1, 3).reshape(devices, 6, slot_total * 4).astype(jnp.int32)
    rank = jnp.cumsum(use_flat, axis=2) - 1
    face_orders = jax.vmap(lambda subkey: jax.random.permutation(subkey, devices))(jax.random.split(subkeys[7], devices * 6)).astype(jnp.int32).reshape(devices, 6, devices)
    peer_flat = jnp.take_along_axis(face_orders, jnp.maximum(rank, 0) % devices, axis=2)
    device_index = jnp.broadcast_to(device_ids[:, None, None], peer_flat.shape)
    face_index = jnp.broadcast_to(jnp.arange(6, dtype=jnp.int32)[None, :, None], peer_flat.shape)
    named_faces = jnp.zeros((devices, 6, devices), jnp.int32).at[device_index, face_index, peer_flat].max(use_flat)
    opposite = jnp.arange(6, dtype=jnp.int32) ^ 1
    present = (named_faces[:, opposite, :].transpose(2, 0, 1) > 0) | (device_ids[:, None, None] == (device_ids[None, :, None] + 1) % devices)
    send_pick = jax.random.randint(subkeys[6], (devices, devices, 6), 0, live_total[:, None, None])
    send_faces = jnp.where(present, send_pick, -1).astype(jnp.int32)
    chosen_peer = peer_flat.reshape(devices, 6, slot_total, 4).transpose(0, 2, 1, 3)
    ghost_peer = jnp.where(in_use, chosen_peer, -1).astype(jnp.int32).reshape(devices * slot_total, 6, 4)
    halves = jax.random.randint(subkeys[9], (devices, slot_total, 6, 2), 1, 3)
    coarse_code = halves[..., 0] * 5 + halves[..., 1]
    finer_level_code = (3 + entry_ids // 2) * 5 + 3 + entry_ids % 2
    op_code = jnp.where((relation == 2)[..., None], coarse_code[..., None], jnp.where((relation == 3)[..., None], finer_level_code, 0))
    ghost_code = jnp.where(in_use, op_code, 0).astype(jnp.int32).reshape(devices * slot_total, 6, 4)
    return (levels.reshape(-1), send_faces, ghost_peer, ghost_code, child_send, parent_peer.reshape(devices * slot_total, 8))


def draw_levels(key, part):
    return layout(key)[0]


def draw_send_faces(key, part):
    return layout(key)[1]


def draw_ghost_peer(key, part):
    return layout(key)[2]


def draw_ghost_code(key, part):
    return layout(key)[3]


def draw_child_send(key, part):
    return layout(key)[4]


def draw_parent_peer(key, part):
    return layout(key)[5]


def draw_fields(key, part):
    subkeys = jax.random.split(jax.random.fold_in(key, 9127), 2)
    dims = (N_BLK * SLOTS, BLOCK_EDGE_CELLS, BLOCK_EDGE_CELLS * BLOCK_EDGE_CELLS)
    density = 0.6 + jax.random.uniform(subkeys[0], dims, jnp.float32)
    velocity = jnp.clip(0.25 * jax.random.normal(subkeys[1], (3,) + dims, jnp.float32), -0.5, 0.5)
    return jnp.concatenate([density[None], density[None] * velocity], axis=0).transpose(1, 0, 2, 3)


def level_of(own_key, shape, cuts, smallest, high):
    def one(dim, shards_of):
        heights = jax.random.uniform(jax.random.fold_in(jax.random.fold_in(own_key, 6), dim), (shards_of,), jnp.float32, smallest / len(cuts), high / len(cuts))
        return jnp.repeat(jnp.exp(heights), shape[dim] // shards_of).reshape((-1,) + (1,) * (len(shape) - dim - 1))

    factor_of = one(*cuts[0])
    for cut in cuts[1:]:
        factor_of = factor_of * one(*cut)
    return factor_of


def centred(own_key, shape, width, bound, cuts=(), kind=jnp.bfloat16):
    values = width * jax.random.normal(own_key, shape, jnp.float32)
    if cuts:
        values = values * level_of(own_key, shape, cuts, -0.22, 0.18)
    return jnp.clip(values, -bound, bound).astype(kind)


def setup_inputs(seed: int = 0) -> dict:
    key_of = jax.random.split(jax.random.key(seed), 9)
    return {
        "fields": draw_fields(jax.random.fold_in(key_of[8], 71), 0),
        "guidance": centred(key_of[1], (BLOCK_SLOT_TOTAL, 4, BLOCK_EDGE_CELLS, BLOCK_EDGE_CELLS * BLOCK_EDGE_CELLS), 1.0, 6.0, ((0, 32),), jnp.float32),
        "levels": draw_levels(jax.random.fold_in(key_of[8], 71), 0),
        "send_faces": draw_send_faces(jax.random.fold_in(key_of[8], 71), 0),
        "ghost_peer": draw_ghost_peer(jax.random.fold_in(key_of[8], 71), 0),
        "ghost_code": draw_ghost_code(jax.random.fold_in(key_of[8], 71), 0),
        "child_send": draw_child_send(jax.random.fold_in(key_of[8], 71), 0),
        "parent_peer": draw_parent_peer(jax.random.fold_in(key_of[8], 71), 0),
    }


sound_speed = 1.0
base_ratio = 0.04
speed_floor = 0.01
highest = lax.Precision.HIGHEST

def axis_tables(extent):
    row_ids = jnp.arange(extent)[:, None]
    col_ids = jnp.arange(extent)[None, :]
    half_size = extent // 2
    tables = [(row_ids == col_ids).astype(jnp.float32)]
    for offset in range(2):
        tables.append((col_ids == offset * half_size + row_ids // 2).astype(jnp.float32))
    for offset in range(2):
        inside = (row_ids >= offset * half_size) & (row_ids < offset * half_size + half_size) & (col_ids // 2 == row_ids - offset * half_size)
        tables.append(0.5 * inside.astype(jnp.float32))
    return jnp.stack(tables)

def rusanov(behind, beyond, normal_direction):

    def physical(values):
        velocity = values[1 + normal_direction] / values[0]
        momentum_flux = values[1:] * velocity
        momentum_flux = momentum_flux.at[normal_direction].add(sound_speed * sound_speed * values[0])
        return (jnp.concatenate([values[1 + normal_direction][None], momentum_flux]), velocity)
    flux_behind, speed_behind = physical(behind)
    flux_beyond, speed_beyond = physical(beyond)
    wave_speed = sound_speed + jnp.sqrt(0.5 * (speed_behind * speed_behind + speed_beyond * speed_beyond) + speed_floor)
    return 0.5 * (flux_behind + flux_beyond) - 0.5 * wave_speed * (beyond - behind)

def face_layers(volume):
    return jnp.stack([volume[:, 0], volume[:, -1], volume[:, :, 0], volume[:, :, -1], volume[:, :, :, 0], volume[:, :, :, -1]])

def boundary_fluxes(layers, ghosts):
    stacked = []
    for surface in range(6):
        if surface % 2 == 0:
            stacked.append(rusanov(ghosts[surface], layers[surface], surface // 2))
        else:
            stacked.append(rusanov(layers[surface], ghosts[surface], surface // 2))
    return jnp.stack(stacked)

def interior_change(volume, step_ratio):
    extent = volume.shape[1]
    summed = jnp.zeros_like(volume)
    for normal_direction in range(3):
        direction = normal_direction + 1
        behind = lax.slice_in_dim(volume, 0, extent - 1, axis=direction)
        beyond = lax.slice_in_dim(volume, 1, extent, axis=direction)
        inner_flux = rusanov(behind, beyond, normal_direction)
        widths = [(0, 0)] * 4
        widths[direction] = (1, 1)
        padded = jnp.pad(inner_flux, widths)
        summed = summed + (lax.slice_in_dim(padded, 1, extent + 1, axis=direction) - lax.slice_in_dim(padded, 0, extent, axis=direction))
    return -step_ratio * summed

def boundary_change(corrected, step_ratio):
    extent = corrected.shape[-1]
    change = jnp.zeros((4, extent, extent, extent), corrected.dtype)
    change = change.at[:, 0].add(step_ratio * corrected[0])
    change = change.at[:, extent - 1].add(-step_ratio * corrected[1])
    change = change.at[:, :, 0].add(step_ratio * corrected[2])
    change = change.at[:, :, extent - 1].add(-step_ratio * corrected[3])
    change = change.at[:, :, :, 0].add(step_ratio * corrected[4])
    change = change.at[:, :, :, extent - 1].add(-step_ratio * corrected[5])
    return change

def update_volume(volume, corrected, step_ratio):
    return volume + interior_change(volume, step_ratio) + boundary_change(corrected, step_ratio)

def average_volume(volume):
    extent = volume.shape[1]
    half_size = extent // 2
    return volume.reshape(4, half_size, 2, half_size, 2, half_size, 2).mean(axis=(2, 4, 6))

def place_octants(pieces):
    half_size = pieces.shape[-1]
    extent = 2 * half_size
    return pieces.reshape(2, 2, 2, 4, half_size, half_size, half_size).transpose(3, 0, 4, 1, 5, 2, 6).reshape(4, extent, extent, extent)

def assemble(source, sources, op_codes, toward, tables):
    opposite = (jnp.arange(6, dtype=jnp.int32) ^ 1)[None, :, None]
    chosen = jnp.maximum(sources, 0)
    local_slot = jnp.maximum(toward[chosen, opposite], 0)
    row_ids = ((chosen * SLOTS + local_slot) * 6 + opposite).astype(jnp.int32)
    picked = source[row_ids]
    first_map = tables[op_codes // 5]
    second = tables[op_codes % 5]
    remapped_result = jnp.einsum('sfeij,sfecjl,sfeml->sfecim', first_map, picked, second, precision=highest)
    active = (sources >= 0).astype(remapped_result.dtype)[:, :, :, None, None, None]
    return lax.optimization_barrier(jnp.sum(remapped_result * active, axis=2))

def advance(volumes, levels, send_faces, ghost_peer, ghost_code, child_send, parent_peer):
    extent = volumes.shape[2]
    tables = axis_tables(extent).astype(volumes.dtype)
    devices = jnp.arange(N_BLK, dtype=jnp.int32)

    def device_slab(array, device):
        return lax.dynamic_slice_in_dim(array, device * SLOTS, SLOTS)

    def collect(source):

        def per_device(device):
            return assemble(source, device_slab(ghost_peer, device), device_slab(ghost_code, device), send_faces[:, device, :], tables)
        return lax.map(per_device, devices).reshape(volumes.shape[0], 6, 4, extent, extent)
    occupied = (levels >= 0)[:, None, None, None, None]
    layers = jax.vmap(face_layers)(volumes)
    ghosts = jnp.where(occupied, collect(layers.reshape(-1, 4, extent, extent)), layers)
    fluxes = jax.vmap(boundary_fluxes)(layers, ghosts)
    refined = (ghost_peer[:, :, 1] >= 0)[:, :, None, None, None]
    corrected = jnp.where(refined, collect(fluxes.reshape(-1, 4, extent, extent)), fluxes)
    degree = levels.astype(volumes.dtype)
    step_ratio = base_ratio * (1.0 + degree + 0.5 * degree * (degree - 1.0))
    update_all = jax.checkpoint(jax.vmap(update_volume))

    def per_slab(device):
        return update_all(device_slab(volumes, device), device_slab(corrected, device), device_slab(step_ratio, device))
    updated = lax.map(per_slab, devices).reshape(volumes.shape)
    updated = jnp.where(occupied, updated, volumes)
    coarse = jax.vmap(average_volume)(updated)
    owners = (jnp.arange(volumes.shape[0], dtype=jnp.int32) // SLOTS).astype(jnp.int32)
    chosen = jnp.maximum(parent_peer, 0)
    child_slot = (chosen * SLOTS + jnp.maximum(child_send[chosen, owners[:, None]], 0)).astype(jnp.int32)
    assembled = jax.vmap(place_octants)(coarse[child_slot])
    covered = (parent_peer[:, 0] >= 0)[:, None, None, None, None]
    return jnp.where(covered, assembled, updated)

def reference(fields, guidance, levels, send_faces, ghost_peer, ghost_code, child_send, parent_peer):
    extent = fields.shape[2]
    volumes = fields.reshape(fields.shape[0], 4, extent, extent, extent)

    def window(initial):
        middle = advance(initial, levels, send_faces, ghost_peer, ghost_code, child_send, parent_peer)
        return advance(middle, levels, send_faces, ghost_peer, ghost_code, child_send, parent_peer)
    final_state, adjoint_function = jax.vjp(window, volumes)
    gradient = adjoint_function(guidance.reshape(volumes.shape))[0]
    return (final_state.reshape(fields.shape), gradient.reshape(fields.shape))
```

```python
import jax
import jax.numpy as jnp
import numpy as np
from jax import lax
from jax.experimental import pallas as pl
from jax.experimental.pallas import tpu as pltpu
from jax.sharding import PartitionSpec as P

sound_speed = 1.0
base_ratio = 0.04
speed_floor = 0.01
f32 = jnp.float32
bf16 = jnp.bfloat16


def half_map(extent):
    half = extent // 2
    square = extent * extent
    table = np.zeros((2, extent, extent, half, 2, half), np.float32)
    for group in range(2):
        for i in range(extent):
            for j in range(extent):
                table[group, i, j, i // 2, group, j // 2] = 0.25
    return table.reshape(2 * square, square // 2)


def dot2(values, table):
    high = values.astype(bf16)
    low = (values - high.astype(f32)).astype(bf16)
    return jnp.dot(high, table, preferred_element_type=f32) + jnp.dot(
        low, table, preferred_element_type=f32
    )


def roll(values, shift):
    lanes = values.shape[1]
    shift = shift % lanes
    return values if shift == 0 else pltpu.roll(values, shift, 1)


def flux_of(behind, beyond, normal, inv_behind, inv_beyond):
    v = behind[1 + normal] * inv_behind
    w = beyond[1 + normal] * inv_beyond
    c = sound_speed + jnp.sqrt(0.5 * (v * v + w * w) + speed_floor)
    result = [0.5 * ((behind[1 + normal] + beyond[1 + normal]) - c * (beyond[0] - behind[0]))]
    for k in range(1, 4):
        total = behind[k] * v + beyond[k] * w
        if k == 1 + normal:
            total = total + (sound_speed * sound_speed) * (behind[0] + beyond[0])
        result.append(0.5 * (total - c * (beyond[k] - behind[k])))
    return result


def flux_pull(behind, beyond, normal, inv_behind, inv_beyond, cot):
    v = behind[1 + normal] * inv_behind
    w = beyond[1 + normal] * inv_beyond
    inside = 0.5 * (v * v + w * w) + speed_floor
    root = jnp.sqrt(inside)
    c = sound_speed + root
    half_cot = [0.5 * part for part in cot]
    jump = half_cot[0] * (beyond[0] - behind[0])
    v_cot = half_cot[1] * behind[1]
    w_cot = half_cot[1] * beyond[1]
    for k in range(1, 4):
        jump = jump + half_cot[k] * (beyond[k] - behind[k])
        if k > 1:
            v_cot = v_cot + half_cot[k] * behind[k]
            w_cot = w_cot + half_cot[k] * beyond[k]
    scale = jump * (-0.5) / root
    v_cot = (v_cot + scale * v) * inv_behind
    w_cot = (w_cot + scale * w) * inv_beyond
    plus = v + c
    minus = w - c
    behind_cot = []
    beyond_cot = []
    pressure = (sound_speed * sound_speed) * half_cot[1 + normal]
    for k in range(4):
        if k == 0:
            behind_cot.append(c * half_cot[0] + pressure - v_cot * v)
            beyond_cot.append(pressure - c * half_cot[0] - w_cot * w)
        else:
            left = half_cot[k] * plus
            right = half_cot[k] * minus
            if k == 1 + normal:
                left = left + half_cot[0] + v_cot
                right = right + half_cot[0] + w_cot
            behind_cot.append(left)
            beyond_cot.append(right)
    return behind_cot, beyond_cot


class Plan:
    def __init__(self, slots, extent, peers):
        self.S = slots
        self.E = extent
        self.P = peers
        self.H = extent // 2
        self.COL = extent * extent // 2
        self.slab = (2, extent * 4 * slots, self.COL)
        self.ff = (2, 6 * 4 * slots, self.COL)
        self.fb = (2, 3 * slots * 8, self.COL)
        self.native = (slots * 4 * extent, 2 * self.COL)
        self.coarse = (slots * 16, self.COL)

    def lane(self, rows):
        return lax.broadcasted_iota(jnp.int32, (rows, self.COL), 1)

    def low(self, rows):
        return (self.lane(rows) & (self.E - 1)) < self.H

    def per_slot(self, scalar_of):
        sub = lax.broadcasted_iota(jnp.int32, (self.S, self.COL), 0)
        value = jnp.zeros((self.S, self.COL), jnp.int32)
        for s in range(self.S):
            value = jnp.where(sub == s, scalar_of(s), value)
        return value

    def ratio(self, levels):
        level = self.per_slot(lambda s: levels[s])
        degree = level.astype(f32)
        ratio = base_ratio * (1.0 + degree + 0.5 * degree * (degree - 1.0))
        return jnp.where(level >= 0, ratio, 0.0)

    def slab_at(self, ref):
        return lambda q, x, c: ref[q, (x * 4 + c) * self.S : (x * 4 + c + 1) * self.S, :]

    def native_at(self, planes):
        step = 4 * self.E
        return lambda q, x, c: planes[q][pl.ds(c * self.E + x, self.S, stride=step), :]

    def ff_at(self, ref):
        return lambda q, f, c: ref[q, (f * 4 + c) * self.S : (f * 4 + c + 1) * self.S, :]

    def fb_rows(self, f, c, swapped=False):
        side = f % 2
        half = 1 - side if swapped else side
        return pl.ds((f // 2) * self.S * 8 + half * 4 + c, self.S, stride=8)

    def extract(self, get, c):
        E, H, COL = self.E, self.H, self.COL
        lane = self.lane(self.S)
        group = lax.shift_right_logical(lane, E.bit_length() - 1)
        within = lane & (E - 1)
        faces = [[get(q, 0, c) for q in range(2)], [get(q, E - 1, c) for q in range(2)]]
        low_y, high_y, low_z, high_z = [], [], [], []
        for q in range(2):
            first, last, near, far = None, None, None, None
            for k in range(H):
                a = roll(get(0, q * H + k, c), E * k)
                b = roll(get(1, q * H + k, c), E * k - (COL - E))
                first = a if first is None else jnp.where(group == k, a, first)
                last = b if last is None else jnp.where(group == k, b, last)
            for x in range(E):
                source = get(q, x, c)
                a = roll(source, x)
                b = roll(source, x - (E - 1))
                near = a if near is None else jnp.where(within == x, a, near)
                far = b if far is None else jnp.where(within == x, b, far)
            low_y.append(first)
            high_y.append(last)
            low_z.append(near)
            high_z.append(far)
        return faces + [low_y, high_y, low_z, high_z]

    def spread(self, face, q, x, c):
        E, H, COL = self.E, self.H, self.COL
        lane = self.lane(self.S)
        within = lane & (E - 1)
        k = x % H
        y_face = face(x // H, 2 + q, c)
        if q == 0:
            total = jnp.where(lane < E, roll(y_face, -E * k), 0.0)
        else:
            total = jnp.where(lane >= COL - E, roll(y_face, (COL - E) - E * k), 0.0)
        near = roll(face(q, 4, c), -x)
        far = roll(face(q, 5, c), E - 1 - x)
        total = total + jnp.where(within == 0, near, jnp.where(within == E - 1, far, 0.0))
        if x == 0:
            total = total + face(q, 0, c)
        if x == E - 1:
            total = total + face(q, 1, c)
        return total

    def pack_faces(self, fb, send, out):
        sub = lax.broadcasted_iota(jnp.int32, (8, self.COL), 0)

        def one(peer, carry):
            for axis in range(3):
                slots = [jnp.maximum(send[peer * 6 + axis * 2 + side], 0) for side in range(2)]
                for q in range(2):
                    lo, hi = [
                        fb[q, pl.ds(pl.multiple_of((axis * self.S + slot) * 8, 8), 8), :]
                        for slot in slots
                    ]
                    row = axis * 16 + q * 8
                    out[peer, row : row + 8, :] = jnp.where(sub < 4, lo, hi)
            return carry

        lax.fori_loop(0, self.P, one, 0)

    def take_faces(self, packets, send, sums):
        def one(peer, carry):
            for f in range(6):
                slot = jnp.maximum(send[peer * 6 + f], 0)
                rows = pl.ds(pl.multiple_of(slot * 8, 8), 8)
                for q in range(2):
                    at = (f // 2) * 16 + q * 8
                    sums[f][q, rows, :] += packets[peer, at : at + 8, :]
            return carry

        for f in range(6):
            sums[f][...] = jnp.zeros(sums[f].shape, f32)
        lax.fori_loop(0, self.P, one, 0)

    def pack_averages(self, face, rb, send, out, row0, half):
        S, COL = self.S, self.COL
        rows = []
        for axis in range(3):
            for c in range(4):
                rows.append(
                    jnp.concatenate(
                        [face(q, 2 * axis + side, c) for side in range(2) for q in range(2)], axis=1
                    )
                )
        small = dot2(jnp.concatenate(rows, axis=0), half[...])
        for k in range(12):
            rb[pl.ds(k, S, stride=16), :] = small[k * S : (k + 1) * S]
        zero = jnp.zeros((S, COL), f32)
        for k in range(12, 16):
            rb[pl.ds(k, S, stride=16), :] = zero
        sub = lax.broadcasted_iota(jnp.int32, (8, COL), 0)
        low = self.low(8)

        def one(peer, carry):
            def part(f, at):
                slot = jnp.maximum(send[peer * 6 + f], 0)
                return rb[pl.ds(pl.multiple_of(slot * 16 + at, 8), 8), :]

            first = jnp.where(low, part(0, 0), part(1, 0))
            second = jnp.where(low, part(2, 0), part(3, 0))
            out[peer, row0 : row0 + 8, :] = jnp.where(sub < 4, first, second)
            out[peer, row0 + 8 : row0 + 16, :] = jnp.where(low, part(4, 8), part(5, 8))
            return carry

        lax.fori_loop(0, self.P, one, 0)

    def pack_quarters(self, fb, table, out, row0):
        E, H = self.E, self.H
        low = self.low(4)

        def clear(peer, carry):
            out[peer, row0 : row0 + 16, :] = jnp.zeros((16, self.COL), f32)
            return carry

        lax.fori_loop(0, self.P, clear, 0)
        for s in range(self.S):
            for f in range(6):
                base = (s * 6 + f) * 8

                def send_quarters(s=s, f=f, base=base):
                    axis, side = f // 2, f % 2
                    keep = low if side == 1 else jnp.logical_not(low)
                    row = (axis * self.S + s) * 8 + side * 4
                    at = row0 + axis * 4
                    for h in range(2):
                        values = fb[h, row : row + 4, :]
                        for g in range(2):
                            moved = roll(values, H * ((1 - side) - g))
                            peer = table[base + h * 2 + g]
                            out[peer, at : at + 4, :] += jnp.where(keep, moved, 0.0)

                pl.when(table[base + 4] == 2)(send_quarters)

    def take_quarters(self, packets, row0, send, sums, face_out, half_back):
        S, COL = self.S, self.COL

        def one(peer, carry):
            block = packets[peer, row0 : row0 + 16, :]
            for f in range(6):
                slot = jnp.maximum(send[peer * 6 + f], 0)
                rows = pl.ds(pl.multiple_of(slot * 16, 8), 16)
                sums[f][rows, :] += block
            return carry

        for f in range(6):
            sums[f][...] = jnp.zeros(sums[f].shape, f32)
        lax.fori_loop(0, self.P, one, 0)
        for f in range(6):
            axis, side = f // 2, f % 2
            rows = jnp.concatenate(
                [sums[f][pl.ds(axis * 4 + c, S, stride=16), :] for c in range(4)], axis=0
            )
            wide = dot2(rows, half_back[:, side * 2 * COL : (side + 1) * 2 * COL])
            for c in range(4):
                face_out(f, c, [wide[c * S : (c + 1) * S, q * COL : (q + 1) * COL] for q in range(2)])

    def ghosts(self, packets, table, planes, near, kinds, gb, half, half_back):
        S, COL, H = self.S, self.COL, self.H
        for s in range(S):
            for f in range(6):
                base = (s * 6 + f) * 8
                axis, half_row = f // 2, (1 - f % 2) * 4
                row = (axis * S + s) * 8 + half_row
                first = None
                for k in range(4):
                    peer = table[base + k]
                    got = []
                    for q in range(2):
                        at = axis * 16 + q * 8 + half_row
                        values = packets[peer, at : at + 4, :]
                        planes[k * 2 + q, row : row + 4, :] = values
                        got.append(values)
                    if k == 0:
                        first = got
                source = jnp.where(table[base + 5] == 1, first[1], first[0])
                source = jnp.where(table[base + 6] == 1, roll(source, -H), source)
                near[row : row + 4, :] = source
                kinds[row : row + 4, :] = jnp.full((4, COL), table[base + 4], jnp.int32)
        for axis in range(3):
            rows = slice(axis * S * 8, (axis + 1) * S * 8)
            kind = kinds[rows, :]
            coarse = 4.0 * dot2(near[rows, :], half_back[:, : 2 * COL])
            for h in range(2):
                parts = [planes[(h * 2 + g) * 2 + q, rows, :] for g in range(2) for q in range(2)]
                fine = dot2(jnp.concatenate(parts, axis=1), half[...])
                value = jnp.where(kind == 1, coarse[:, h * COL : (h + 1) * COL], planes[h, rows, :])
                gb[h, rows, :] = jnp.where(kind == 2, fine, value)

    def pack_ghost_cot(self, gb, table, wide, near, out, half, half_back):
        S, COL, H = self.S, self.COL, self.H
        low = self.low(4)

        def clear(peer, carry):
            out[peer, 0:48, :] = jnp.zeros((48, COL), f32)
            return carry

        lax.fori_loop(0, self.P, clear, 0)
        rows_all = 3 * S * 8
        for h in range(2):
            for g in range(2):
                spread = dot2(gb[h, :, :], half_back[:, g * 2 * COL : (g + 1) * 2 * COL])
                for q in range(2):
                    wide[(h * 2 + g) * 2 + q, :, :] = spread[:, q * COL : (q + 1) * COL]
        both = jnp.concatenate([gb[0, :, :], gb[1, :, :]], axis=1)
        near[...] = 4.0 * dot2(both, half[0 : 2 * COL, :])
        del rows_all
        for s in range(S):
            for f in range(6):
                base = (s * 6 + f) * 8
                axis, half_row = f // 2, (1 - f % 2) * 4
                row = (axis * S + s) * 8 + half_row
                kind = table[base + 4]

                def same(base=base, axis=axis, half_row=half_row, row=row):
                    peer = table[base]
                    for q in range(2):
                        at = axis * 16 + q * 8 + half_row
                        out[peer, at : at + 4, :] += gb[q, row : row + 4, :]

                def coarse(base=base, axis=axis, half_row=half_row, row=row):
                    peer = table[base]
                    values = near[row : row + 4, :]
                    values = jnp.where(table[base + 6] == 1, roll(values, H), values)
                    for q in range(2):
                        at = axis * 16 + q * 8 + half_row
                        out[peer, at : at + 4, :] += jnp.where(table[base + 5] == q, values, 0.0)

                def fine(base=base, axis=axis, half_row=half_row, row=row):
                    for k in range(4):
                        peer = table[base + k]
                        for q in range(2):
                            at = axis * 16 + q * 8 + half_row
                            out[peer, at : at + 4, :] += wide[k * 2 + q, row : row + 4, :]

                pl.when(kind == 0)(same)
                pl.when(kind == 1)(coarse)
                pl.when(kind == 2)(fine)

    def corrected(self, b_fb, packets, row0, table, out):
        H = self.H
        low = self.low(4)
        out[...] = b_fb[...]
        for s in range(self.S):
            for f in range(6):
                base = (s * 6 + f) * 8

                def replace(s=s, f=f, base=base):
                    axis, side = f // 2, f % 2
                    row = (axis * self.S + s) * 8 + side * 4
                    at = row0 + axis * 4
                    for h in range(2):
                        got = []
                        for g in range(2):
                            values = packets[table[base + h * 2 + g], at : at + 4, :]
                            got.append(roll(values, H * (g - (1 - side))))
                        out[h, row : row + 4, :] = jnp.where(low, got[0], got[1])

                pl.when(table[base + 4] == 2)(replace)

    def pack_octants(self, load, parents, out, row0):
        H = self.H
        low = self.low(4)
        for s in range(self.S):

            def send(s=s):
                for ox in range(2):
                    for oy in range(2):
                        peers = [parents[s * 8 + ox * 4 + oy * 2 + oz] for oz in range(2)]
                        for pair in range(H // 2):
                            x = ox * H + pair * 2
                            first, second = load(s, x, oy), load(s, x + 1, oy)
                            at = row0 + pair * 4
                            out[peers[0], at : at + 4, :] = jnp.where(low, first, roll(second, H))
                            out[peers[1], at : at + 4, :] = jnp.where(low, roll(first, -H), second)

            pl.when(parents[s * 8] >= 0)(send)

    def place_octants(self, packets, row0, parents, store):
        H = self.H
        low = self.low(4)
        for s in range(self.S):

            def place(s=s):
                for ox in range(2):
                    for oy in range(2):
                        peers = [parents[s * 8 + ox * 4 + oy * 2 + oz] for oz in range(2)]
                        for pair in range(H // 2):
                            x = ox * H + pair * 2
                            at = row0 + pair * 4
                            first = packets[peers[0], at : at + 4, :]
                            second = packets[peers[1], at : at + 4, :]
                            store(s, x, oy, jnp.where(low, first, roll(second, H)))
                            store(s, x + 1, oy, jnp.where(low, roll(first, -H), second))

            pl.when(parents[s * 8] >= 0)(place)

    def slab_rows(self, s, x):
        return pl.ds(x * 4 * self.S + s, 4, stride=self.S)

    def native_rows(self, s, x):
        return pl.ds(s * 4 * self.E + x, 4, stride=self.E)

    def pack_children(self, get, cb, children, out, row0, half):
        S = self.S
        rows = []
        for pair in range(self.E // 4):
            for c in range(4):
                x = 4 * pair
                rows.append(
                    jnp.concatenate(
                        [get(q, x + 2 * a, c) + get(q, x + 2 * a + 1, c) for a in range(2) for q in range(2)],
                        axis=1,
                    )
                )
        small = 0.5 * dot2(jnp.concatenate(rows, axis=0), half[...])
        for k in range(16):
            cb[pl.ds(k, S, stride=16), :] = small[k * S : (k + 1) * S]

        def one(peer, carry):
            slot = jnp.maximum(children[peer], 0)
            out[peer, row0 : row0 + 16, :] = cb[pl.ds(pl.multiple_of(slot * 16, 8), 16), :]
            return carry

        lax.fori_loop(0, self.P, one, 0)

    def upward(self, packets, row0, cc, children, parents, get, put, half_back):
        S, COL = self.S, self.COL
        cc[...] = jnp.zeros(cc.shape, f32)

        def one(peer, carry):
            child = children[peer]
            slot = jnp.where(child < 0, S, child)
            rows = pl.ds(pl.multiple_of(slot * 16, 8), 16)
            cc[rows, :] += jnp.where(child < 0, 0.0, packets[peer, row0 : row0 + 16, :])
            return carry

        lax.fori_loop(0, self.P, one, 0)
        rows = jnp.concatenate([cc[pl.ds(k, S, stride=16), :] for k in range(16)], axis=0)
        wide = 0.5 * dot2(rows, half_back[...])
        covered = self.per_slot(lambda s: parents[s * 8]) >= 0
        for x in range(self.E):
            for c in range(4):
                row = ((x // 4) * 4 + c) * S
                for q in range(2):
                    lane0 = ((x // 2) % 2 * 2 + q) * COL
                    added = wide[row : row + S, lane0 : lane0 + COL]
                    put(q, x, c, jnp.where(covered, 0.0, get(q, x, c)) + added)

    def shifted(self, planes, amount):
        COL = self.COL
        lane = self.lane(self.S)
        moved = [roll(values, amount) for values in planes]
        if amount > 0:
            return [jnp.where(lane < amount, moved[1 - q], moved[q]) for q in range(2)]
        return [jnp.where(lane >= COL + amount, moved[1 - q], moved[q]) for q in range(2)]

    def interior(self, get, levels, forward_put, cot_get=None, cot_put=None):
        S, E, COL = self.S, self.E, self.COL
        ratio = self.ratio(levels)
        lane = self.lane(S)
        y_inside = [lane >= 0, lane < COL - E]
        z_inside = (lane & (E - 1)) != E - 1
        zero = jnp.zeros((S, COL), f32)

        def row_of(x, c):
            return pl.ds(pl.multiple_of((x * 4 + c) * S, S), S)

        def one(x, carry):
            after = jnp.minimum(x + 1, E - 1)
            x_inside = x < E - 1
            here = [[get(q, row_of(x, c)) for c in range(4)] for q in range(2)]
            inverse = [1.0 / here[q][0] for q in range(2)]
            ahead = [[get(q, row_of(after, c)) for c in range(4)] for q in range(2)]
            ahead_inv = [1.0 / ahead[q][0] for q in range(2)]
            flux_carry, cot_carry = carry
            new_flux, new_cot = [], []
            change = [[None] * 4 for _ in range(2)]
            if cot_get is not None:
                weight = [[get_c(q, row_of(x, c)) for c in range(4)] for q in range(2)]
                scaled = [[ratio * weight[q][c] for c in range(4)] for q in range(2)]
                ahead_scaled = [
                    [ratio * get_c(q, row_of(after, c)) for c in range(4)] for q in range(2)
                ]
                back = [[weight[q][c] for c in range(4)] for q in range(2)]
            for q in range(2):
                if forward_put is not None:
                    flux = flux_of(here[q], ahead[q], 0, inverse[q], ahead_inv[q])
                    flux = [jnp.where(x_inside, part, 0.0) for part in flux]
                    change[q] = [flux[c] - flux_carry[q * 4 + c] for c in range(4)]
                    new_flux += flux
                if cot_get is not None:
                    cot = [
                        jnp.where(x_inside, ahead_scaled[q][c] - scaled[q][c], 0.0) for c in range(4)
                    ]
                    left, right = flux_pull(here[q], ahead[q], 0, inverse[q], ahead_inv[q], cot)
                    back[q] = [back[q][c] + left[c] + cot_carry[q * 4 + c] for c in range(4)]
                    new_cot += right
            for normal, step, inside in ((1, E, y_inside), (2, 1, [z_inside, z_inside])):
                turned = [self.shifted([here[q][c] for q in range(2)], -step) for c in range(4)]
                turned_inv = self.shifted(inverse, -step)
                beyond = [[turned[c][q] for c in range(4)] for q in range(2)]
                if forward_put is not None:
                    flux = []
                    for q in range(2):
                        got = flux_of(here[q], beyond[q], normal, inverse[q], turned_inv[q])
                        flux.append([jnp.where(inside[q], part, 0.0) for part in got])
                    for c in range(4):
                        behind = self.shifted([flux[q][c] for q in range(2)], step)
                        for q in range(2):
                            change[q][c] = change[q][c] + (flux[q][c] - behind[q])
                if cot_get is not None:
                    turned_w = [self.shifted([scaled[q][c] for q in range(2)], -step) for c in range(4)]
                    rights = []
                    for q in range(2):
                        cot = [
                            jnp.where(inside[q], turned_w[c][q] - scaled[q][c], 0.0) for c in range(4)
                        ]
                        left, right = flux_pull(here[q], beyond[q], normal, inverse[q], turned_inv[q], cot)
                        back[q] = [back[q][c] + left[c] for c in range(4)]
                        rights.append(right)
                    for c in range(4):
                        moved = self.shifted([rights[q][c] for q in range(2)], step)
                        for q in range(2):
                            back[q][c] = back[q][c] + moved[q]
            for q in range(2):
                for c in range(4):
                    if forward_put is not None:
                        forward_put(q, row_of(x, c), here[q][c] - ratio * change[q][c])
                    if cot_get is not None:
                        cot_put(q, row_of(x, c), back[q][c])
            return (new_flux, new_cot)

        get_c = cot_get
        start = (
            [zero] * 8 if forward_put is not None else [],
            [zero] * 8 if cot_get is not None else [],
        )
        lax.fori_loop(0, E, one, start)


def run(body, name, scalars, arrays, outs, scratch):
    specs = [pl.BlockSpec(memory_space=pltpu.SMEM) for _ in scalars]
    operands = list(scalars)
    for item in arrays:
        if isinstance(item, tuple):
            block = (item[0].shape[0], item[0].shape[1] // 2)
            for q in range(2):
                specs.append(pl.BlockSpec(block, lambda i, q=q: (0, q)))
                operands.append(item[0])
        else:
            zeros = (0,) * item.ndim
            specs.append(pl.BlockSpec(item.shape, lambda i, zeros=zeros: zeros))
            operands.append(item)
    out_specs = []
    for shape, native in outs:
        if native:
            out_specs.append(pl.BlockSpec(memory_space=pl.ANY))
        else:
            zeros = (0,) * len(shape)
            out_specs.append(pl.BlockSpec(shape, lambda i, zeros=zeros: zeros))
    return pl.pallas_call(
        body,
        name=name,
        grid=(1,),
        in_specs=specs,
        out_specs=out_specs,
        out_shape=[jax.ShapeDtypeStruct(shape, f32) for shape, native in outs],
        scratch_shapes=scratch,
        compiler_params=pltpu.CompilerParams(vmem_limit_bytes=48 * 1024 * 1024),
    )(*operands)


def write_native(planes, out, sems):
    copies = []
    lanes = planes[0].shape[1]
    for q in range(2):
        copies.append(
            pltpu.make_async_copy(planes[q], out.at[:, pl.ds(q * lanes, lanes)], sems.at[q])
        )
        copies[-1].start()
    for copy in copies:
        copy.wait()


def boundary_fluxes(plan, layers, ghost, emit):
    for f in range(6):
        result = []
        for q in range(2):
            inner = [layers(q, f, c) for c in range(4)]
            outer = [ghost(q, f, c) for c in range(4)]
            inner_inv, outer_inv = 1.0 / inner[0], 1.0 / outer[0]
            if f % 2 == 0:
                result.append(flux_of(outer, inner, f // 2, outer_inv, inner_inv))
            else:
                result.append(flux_of(inner, outer, f // 2, inner_inv, outer_inv))
        for c in range(4):
            emit(f, c, [result[q][c] for q in range(2)])


def boundary_pull(plan, layers, ghost, cot, emit):
    for f in range(6):
        result = []
        for q in range(2):
            inner = [layers(q, f, c) for c in range(4)]
            outer = [ghost(q, f, c) for c in range(4)]
            weight = [cot(q, f, c) for c in range(4)]
            inner_inv, outer_inv = 1.0 / inner[0], 1.0 / outer[0]
            if f % 2 == 0:
                out_cot, in_cot = flux_pull(outer, inner, f // 2, outer_inv, inner_inv, weight)
            else:
                in_cot, out_cot = flux_pull(inner, outer, f // 2, inner_inv, outer_inv, weight)
            result.append((in_cot, out_cot))
        for c in range(4):
            emit(f, c, [result[q][0][c] for q in range(2)], [result[q][1][c] for q in range(2)])


def on_device(fields, guidance, levels, send_faces, ghost_peer, ghost_code, child_send, parent_peer):
    slots, _, extent, square = fields.shape
    peers = send_faces.shape[1]
    plan = Plan(slots, extent, peers)
    S, E, COL = slots, extent, plan.COL
    half_np = half_map(extent)
    half = jnp.asarray(half_np, bf16)
    half_back = jnp.asarray(np.ascontiguousarray(half_np.T), bf16)

    first_map, second_map = ghost_code // 5, ghost_code % 5
    turned = (jnp.arange(6) >= 4)[None, :, None]
    major = jnp.where(turned, second_map, first_map)
    minor = jnp.where(turned, first_map, second_map)
    refined = ghost_peer[:, :, 1] >= 0
    quarter = (major - 3) * 2 + (minor - 3)
    chosen = jnp.maximum(ghost_peer, 0)
    columns = [
        jnp.where(refined, jnp.sum(jnp.where(quarter == k, chosen, 0), axis=2), chosen[:, :, 0])
        for k in range(4)
    ]
    coarser = ghost_code[:, :, 0] > 0
    kind = jnp.where(
        ghost_peer[:, :, 0] < 0, 3, jnp.where(refined, 2, jnp.where(coarser, 1, 0))
    )
    single = jnp.logical_and(coarser, jnp.logical_not(refined))
    columns += [
        kind,
        jnp.where(single, major[:, :, 0] - 1, 0),
        jnp.where(single, minor[:, :, 0] - 1, 0),
        jnp.zeros_like(kind),
    ]
    table = jnp.stack(columns, axis=-1).astype(jnp.int32).reshape(-1)
    send = send_faces.reshape(-1)
    children = child_send.reshape(-1)
    parents = parent_peer.reshape(-1)
    native_fields = fields.reshape(plan.native)
    native_guidance = guidance.reshape(plan.native)

    def exchange(packets):
        return lax.all_to_all(packets, "blk", split_axis=0, concat_axis=0, tiled=True)

    def vm(*shape):
        return pltpu.VMEM(shape, f32)

    def occupied_of(levels_ref):
        return plan.per_slot(lambda s: levels_ref[s]) >= 0

    fb_scratch = vm(*plan.fb)
    signs = [1.0, -1.0, 1.0, -1.0, 1.0, -1.0]

    def layers_of(get, fb, ff):
        for c in range(4):
            faces = plan.extract(get, c)
            for f in range(6):
                for q in range(2):
                    if fb is not None:
                        fb[q, plan.fb_rows(f, c), :] = faces[f][q]
                    if ff is not None:
                        ff[q, (f * 4 + c) * S : (f * 4 + c + 1) * S, :] = faces[f][q]

    def corrected_cot_of(get, levels_ref, fb):
        ratio = plan.ratio(levels_ref)
        for c in range(4):
            faces = plan.extract(get, c)
            for f in range(6):
                for q in range(2):
                    fb[q, plan.fb_rows(f, c), :] = (signs[f] * ratio) * faces[f][q]

    def finished(partial, corr, levels_ref, put):
        ratio = plan.ratio(levels_ref)
        occupied = ratio > 0.0
        get = plan.slab_at(partial)

        def face(q, f, c):
            value = corr[q, plan.fb_rows(f, c), :]
            return jnp.where(occupied, (signs[f] * ratio) * value, 0.0)

        for x in range(E):
            for c in range(4):
                for q in range(2):
                    put(q, x, c, get(q, x, c) + plan.spread(face, q, x, c))

    def ghost_reader(gb, layers, levels_ref):
        occupied = occupied_of(levels_ref)
        return lambda q, f, c: jnp.where(
            occupied, gb[q, plan.fb_rows(f, c, True), :], layers(q, f, c)
        )

    def slab_put(ref):
        def put(q, x, c, value):
            ref[q, (x * 4 + c) * S : (x * 4 + c + 1) * S, :] = value

        return put

    def dyn_get(ref):
        return lambda q, rows: ref[q, rows, :]

    def dyn_put(ref):
        def put(q, rows, value):
            ref[q, rows, :] = value

        return put

    ghost_scratch = [
        vm(8, 3 * S * 8, COL),
        vm(3 * S * 8, COL),
        pltpu.VMEM((3 * S * 8, COL), jnp.int32),
    ]

    def first_pack(send_s, parents_s, f0, f1, g0, g1, volume, layers, packets, fb):
        get = plan.native_at([f0, f1])
        for x in range(E):
            for c in range(4):
                for q in range(2):
                    volume[q, (x * 4 + c) * S : (x * 4 + c + 1) * S, :] = get(q, x, c)
        layers_of(plan.slab_at(volume), fb, layers)
        plan.pack_faces(fb, send_s, packets)
        planes = [g0, g1]
        plan.pack_octants(lambda s, x, q: planes[q][plan.native_rows(s, x), :], parents_s, packets, 48)

    volume1, layers1, packets = run(
        first_pack,
        "first_pack",
        [send, parents],
        [(native_fields,), (native_guidance,)],
        [(plan.slab, False), (plan.ff, False), ((peers, 64, COL), False)],
        [fb_scratch],
    )
    received1 = exchange(packets)

    def interior_first(levels_s, volume, partial):
        plan.interior(dyn_get(volume), levels_s, dyn_put(partial))

    (partial1,) = run(interior_first, "interior_first", [levels], [volume1], [(plan.slab, False)], [])

    def first_flux(levels_s, send_s, table_s, children_s, parents_s, g0, g1, layers, recv, half_r,
                   back_r, gb, b_fb, up, cot_fb, packets, planes, near, kinds, ff, rb, cc):
        plan.ghosts(recv, table_s, planes, near, kinds, gb, half_r, back_r)
        layer = plan.ff_at(layers)

        def emit(f, c, values):
            for q in range(2):
                b_fb[q, plan.fb_rows(f, c), :] = values[q]
                ff[q, (f * 4 + c) * S : (f * 4 + c + 1) * S, :] = values[q]

        boundary_fluxes(plan, layer, ghost_reader(gb, layer, levels_s), emit)
        plan.pack_averages(plan.ff_at(ff), rb, send_s, packets, 0, half_r)
        plan.upward(recv, 48, cc, children_s, parents_s, plan.native_at([g0, g1]), slab_put(up), back_r)
        corrected_cot_of(plan.slab_at(up), levels_s, cot_fb)
        plan.pack_quarters(cot_fb, table_s, packets, 16)

    ghosts1, fluxes1, up2, corrcot2, packets = run(
        first_flux,
        "first_flux",
        [levels, send, table, children, parents],
        [(native_guidance,), layers1, received1, half, half_back],
        [(plan.fb, False), (plan.fb, False), (plan.slab, False), (plan.fb, False),
         ((peers, 32, COL), False)],
        ghost_scratch + [vm(*plan.ff), vm(*plan.coarse), vm((S + 1) * 16, COL)],
    )
    received2 = exchange(packets)

    quarter_sums = [vm(S * 16, COL) for _ in range(6)]
    face_sums = [vm(2, S * 8, COL) for _ in range(6)]

    def flux_cot_of(recv, row0, cot_fb, table_s, send_s, sums, kinds, flux_cot, back_r):
        for s in range(S):
            for f in range(6):
                row = ((f // 2) * S + s) * 8 + (f % 2) * 4
                kinds[row : row + 4, :] = jnp.full((4, COL), table_s[(s * 6 + f) * 8 + 4], jnp.int32)

        def face_out(f, c, wide):
            keep = kinds[plan.fb_rows(f, c), :] != 2
            for q in range(2):
                own = jnp.where(keep, cot_fb[q, plan.fb_rows(f, c), :], 0.0)
                flux_cot[q, (f * 4 + c) * S : (f * 4 + c + 1) * S, :] = own + wide[q]

        plan.take_quarters(recv, row0, send_s, sums, face_out, back_r)

    def first_update(levels_s, send_s, table_s, children_s, partial, b_fb, cot_fb, recv, half_r,
                     back_r, updated, flux_cot, packets, corr, cb, kinds, *sums):
        plan.corrected(b_fb, recv, 0, table_s, corr)
        finished(partial, corr, levels_s, slab_put(updated))
        plan.pack_children(plan.slab_at(updated), cb, children_s, packets, 0, half_r)
        flux_cot_of(recv, 16, cot_fb, table_s, send_s, sums, kinds, flux_cot, back_r)

    updated1, fluxcot2, packets = run(
        first_update,
        "first_update",
        [levels, send, table, children],
        [partial1, fluxes1, corrcot2, received2, half, half_back],
        [(plan.slab, False), (plan.ff, False), ((peers, 16, COL), False)],
        [fb_scratch, vm(*plan.coarse), pltpu.VMEM((3 * S * 8, COL), jnp.int32)] + quarter_sums,
    )
    received3 = exchange(packets)

    def middle_pack(send_s, parents_s, updated, recv, volume, layers, packets, fb):
        volume[...] = updated[...]

        def store(s, x, q, value):
            volume[q, plan.slab_rows(s, x), :] = value

        plan.place_octants(recv, 0, parents_s, store)
        layers_of(plan.slab_at(volume), fb, layers)
        plan.pack_faces(fb, send_s, packets)

    volume2, layers2, packets = run(
        middle_pack,
        "middle_pack",
        [send, parents],
        [updated1, received3],
        [(plan.slab, False), (plan.ff, False), ((peers, 48, COL), False)],
        [fb_scratch],
    )
    received4 = exchange(packets)

    def interior_both(levels_s, volume, cot, partial, through):
        plan.interior(dyn_get(volume), levels_s, dyn_put(partial), dyn_get(cot), dyn_put(through))

    partial2, through2 = run(
        interior_both, "interior_both", [levels], [volume2, up2],
        [(plan.slab, False), (plan.slab, False)], [],
    )

    def second_flux(levels_s, send_s, table_s, layers, recv, flux_cot, half_r, back_r, b_fb,
                    layer_cot, packets, planes, near, kinds, gb, ff, rb, gcot):
        plan.ghosts(recv, table_s, planes, near, kinds, gb, half_r, back_r)
        layer = plan.ff_at(layers)
        ghost = ghost_reader(gb, layer, levels_s)

        def emit(f, c, values):
            for q in range(2):
                b_fb[q, plan.fb_rows(f, c), :] = values[q]
                ff[q, (f * 4 + c) * S : (f * 4 + c + 1) * S, :] = values[q]

        boundary_fluxes(plan, layer, ghost, emit)
        plan.pack_averages(plan.ff_at(ff), rb, send_s, packets, 48, half_r)

        def emit_cot(f, c, inner, outer):
            for q in range(2):
                layer_cot[q, (f * 4 + c) * S : (f * 4 + c + 1) * S, :] = inner[q]
                gcot[q, plan.fb_rows(f, c, True), :] = outer[q]

        boundary_pull(plan, layer, ghost, plan.ff_at(flux_cot), emit_cot)
        plan.pack_ghost_cot(gcot, table_s, planes, near, packets, half_r, back_r)

    fluxes2, layercot2, packets = run(
        second_flux,
        "second_flux",
        [levels, send, table],
        [layers2, received4, fluxcot2, half, half_back],
        [(plan.fb, False), (plan.ff, False), ((peers, 64, COL), False)],
        ghost_scratch + [fb_scratch, vm(*plan.ff), vm(*plan.coarse), fb_scratch],
    )
    received5 = exchange(packets)

    def total_face(layer_cot, sums):
        own = plan.ff_at(layer_cot)

        def face(q, f, c):
            return own(q, f, c) + sums[f][q, pl.ds((f % 2) * 4 + c, S, stride=8), :]

        return face

    def add_layers(through, layer_cot, total, sums, put):
        face = total_face(layer_cot, sums)
        for f in range(6):
            for c in range(4):
                for q in range(2):
                    total[q, (f * 4 + c) * S : (f * 4 + c + 1) * S, :] = face(q, f, c)
        get = plan.slab_at(through)
        summed = plan.ff_at(total)
        for x in range(E):
            for c in range(4):
                for q in range(2):
                    put(q, x, c, get(q, x, c) + plan.spread(summed, q, x, c))

    def second_update(levels_s, send_s, table_s, children_s, parents_s, partial, b_fb, through,
                      layer_cot, recv, half_r, updated, inner, packets, corr, cb, total, *sums):
        plan.corrected(b_fb, recv, 48, table_s, corr)
        finished(partial, corr, levels_s, slab_put(updated))
        plan.pack_children(plan.slab_at(updated), cb, children_s, packets, 0, half_r)
        plan.take_faces(recv, send_s, sums)
        add_layers(through, layer_cot, total, sums, slab_put(inner))
        plan.pack_octants(
            lambda s, x, q: inner[q, plan.slab_rows(s, x), :], parents_s, packets, 16
        )

    updated2, inner_cot, packets = run(
        second_update,
        "second_update",
        [levels, send, table, children, parents],
        [partial2, fluxes2, through2, layercot2, received5, half],
        [(plan.slab, False), (plan.slab, False), ((peers, 32, COL), False)],
        [fb_scratch, vm(*plan.coarse), vm(*plan.ff)] + face_sums,
    )
    received6 = exchange(packets)

    native_planes = [vm(S * 4 * E, COL), vm(S * 4 * E, COL)]

    def last_state(levels_s, table_s, children_s, parents_s, updated, inner, recv, back_r,
                   final, up, cot_fb, packets, n0, n1, cc, sems):
        plan.upward(recv, 16, cc, children_s, parents_s, plan.slab_at(inner), slab_put(up), back_r)
        corrected_cot_of(plan.slab_at(up), levels_s, cot_fb)
        plan.pack_quarters(cot_fb, table_s, packets, 0)
        planes = [n0, n1]
        get = plan.slab_at(updated)
        for x in range(E):
            for c in range(4):
                for q in range(2):
                    planes[q][pl.ds(c * E + x, S, stride=4 * E), :] = get(q, x, c)

        def store(s, x, q, value):
            planes[q][plan.native_rows(s, x), :] = value

        plan.place_octants(recv, 0, parents_s, store)
        write_native(planes, final, sems)

    final_fields, up1, corrcot1, packets = run(
        last_state,
        "last_state",
        [levels, table, children, parents],
        [updated2, inner_cot, received6, half_back],
        [(plan.native, True), (plan.slab, False), (plan.fb, False), ((peers, 16, COL), False)],
        native_planes + [vm((S + 1) * 16, COL), pltpu.SemaphoreType.DMA((2,))],
    )
    received7 = exchange(packets)

    def interior_back(levels_s, volume, cot, through):
        plan.interior(dyn_get(volume), levels_s, None, dyn_get(cot), dyn_put(through))

    (through1,) = run(
        interior_back, "interior_back", [levels], [volume1, up1], [(plan.slab, False)], []
    )

    def first_pull(levels_s, send_s, table_s, layers, gb, cot_fb, recv, half_r, back_r, layer_cot,
                   packets, planes, near, kinds, flux_cot, gcot, *sums):
        flux_cot_of(recv, 0, cot_fb, table_s, send_s, sums, kinds, flux_cot, back_r)
        layer = plan.ff_at(layers)

        def emit_cot(f, c, inner, outer):
            for q in range(2):
                layer_cot[q, (f * 4 + c) * S : (f * 4 + c + 1) * S, :] = inner[q]
                gcot[q, plan.fb_rows(f, c, True), :] = outer[q]

        boundary_pull(plan, layer, ghost_reader(gb, layer, levels_s), plan.ff_at(flux_cot), emit_cot)
        plan.pack_ghost_cot(gcot, table_s, planes, near, packets, half_r, back_r)

    layercot1, packets = run(
        first_pull,
        "first_pull",
        [levels, send, table],
        [layers1, ghosts1, corrcot1, received7, half, half_back],
        [(plan.ff, False), ((peers, 48, COL), False)],
        ghost_scratch + [vm(*plan.ff), fb_scratch] + quarter_sums,
    )
    received8 = exchange(packets)

    def last_cot(send_s, through, layer_cot, recv, gradient, total, n0, n1, sems, *sums):
        plan.take_faces(recv, send_s, sums)
        planes = [n0, n1]

        def put(q, x, c, value):
            planes[q][pl.ds(c * E + x, S, stride=4 * E), :] = value

        add_layers(through, layer_cot, total, sums, put)
        write_native(planes, gradient, sems)

    (gradient,) = run(
        last_cot,
        "last_cot",
        [send],
        [through1, layercot1, received8],
        [(plan.native, True)],
        [vm(*plan.ff)] + native_planes + [pltpu.SemaphoreType.DMA((2,))] + face_sums,
    )
    return (final_fields.reshape(fields.shape), gradient.reshape(fields.shape))


def solution(mesh):
    placed = (
        P("blk", None, None, None),
        P("blk", None, None, None),
        P("blk"),
        P("blk", None, None),
        P("blk", None, None),
        P("blk", None, None),
        P("blk", None),
        P("blk", None),
    )
    return jax.shard_map(
        on_device,
        mesh=mesh,
        in_specs=placed,
        out_specs=(P("blk", None, None, None), P("blk", None, None, None)),
        check_vma=False,
    )
```

```python
import jax
import jax.numpy as jnp
import numpy as np
from jax import lax
from jax.experimental import pallas as pl
from jax.experimental.pallas import tpu as pltpu
from jax.sharding import PartitionSpec as P

sound_speed = 1.0
base_ratio = 0.04
speed_floor = 0.01
f32 = jnp.float32
bf16 = jnp.bfloat16


def half_map(extent):
    half = extent // 2
    square = extent * extent
    table = np.zeros((2, extent, extent, half, 2, half), np.float32)
    for group in range(2):
        for i in range(extent):
            for j in range(extent):
                table[group, i, j, i // 2, group, j // 2] = 0.25
    return table.reshape(2 * square, square // 2)


def dot2(values, table):
    high = values.astype(bf16)
    low = (values - high.astype(f32)).astype(bf16)
    return jnp.dot(high, table, preferred_element_type=f32) + jnp.dot(
        low, table, preferred_element_type=f32
    )


def roll(values, shift):
    lanes = values.shape[1]
    shift = shift % lanes
    return values if shift == 0 else pltpu.roll(values, shift, 1)


def flux_of(behind, beyond, normal, inv_behind, inv_beyond):
    v = behind[1 + normal] * inv_behind
    w = beyond[1 + normal] * inv_beyond
    c = sound_speed + jnp.sqrt(0.5 * (v * v + w * w) + speed_floor)
    result = [0.5 * ((behind[1 + normal] + beyond[1 + normal]) - c * (beyond[0] - behind[0]))]
    for k in range(1, 4):
        total = behind[k] * v + beyond[k] * w
        if k == 1 + normal:
            total = total + (sound_speed * sound_speed) * (behind[0] + beyond[0])
        result.append(0.5 * (total - c * (beyond[k] - behind[k])))
    return result


def flux_pull(behind, beyond, normal, inv_behind, inv_beyond, cot):
    v = behind[1 + normal] * inv_behind
    w = beyond[1 + normal] * inv_beyond
    inside = 0.5 * (v * v + w * w) + speed_floor
    root = jnp.sqrt(inside)
    c = sound_speed + root
    half_cot = [0.5 * part for part in cot]
    jump = half_cot[0] * (beyond[0] - behind[0])
    v_cot = half_cot[1] * behind[1]
    w_cot = half_cot[1] * beyond[1]
    for k in range(1, 4):
        jump = jump + half_cot[k] * (beyond[k] - behind[k])
        if k > 1:
            v_cot = v_cot + half_cot[k] * behind[k]
            w_cot = w_cot + half_cot[k] * beyond[k]
    scale = jump * (-0.5) / root
    v_cot = (v_cot + scale * v) * inv_behind
    w_cot = (w_cot + scale * w) * inv_beyond
    plus = v + c
    minus = w - c
    behind_cot = []
    beyond_cot = []
    pressure = (sound_speed * sound_speed) * half_cot[1 + normal]
    for k in range(4):
        if k == 0:
            behind_cot.append(c * half_cot[0] + pressure - v_cot * v)
            beyond_cot.append(pressure - c * half_cot[0] - w_cot * w)
        else:
            left = half_cot[k] * plus
            right = half_cot[k] * minus
            if k == 1 + normal:
                left = left + half_cot[0] + v_cot
                right = right + half_cot[0] + w_cot
            behind_cot.append(left)
            beyond_cot.append(right)
    return behind_cot, beyond_cot


class Plan:
    def __init__(self, slots, extent, peers):
        self.S = slots
        self.E = extent
        self.P = peers
        self.H = extent // 2
        self.COL = extent * extent // 2
        self.slab = (2, extent * 4 * slots, self.COL)
        self.ff = (2, 6 * 4 * slots, self.COL)
        self.fb = (2, 3 * slots * 8, self.COL)
        self.native = (slots * 4 * extent, 2 * self.COL)
        self.coarse = (slots * 16, self.COL)

    def lane(self, rows):
        return lax.broadcasted_iota(jnp.int32, (rows, self.COL), 1)

    def low(self, rows):
        return (self.lane(rows) & (self.E - 1)) < self.H

    def per_slot(self, scalar_of):
        sub = lax.broadcasted_iota(jnp.int32, (self.S, self.COL), 0)
        value = jnp.zeros((self.S, self.COL), jnp.int32)
        for s in range(self.S):
            value = jnp.where(sub == s, scalar_of(s), value)
        return value

    def ratio(self, levels):
        level = self.per_slot(lambda s: levels[s])
        degree = level.astype(f32)
        ratio = base_ratio * (1.0 + degree + 0.5 * degree * (degree - 1.0))
        return jnp.where(level >= 0, ratio, 0.0)

    def slab_at(self, ref):
        return lambda q, x, c: ref[q, (x * 4 + c) * self.S : (x * 4 + c + 1) * self.S, :]

    def native_at(self, planes):
        step = 4 * self.E
        return lambda q, x, c: planes[q][pl.ds(c * self.E + x, self.S, stride=step), :]

    def ff_at(self, ref):
        return lambda q, f, c: ref[q, (f * 4 + c) * self.S : (f * 4 + c + 1) * self.S, :]

    def fb_rows(self, f, c, swapped=False):
        side = f % 2
        half = 1 - side if swapped else side
        return pl.ds((f // 2) * self.S * 8 + half * 4 + c, self.S, stride=8)

    def extract(self, get, c):
        E, H, COL = self.E, self.H, self.COL
        lane = self.lane(self.S)
        group = lax.shift_right_logical(lane, E.bit_length() - 1)
        within = lane & (E - 1)
        faces = [[get(q, 0, c) for q in range(2)], [get(q, E - 1, c) for q in range(2)]]
        low_y, high_y, low_z, high_z = [], [], [], []
        for q in range(2):
            first, last, near, far = None, None, None, None
            for k in range(H):
                a = roll(get(0, q * H + k, c), E * k)
                b = roll(get(1, q * H + k, c), E * k - (COL - E))
                first = a if first is None else jnp.where(group == k, a, first)
                last = b if last is None else jnp.where(group == k, b, last)
            for x in range(E):
                source = get(q, x, c)
                a = roll(source, x)
                b = roll(source, x - (E - 1))
                near = a if near is None else jnp.where(within == x, a, near)
                far = b if far is None else jnp.where(within == x, b, far)
            low_y.append(first)
            high_y.append(last)
            low_z.append(near)
            high_z.append(far)
        return faces + [low_y, high_y, low_z, high_z]

    def spread(self, face, q, x, c):
        E, H, COL = self.E, self.H, self.COL
        lane = self.lane(self.S)
        within = lane & (E - 1)
        k = x % H
        y_face = face(x // H, 2 + q, c)
        if q == 0:
            total = jnp.where(lane < E, roll(y_face, -E * k), 0.0)
        else:
            total = jnp.where(lane >= COL - E, roll(y_face, (COL - E) - E * k), 0.0)
        near = roll(face(q, 4, c), -x)
        far = roll(face(q, 5, c), E - 1 - x)
        total = total + jnp.where(within == 0, near, jnp.where(within == E - 1, far, 0.0))
        if x == 0:
            total = total + face(q, 0, c)
        if x == E - 1:
            total = total + face(q, 1, c)
        return total

    def pack_faces(self, fb, send, out):
        sub = lax.broadcasted_iota(jnp.int32, (8, self.COL), 0)

        def one(peer, carry):
            for axis in range(3):
                slots = [jnp.maximum(send[peer, axis * 2 + side], 0) for side in range(2)]
                for q in range(2):
                    lo, hi = [
                        fb[q, pl.ds(pl.multiple_of((axis * self.S + slot) * 8, 8), 8), :]
                        for slot in slots
                    ]
                    row = axis * 16 + q * 8
                    out[peer, row : row + 8, :] = jnp.where(sub < 4, lo, hi)
            return carry

        lax.fori_loop(0, self.P, one, 0)

    def take_faces(self, packets, send, sums):
        def one(peer, carry):
            for f in range(6):
                slot = jnp.maximum(send[peer, f], 0)
                rows = pl.ds(pl.multiple_of(slot * 8, 8), 8)
                for q in range(2):
                    at = (f // 2) * 16 + q * 8
                    sums[f][q, rows, :] += packets[peer, at : at + 8, :]
            return carry

        for f in range(6):
            sums[f][...] = jnp.zeros(sums[f].shape, f32)
        lax.fori_loop(0, self.P, one, 0)

    def pack_averages(self, face, rb, send, out, row0, half):
        S, COL = self.S, self.COL
        rows = []
        for axis in range(3):
            for c in range(4):
                rows.append(
                    jnp.concatenate(
                        [face(q, 2 * axis + side, c) for side in range(2) for q in range(2)], axis=1
                    )
                )
        small = dot2(jnp.concatenate(rows, axis=0), half[...])
        for k in range(12):
            rb[pl.ds(k, S, stride=16), :] = small[k * S : (k + 1) * S]
        zero = jnp.zeros((S, COL), f32)
        for k in range(12, 16):
            rb[pl.ds(k, S, stride=16), :] = zero
        sub = lax.broadcasted_iota(jnp.int32, (8, COL), 0)
        low = self.low(8)

        def one(peer, carry):
            def part(f, at):
                slot = jnp.maximum(send[peer, f], 0)
                return rb[pl.ds(pl.multiple_of(slot * 16 + at, 8), 8), :]

            first = jnp.where(low, part(0, 0), part(1, 0))
            second = jnp.where(low, part(2, 0), part(3, 0))
            out[peer, row0 : row0 + 8, :] = jnp.where(sub < 4, first, second)
            out[peer, row0 + 8 : row0 + 16, :] = jnp.where(low, part(4, 8), part(5, 8))
            return carry

        lax.fori_loop(0, self.P, one, 0)

    def pack_quarters(self, fb, table, out, row0):
        E, H = self.E, self.H
        low = self.low(4)

        def clear(peer, carry):
            out[peer, row0 : row0 + 16, :] = jnp.zeros((16, self.COL), f32)
            return carry

        lax.fori_loop(0, self.P, clear, 0)
        for s in range(self.S):
            for f in range(6):
                base = (s * 6 + f) * 8

                def send_quarters(s=s, f=f, base=base):
                    axis, side = f // 2, f % 2
                    keep = low if side == 1 else jnp.logical_not(low)
                    row = (axis * self.S + s) * 8 + side * 4
                    at = row0 + axis * 4
                    for h in range(2):
                        values = fb[h, row : row + 4, :]
                        for g in range(2):
                            moved = roll(values, H * ((1 - side) - g))
                            peer = table[base + h * 2 + g]
                            out[peer, at : at + 4, :] += jnp.where(keep, moved, 0.0)

                pl.when(table[base + 4] == 2)(send_quarters)

    def take_quarters(self, packets, row0, send, sums, face_out, half_back):
        S, COL = self.S, self.COL

        def one(peer, carry):
            block = packets[peer, row0 : row0 + 16, :]
            for f in range(6):
                slot = jnp.maximum(send[peer, f], 0)
                rows = pl.ds(pl.multiple_of(slot * 16, 8), 16)
                sums[f][rows, :] += block
            return carry

        for f in range(6):
            sums[f][...] = jnp.zeros(sums[f].shape, f32)
        lax.fori_loop(0, self.P, one, 0)
        for f in range(6):
            axis, side = f // 2, f % 2
            rows = jnp.concatenate(
                [sums[f][pl.ds(axis * 4 + c, S, stride=16), :] for c in range(4)], axis=0
            )
            wide = dot2(rows, half_back[:, side * 2 * COL : (side + 1) * 2 * COL])
            for c in range(4):
                face_out(f, c, [wide[c * S : (c + 1) * S, q * COL : (q + 1) * COL] for q in range(2)])

    def ghosts(self, packets, table, planes, near, kinds, gb, half, half_back):
        S, COL, H = self.S, self.COL, self.H
        for s in range(S):
            for f in range(6):
                base = (s * 6 + f) * 8
                axis, half_row = f // 2, (1 - f % 2) * 4
                row = (axis * S + s) * 8 + half_row
                first = None
                for k in range(4):
                    peer = table[base + k]
                    got = []
                    for q in range(2):
                        at = axis * 16 + q * 8 + half_row
                        values = packets[peer, at : at + 4, :]
                        planes[k * 2 + q, row : row + 4, :] = values
                        got.append(values)
                    if k == 0:
                        first = got
                source = jnp.where(table[base + 5] == 1, first[1], first[0])
                source = jnp.where(table[base + 6] == 1, roll(source, -H), source)
                near[row : row + 4, :] = source
                kinds[row : row + 4, :] = jnp.full((4, COL), table[base + 4], jnp.int32)
        for axis in range(3):
            rows = slice(axis * S * 8, (axis + 1) * S * 8)
            kind = kinds[rows, :]
            coarse = 4.0 * dot2(near[rows, :], half_back[:, : 2 * COL])
            for h in range(2):
                parts = [planes[(h * 2 + g) * 2 + q, rows, :] for g in range(2) for q in range(2)]
                fine = dot2(jnp.concatenate(parts, axis=1), half[...])
                value = jnp.where(kind == 1, coarse[:, h * COL : (h + 1) * COL], planes[h, rows, :])
                gb[h, rows, :] = jnp.where(kind == 2, fine, value)

    def pack_ghost_cot(self, gb, table, wide, near, out, half, half_back):
        S, COL, H = self.S, self.COL, self.H
        low = self.low(4)

        def clear(peer, carry):
            out[peer, 0:48, :] = jnp.zeros((48, COL), f32)
            return carry

        lax.fori_loop(0, self.P, clear, 0)
        rows_all = 3 * S * 8
        for h in range(2):
            for g in range(2):
                spread = dot2(gb[h, :, :], half_back[:, g * 2 * COL : (g + 1) * 2 * COL])
                for q in range(2):
                    wide[(h * 2 + g) * 2 + q, :, :] = spread[:, q * COL : (q + 1) * COL]
        both = jnp.concatenate([gb[0, :, :], gb[1, :, :]], axis=1)
        near[...] = 4.0 * dot2(both, half[0 : 2 * COL, :])
        del rows_all
        for s in range(S):
            for f in range(6):
                base = (s * 6 + f) * 8
                axis, half_row = f // 2, (1 - f % 2) * 4
                row = (axis * S + s) * 8 + half_row
                kind = table[base + 4]

                def same(base=base, axis=axis, half_row=half_row, row=row):
                    peer = table[base]
                    for q in range(2):
                        at = axis * 16 + q * 8 + half_row
                        out[peer, at : at + 4, :] += gb[q, row : row + 4, :]

                def coarse(base=base, axis=axis, half_row=half_row, row=row):
                    peer = table[base]
                    values = near[row : row + 4, :]
                    values = jnp.where(table[base + 6] == 1, roll(values, H), values)
                    for q in range(2):
                        at = axis * 16 + q * 8 + half_row
                        out[peer, at : at + 4, :] += jnp.where(table[base + 5] == q, values, 0.0)

                def fine(base=base, axis=axis, half_row=half_row, row=row):
                    for k in range(4):
                        peer = table[base + k]
                        for q in range(2):
                            at = axis * 16 + q * 8 + half_row
                            out[peer, at : at + 4, :] += wide[k * 2 + q, row : row + 4, :]

                pl.when(kind == 0)(same)
                pl.when(kind == 1)(coarse)
                pl.when(kind == 2)(fine)

    def corrected(self, b_fb, packets, row0, table, out):
        H = self.H
        low = self.low(4)
        out[...] = b_fb[...]
        for s in range(self.S):
            for f in range(6):
                base = (s * 6 + f) * 8

                def replace(s=s, f=f, base=base):
                    axis, side = f // 2, f % 2
                    row = (axis * self.S + s) * 8 + side * 4
                    at = row0 + axis * 4
                    for h in range(2):
                        got = []
                        for g in range(2):
                            values = packets[table[base + h * 2 + g], at : at + 4, :]
                            got.append(roll(values, H * (g - (1 - side))))
                        out[h, row : row + 4, :] = jnp.where(low, got[0], got[1])

                pl.when(table[base + 4] == 2)(replace)

    def pack_octants(self, load, parents, out, row0):
        H = self.H
        low = self.low(4)
        for s in range(self.S):

            def send(s=s):
                for ox in range(2):
                    for oy in range(2):
                        peers = [parents[s, ox * 4 + oy * 2 + oz] for oz in range(2)]
                        for pair in range(H // 2):
                            x = ox * H + pair * 2
                            first, second = load(s, x, oy), load(s, x + 1, oy)
                            at = row0 + pair * 4
                            out[peers[0], at : at + 4, :] = jnp.where(low, first, roll(second, H))
                            out[peers[1], at : at + 4, :] = jnp.where(low, roll(first, -H), second)

            pl.when(parents[s, 0] >= 0)(send)

    def place_octants(self, packets, row0, parents, store):
        H = self.H
        low = self.low(4)
        for s in range(self.S):

            def place(s=s):
                for ox in range(2):
                    for oy in range(2):
                        peers = [parents[s, ox * 4 + oy * 2 + oz] for oz in range(2)]
                        for pair in range(H // 2):
                            x = ox * H + pair * 2
                            at = row0 + pair * 4
                            first = packets[peers[0], at : at + 4, :]
                            second = packets[peers[1], at : at + 4, :]
                            store(s, x, oy, jnp.where(low, first, roll(second, H)))
                            store(s, x + 1, oy, jnp.where(low, roll(first, -H), second))

            pl.when(parents[s, 0] >= 0)(place)

    def slab_rows(self, s, x):
        return pl.ds(x * 4 * self.S + s, 4, stride=self.S)

    def native_rows(self, s, x):
        return pl.ds(s * 4 * self.E + x, 4, stride=self.E)

    def average_blocks(self, get, cb, half):
        S = self.S
        rows = []
        for pair in range(self.E // 4):
            for c in range(4):
                x = 4 * pair
                rows.append(
                    jnp.concatenate(
                        [get(q, x + 2 * a, c) + get(q, x + 2 * a + 1, c) for a in range(2) for q in range(2)],
                        axis=1,
                    )
                )
        small = 0.5 * dot2(jnp.concatenate(rows, axis=0), half[...])
        for k in range(16):
            cb[pl.ds(k, S, stride=16), :] = small[k * S : (k + 1) * S]

    def pack_children(self, cb, children, out, row0):
        def one(peer, carry):
            slot = jnp.maximum(children[peer], 0)
            out[peer, row0 : row0 + 16, :] = cb[pl.ds(pl.multiple_of(slot * 16, 8), 16), :]
            return carry

        lax.fori_loop(0, self.P, one, 0)

    def upward(self, packets, row0, cc, children, parents, get, put, half_back):
        S, COL = self.S, self.COL
        cc[...] = jnp.zeros(cc.shape, f32)

        def one(peer, carry):
            child = children[peer]
            slot = jnp.where(child < 0, S, child)
            rows = pl.ds(pl.multiple_of(slot * 16, 8), 16)
            cc[rows, :] += jnp.where(child < 0, 0.0, packets[peer, row0 : row0 + 16, :])
            return carry

        lax.fori_loop(0, self.P, one, 0)
        rows = jnp.concatenate([cc[pl.ds(k, S, stride=16), :] for k in range(16)], axis=0)
        wide = 0.5 * dot2(rows, half_back[...])
        covered = self.per_slot(lambda s: parents[s, 0]) >= 0
        for x in range(self.E):
            for c in range(4):
                row = ((x // 4) * 4 + c) * S
                for q in range(2):
                    lane0 = ((x // 2) % 2 * 2 + q) * COL
                    added = wide[row : row + S, lane0 : lane0 + COL]
                    put(q, x, c, jnp.where(covered, 0.0, get(q, x, c)) + added)

    def shifted(self, planes, amount):
        COL = self.COL
        lane = self.lane(self.S)
        moved = [roll(values, amount) for values in planes]
        if amount > 0:
            return [jnp.where(lane < amount, moved[1 - q], moved[q]) for q in range(2)]
        return [jnp.where(lane >= COL + amount, moved[1 - q], moved[q]) for q in range(2)]

    def interior(self, get, levels, forward_put, cot_get=None, cot_put=None):
        S, E, COL = self.S, self.E, self.COL
        ratio = self.ratio(levels)
        lane = self.lane(S)
        y_inside = [lane >= 0, lane < COL - E]
        z_inside = (lane & (E - 1)) != E - 1
        zero = jnp.zeros((S, COL), f32)

        def row_of(x, c):
            return pl.ds(pl.multiple_of((x * 4 + c) * S, S), S)

        def one(x, carry):
            after = jnp.minimum(x + 1, E - 1)
            x_inside = x < E - 1
            here = [[get(q, row_of(x, c)) for c in range(4)] for q in range(2)]
            inverse = [1.0 / here[q][0] for q in range(2)]
            ahead = [[get(q, row_of(after, c)) for c in range(4)] for q in range(2)]
            ahead_inv = [1.0 / ahead[q][0] for q in range(2)]
            flux_carry, cot_carry = carry
            new_flux, new_cot = [], []
            change = [[None] * 4 for _ in range(2)]
            if cot_get is not None:
                weight = [[get_c(q, row_of(x, c)) for c in range(4)] for q in range(2)]
                scaled = [[ratio * weight[q][c] for c in range(4)] for q in range(2)]
                ahead_scaled = [
                    [ratio * get_c(q, row_of(after, c)) for c in range(4)] for q in range(2)
                ]
                back = [[weight[q][c] for c in range(4)] for q in range(2)]
            for q in range(2):
                if forward_put is not None:
                    flux = flux_of(here[q], ahead[q], 0, inverse[q], ahead_inv[q])
                    flux = [jnp.where(x_inside, part, 0.0) for part in flux]
                    change[q] = [flux[c] - flux_carry[q * 4 + c] for c in range(4)]
                    new_flux += flux
                if cot_get is not None:
                    cot = [
                        jnp.where(x_inside, ahead_scaled[q][c] - scaled[q][c], 0.0) for c in range(4)
                    ]
                    left, right = flux_pull(here[q], ahead[q], 0, inverse[q], ahead_inv[q], cot)
                    back[q] = [back[q][c] + left[c] + cot_carry[q * 4 + c] for c in range(4)]
                    new_cot += right
            for normal, step, inside in ((1, E, y_inside), (2, 1, [z_inside, z_inside])):
                turned = [self.shifted([here[q][c] for q in range(2)], -step) for c in range(4)]
                turned_inv = self.shifted(inverse, -step)
                beyond = [[turned[c][q] for c in range(4)] for q in range(2)]
                if forward_put is not None:
                    flux = []
                    for q in range(2):
                        got = flux_of(here[q], beyond[q], normal, inverse[q], turned_inv[q])
                        flux.append([jnp.where(inside[q], part, 0.0) for part in got])
                    for c in range(4):
                        behind = self.shifted([flux[q][c] for q in range(2)], step)
                        for q in range(2):
                            change[q][c] = change[q][c] + (flux[q][c] - behind[q])
                if cot_get is not None:
                    turned_w = [self.shifted([scaled[q][c] for q in range(2)], -step) for c in range(4)]
                    rights = []
                    for q in range(2):
                        cot = [
                            jnp.where(inside[q], turned_w[c][q] - scaled[q][c], 0.0) for c in range(4)
                        ]
                        left, right = flux_pull(here[q], beyond[q], normal, inverse[q], turned_inv[q], cot)
                        back[q] = [back[q][c] + left[c] for c in range(4)]
                        rights.append(right)
                    for c in range(4):
                        moved = self.shifted([rights[q][c] for q in range(2)], step)
                        for q in range(2):
                            back[q][c] = back[q][c] + moved[q]
            for q in range(2):
                for c in range(4):
                    if forward_put is not None:
                        forward_put(q, row_of(x, c), here[q][c] - ratio * change[q][c])
                    if cot_get is not None:
                        cot_put(q, row_of(x, c), back[q][c])
            return (new_flux, new_cot)

        get_c = cot_get
        start = (
            [zero] * 8 if forward_put is not None else [],
            [zero] * 8 if cot_get is not None else [],
        )
        lax.fori_loop(0, E, one, start)


def run(body, name, scalars, arrays, outs, scratch, aliases=None):
    specs = [pl.BlockSpec(memory_space=pltpu.SMEM) for _ in scalars]
    operands = list(scalars)
    for item in arrays:
        if isinstance(item, tuple):
            specs.append(pl.BlockSpec(memory_space=pl.ANY))
            operands.append(item[0])
        else:
            specs.append(pl.BlockSpec(memory_space=pltpu.VMEM))
            operands.append(item)
    out_specs = [
        pl.BlockSpec(memory_space=pl.ANY if native else pltpu.VMEM) for shape, native in outs
    ]
    return pl.pallas_call(
        body,
        name=name,
        in_specs=specs,
        out_specs=out_specs,
        out_shape=[jax.ShapeDtypeStruct(shape, f32) for shape, native in outs],
        scratch_shapes=scratch,
        input_output_aliases=aliases or {},
        compiler_params=pltpu.CompilerParams(vmem_limit_bytes=24 * 1024 * 1024),
    )(*operands)


def native_copies(planes, whole, sems, inward, rows=None):
    lanes = planes[0].shape[1]
    copies = []
    for q in range(2):
        part = whole.at[:, pl.ds(q * lanes, lanes)]
        near = planes[q]
        if rows is not None:
            part = whole.at[pl.ds(*rows), pl.ds(q * lanes, lanes)]
            near = planes[q].at[pl.ds(*rows), :]
        source, target = (part, near) if inward else (near, part)
        copies.append(pltpu.make_async_copy(source, target, sems.at[q]))
    return copies


def boundary_fluxes(plan, layers, ghost, emit):
    for f in range(6):
        result = []
        for q in range(2):
            inner = [layers(q, f, c) for c in range(4)]
            outer = [ghost(q, f, c) for c in range(4)]
            inner_inv, outer_inv = 1.0 / inner[0], 1.0 / outer[0]
            if f % 2 == 0:
                result.append(flux_of(outer, inner, f // 2, outer_inv, inner_inv))
            else:
                result.append(flux_of(inner, outer, f // 2, inner_inv, outer_inv))
        for c in range(4):
            emit(f, c, [result[q][c] for q in range(2)])


def boundary_pull(plan, layers, ghost, cot, emit):
    for f in range(6):
        result = []
        for q in range(2):
            inner = [layers(q, f, c) for c in range(4)]
            outer = [ghost(q, f, c) for c in range(4)]
            weight = [cot(q, f, c) for c in range(4)]
            inner_inv, outer_inv = 1.0 / inner[0], 1.0 / outer[0]
            if f % 2 == 0:
                out_cot, in_cot = flux_pull(outer, inner, f // 2, outer_inv, inner_inv, weight)
            else:
                in_cot, out_cot = flux_pull(inner, outer, f // 2, inner_inv, outer_inv, weight)
            result.append((in_cot, out_cot))
        for c in range(4):
            emit(f, c, [result[q][0][c] for q in range(2)], [result[q][1][c] for q in range(2)])


def on_device(fields, guidance, levels, send_faces, ghost_peer, ghost_code, child_send, parent_peer):
    slots, _, extent, square = fields.shape
    peers = send_faces.shape[1]
    plan = Plan(slots, extent, peers)
    S, E, COL = slots, extent, plan.COL
    half_np = half_map(extent)
    half = jnp.asarray(half_np, bf16)
    half_back = jnp.asarray(np.ascontiguousarray(half_np.T), bf16)

    first_map, second_map = ghost_code // 5, ghost_code % 5
    turned = (jnp.arange(6) >= 4)[None, :, None]
    major = jnp.where(turned, second_map, first_map)
    minor = jnp.where(turned, first_map, second_map)
    refined = ghost_peer[:, :, 1] >= 0
    quarter = (major - 3) * 2 + (minor - 3)
    chosen = jnp.maximum(ghost_peer, 0)
    columns = [
        jnp.where(refined, jnp.sum(jnp.where(quarter == k, chosen, 0), axis=2), chosen[:, :, 0])
        for k in range(4)
    ]
    coarser = ghost_code[:, :, 0] > 0
    kind = jnp.where(
        ghost_peer[:, :, 0] < 0, 3, jnp.where(refined, 2, jnp.where(coarser, 1, 0))
    )
    single = jnp.logical_and(coarser, jnp.logical_not(refined))
    columns += [
        kind,
        jnp.where(single, major[:, :, 0] - 1, 0),
        jnp.where(single, minor[:, :, 0] - 1, 0),
        jnp.zeros_like(kind),
    ]
    table = jnp.stack(columns, axis=-1).astype(jnp.int32).reshape(-1)
    send = send_faces.reshape(peers, 6)
    children = child_send.reshape(-1)
    parents = parent_peer
    native_fields = fields.reshape(plan.native)
    native_guidance = guidance.reshape(plan.native)

    def exchange(packets):
        return lax.all_to_all(packets, "blk", split_axis=0, concat_axis=0, tiled=True)

    def vm(*shape):
        return pltpu.VMEM(shape, f32)

    def occupied_of(levels_ref):
        return plan.per_slot(lambda s: levels_ref[s]) >= 0

    fb_scratch = vm(*plan.fb)
    kind_scratch = pltpu.VMEM((3 * S * 8, COL), jnp.int32)
    native_planes = [vm(S * 4 * E, COL), vm(S * 4 * E, COL)]
    pair_of_sems = pltpu.SemaphoreType.DMA((2,))
    quarter_sums = [vm(S * 16, COL) for _ in range(6)]
    face_sums = [vm(2, S * 8, COL) for _ in range(6)]
    signs = [1.0, -1.0, 1.0, -1.0, 1.0, -1.0]

    def layers_of(get, fb, ff):
        for c in range(4):
            faces = plan.extract(get, c)
            for f in range(6):
                for q in range(2):
                    if fb is not None:
                        fb[q, plan.fb_rows(f, c), :] = faces[f][q]
                    if ff is not None:
                        ff[q, (f * 4 + c) * S : (f * 4 + c + 1) * S, :] = faces[f][q]

    def corrected_cot_of(get, levels_ref, fb):
        ratio = plan.ratio(levels_ref)
        for c in range(4):
            faces = plan.extract(get, c)
            for f in range(6):
                for q in range(2):
                    fb[q, plan.fb_rows(f, c), :] = (signs[f] * ratio) * faces[f][q]

    def finished(partial, corr, levels_ref, put):
        ratio = plan.ratio(levels_ref)
        occupied = ratio > 0.0
        get = plan.slab_at(partial)

        def face(q, f, c):
            value = corr[q, plan.fb_rows(f, c), :]
            return jnp.where(occupied, (signs[f] * ratio) * value, 0.0)

        for x in range(E):
            for c in range(4):
                for q in range(2):
                    put(q, x, c, get(q, x, c) + plan.spread(face, q, x, c))

    def ghost_reader(gb, layers, levels_ref):
        occupied = occupied_of(levels_ref)
        return lambda q, f, c: jnp.where(
            occupied, gb[q, plan.fb_rows(f, c, True), :], layers(q, f, c)
        )

    def slab_put(ref):
        def put(q, x, c, value):
            ref[q, (x * 4 + c) * S : (x * 4 + c + 1) * S, :] = value

        return put

    def dyn_get(ref):
        return lambda q, rows: ref[q, rows, :]

    def dyn_put(ref):
        def put(q, rows, value):
            ref[q, rows, :] = value

        return put

    ghost_scratch = [vm(8, 3 * S * 8, COL), vm(3 * S * 8, COL), kind_scratch]

    def flux_cot_of(recv, row0, cot_fb, table_s, send_s, sums, kinds, flux_cot, back_r):
        for s in range(S):
            for f in range(6):
                row = ((f // 2) * S + s) * 8 + (f % 2) * 4
                kinds[row : row + 4, :] = jnp.full((4, COL), table_s[(s * 6 + f) * 8 + 4], jnp.int32)

        def face_out(f, c, wide):
            keep = kinds[plan.fb_rows(f, c), :] != 2
            for q in range(2):
                own = jnp.where(keep, cot_fb[q, plan.fb_rows(f, c), :], 0.0)
                flux_cot[q, (f * 4 + c) * S : (f * 4 + c + 1) * S, :] = own + wide[q]

        plan.take_quarters(recv, row0, send_s, sums, face_out, back_r)

    def flux_emitter(b_fb, ff):
        def emit(f, c, values):
            for q in range(2):
                b_fb[q, plan.fb_rows(f, c), :] = values[q]
                ff[q, (f * 4 + c) * S : (f * 4 + c + 1) * S, :] = values[q]

        return emit

    def cot_emitter(layer_cot, gcot):
        def emit(f, c, inner, outer):
            for q in range(2):
                layer_cot[q, (f * 4 + c) * S : (f * 4 + c + 1) * S, :] = inner[q]
                gcot[q, plan.fb_rows(f, c, True), :] = outer[q]

        return emit

    def carry_packets(source, out, row0):
        def one(peer, carry):
            out[peer, row0 : row0 + 16, :] = source[peer, :, :]
            return carry

        lax.fori_loop(0, peers, one, 0)

    def add_layers(through, layer_cot, total, sums, put):
        own = plan.ff_at(layer_cot)
        for f in range(6):
            for c in range(4):
                for q in range(2):
                    added = sums[f][q, pl.ds((f % 2) * 4 + c, S, stride=8), :]
                    total[q, (f * 4 + c) * S : (f * 4 + c + 1) * S, :] = own(q, f, c) + added
        get = plan.slab_at(through)
        summed = plan.ff_at(total)
        for x in range(E):
            for c in range(4):
                for q in range(2):
                    put(q, x, c, get(q, x, c) + plan.spread(summed, q, x, c))

    def first_pack(send_s, parents_s, fields_r, guide_r, volume, layers, packets, fb, f0, f1, g0,
                   g1, f_sems, g_sems):
        inward = native_copies([f0, f1], fields_r, f_sems, True)
        guided = native_copies([g0, g1], guide_r, g_sems, True)
        for copy in inward + guided:
            copy.start()
        for copy in inward:
            copy.wait()
        get = plan.native_at([f0, f1])
        for x in range(E):
            for c in range(4):
                for q in range(2):
                    volume[q, (x * 4 + c) * S : (x * 4 + c + 1) * S, :] = get(q, x, c)
        layers_of(plan.slab_at(volume), fb, layers)
        plan.pack_faces(fb, send_s, packets)
        for copy in guided:
            copy.wait()
        planes = [g0, g1]
        plan.pack_octants(lambda s, x, q: planes[q][plan.native_rows(s, x), :], parents_s, packets, 48)

    volume1, layers1, packets = run(
        first_pack,
        "first_pack",
        [send, parents],
        [(native_fields,), (native_guidance,)],
        [(plan.slab, False), (plan.ff, False), ((peers, 64, COL), False)],
        [fb_scratch] + native_planes + native_planes + [pair_of_sems, pair_of_sems],
    )
    received1 = exchange(packets)

    def interior_first(levels_s, volume, partial):
        plan.interior(dyn_get(volume), levels_s, dyn_put(partial))

    (partial1,) = run(interior_first, "interior_first", [levels], [volume1], [(plan.slab, False)], [])

    def first_flux(levels_s, send_s, table_s, layers, recv, half_r, back_r, gb, b_fb, packets,
                   planes, near, kinds, ff, rb):
        plan.ghosts(recv, table_s, planes, near, kinds, gb, half_r, back_r)
        layer = plan.ff_at(layers)
        boundary_fluxes(plan, layer, ghost_reader(gb, layer, levels_s), flux_emitter(b_fb, ff))
        plan.pack_averages(plan.ff_at(ff), rb, send_s, packets, 0, half_r)

    ghosts1, fluxes1, packets = run(
        first_flux,
        "first_flux",
        [levels, send, table],
        [layers1, received1, half, half_back],
        [(plan.fb, False), (plan.fb, False), ((peers, 16, COL), False)],
        ghost_scratch + [vm(*plan.ff), vm(*plan.coarse)],
    )
    received2 = exchange(packets)

    def upward_second(levels_s, table_s, children_s, parents_s, guide_r, recv, back_r, up, cot_fb,
                      packets, cc, g0, g1, sems):
        guided = native_copies([g0, g1], guide_r, sems, True)
        for copy in guided:
            copy.start()
        for copy in guided:
            copy.wait()
        plan.upward(recv, 48, cc, children_s, parents_s, plan.native_at([g0, g1]), slab_put(up), back_r)
        corrected_cot_of(plan.slab_at(up), levels_s, cot_fb)
        plan.pack_quarters(cot_fb, table_s, packets, 0)

    up2, corrcot2, quarters2 = run(
        upward_second,
        "upward_second",
        [levels, table, children, parents],
        [(native_guidance,), received1, half_back],
        [(plan.slab, False), (plan.fb, False), ((peers, 16, COL), False)],
        [vm((S + 1) * 16, COL)] + native_planes + [pair_of_sems],
    )

    def first_update(levels_s, table_s, children_s, partial, b_fb, recv, quarters, half_r, updated,
                     packets, corr, cb):
        plan.corrected(b_fb, recv, 0, table_s, corr)
        finished(partial, corr, levels_s, slab_put(updated))
        plan.average_blocks(plan.slab_at(updated), cb, half_r)
        plan.pack_children(cb, children_s, packets, 0)
        carry_packets(quarters, packets, 16)

    updated1, packets = run(
        first_update,
        "first_update",
        [levels, table, children],
        [partial1, fluxes1, received2, quarters2, half],
        [(plan.slab, False), ((peers, 32, COL), False)],
        [fb_scratch, vm(*plan.coarse)],
    )
    received3 = exchange(packets)

    def middle_pack(send_s, parents_s, updated, recv, volume, layers, packets, fb):
        volume[...] = updated[...]

        def store(s, x, q, value):
            volume[q, plan.slab_rows(s, x), :] = value

        plan.place_octants(recv, 0, parents_s, store)
        layers_of(plan.slab_at(volume), fb, layers)
        plan.pack_faces(fb, send_s, packets)

    volume2, layers2, packets = run(
        middle_pack,
        "middle_pack",
        [send, parents],
        [updated1, received3],
        [(plan.slab, False), (plan.ff, False), ((peers, 48, COL), False)],
        [fb_scratch],
    )
    received4 = exchange(packets)

    def flux_cot_second(send_s, table_s, cot_fb, recv, back_r, flux_cot, kinds, *sums):
        flux_cot_of(recv, 16, cot_fb, table_s, send_s, sums, kinds, flux_cot, back_r)

    (fluxcot2,) = run(
        flux_cot_second,
        "flux_cot_second",
        [send, table],
        [corrcot2, received3, half_back],
        [(plan.ff, False)],
        [kind_scratch] + quarter_sums,
    )

    def interior_both(levels_s, volume, cot, partial, through):
        plan.interior(dyn_get(volume), levels_s, dyn_put(partial), dyn_get(cot), dyn_put(through))

    partial2, through2 = run(
        interior_both, "interior_both", [levels], [volume2, up2],
        [(plan.slab, False), (plan.slab, False)], [],
    )

    def second_pull(levels_s, table_s, layers, recv, flux_cot, half_r, back_r, gb, layer_cot,
                    packets, planes, near, kinds, gcot):
        plan.ghosts(recv, table_s, planes, near, kinds, gb, half_r, back_r)
        layer = plan.ff_at(layers)
        boundary_pull(
            plan, layer, ghost_reader(gb, layer, levels_s), plan.ff_at(flux_cot),
            cot_emitter(layer_cot, gcot),
        )
        plan.pack_ghost_cot(gcot, table_s, planes, near, packets, half_r, back_r)

    ghosts2, layercot2, packets = run(
        second_pull,
        "second_pull",
        [levels, table],
        [layers2, received4, fluxcot2, half, half_back],
        [(plan.fb, False), (plan.ff, False), ((peers, 48, COL), False)],
        ghost_scratch + [fb_scratch],
    )
    received5 = exchange(packets)

    def second_flux(levels_s, send_s, layers, gb, half_r, b_fb, packets, ff, rb):
        layer = plan.ff_at(layers)
        boundary_fluxes(plan, layer, ghost_reader(gb, layer, levels_s), flux_emitter(b_fb, ff))
        plan.pack_averages(plan.ff_at(ff), rb, send_s, packets, 0, half_r)

    fluxes2, averages2 = run(
        second_flux,
        "second_flux",
        [levels, send],
        [layers2, ghosts2, half],
        [(plan.fb, False), ((peers, 16, COL), False)],
        [vm(*plan.ff), vm(*plan.coarse)],
    )

    def middle_cot(send_s, parents_s, through, layer_cot, recv, averages, inner, packets, total, *sums):
        plan.take_faces(recv, send_s, sums)
        add_layers(through, layer_cot, total, sums, slab_put(inner))
        plan.pack_octants(
            lambda s, x, q: inner[q, plan.slab_rows(s, x), :], parents_s, packets, 0
        )
        carry_packets(averages, packets, 16)

    inner_cot, packets = run(
        middle_cot,
        "middle_cot",
        [send, parents],
        [through2, layercot2, received5, averages2],
        [(plan.slab, False), ((peers, 32, COL), False)],
        [vm(*plan.ff)] + face_sums,
    )
    received6 = exchange(packets)

    def upward_first(levels_s, table_s, children_s, parents_s, inner, recv, back_r, up, cot_fb,
                     packets, cc):
        plan.upward(recv, 0, cc, children_s, parents_s, plan.slab_at(inner), slab_put(up), back_r)
        corrected_cot_of(plan.slab_at(up), levels_s, cot_fb)
        plan.pack_quarters(cot_fb, table_s, packets, 0)

    up1, corrcot1, packets = run(
        upward_first,
        "upward_first",
        [levels, table, children, parents],
        [inner_cot, received6, half_back],
        [(plan.slab, False), (plan.fb, False), ((peers, 16, COL), False)],
        [vm((S + 1) * 16, COL)],
    )
    received7 = exchange(packets)

    def second_update(levels_s, table_s, partial, b_fb, recv, half_r, final, cb, corr, updated, n0,
                      n1, sems):
        plan.corrected(b_fb, recv, 16, table_s, corr)
        planes = [n0, n1]
        put_slab = slab_put(updated)

        def put(q, x, c, value):
            put_slab(q, x, c, value)
            planes[q][pl.ds(c * E + x, S, stride=4 * E), :] = value

        finished(partial, corr, levels_s, put)
        copies = native_copies(planes, final, sems, False)
        for copy in copies:
            copy.start()
        plan.average_blocks(plan.slab_at(updated), cb, half_r)
        for copy in copies:
            copy.wait()

    final_open, coarse2 = run(
        second_update,
        "second_update",
        [levels, table],
        [partial2, fluxes2, received6, half],
        [(plan.native, True), (plan.coarse, False)],
        [fb_scratch, vm(*plan.slab)] + native_planes + [pair_of_sems],
    )

    def interior_back(levels_s, volume, cot, through):
        plan.interior(dyn_get(volume), levels_s, None, dyn_get(cot), dyn_put(through))

    (through1,) = run(
        interior_back, "interior_back", [levels], [volume1, up1], [(plan.slab, False)], []
    )

    def first_pull(levels_s, send_s, table_s, children_s, layers, gb, cot_fb, recv, coarse, half_r,
                   back_r, layer_cot, packets, planes, near, kinds, flux_cot, gcot, *sums):
        plan.pack_children(coarse, children_s, packets, 48)
        flux_cot_of(recv, 0, cot_fb, table_s, send_s, sums, kinds, flux_cot, back_r)
        layer = plan.ff_at(layers)
        boundary_pull(
            plan, layer, ghost_reader(gb, layer, levels_s), plan.ff_at(flux_cot),
            cot_emitter(layer_cot, gcot),
        )
        plan.pack_ghost_cot(gcot, table_s, planes, near, packets, half_r, back_r)

    layercot1, packets = run(
        first_pull,
        "first_pull",
        [levels, send, table, children],
        [layers1, ghosts1, corrcot1, received7, coarse2, half, half_back],
        [(plan.ff, False), ((peers, 64, COL), False)],
        ghost_scratch + [vm(*plan.ff), fb_scratch] + quarter_sums,
    )
    received8 = exchange(packets)

    def last_cot(send_s, parents_s, through, layer_cot, recv, open_r, gradient, final, total, n0, n1,
                 p0, p1, sems, *late):
        del open_r
        slot_sems, sums = late[0], late[1:]
        placed = [p0, p1]

        def store(s, x, q, value):
            placed[q][plan.native_rows(s, x), :] = value

        plan.place_octants(recv, 48, parents_s, store)

        def each_covered(act):
            for s in range(S):

                def one(s=s):
                    rows = (s * 4 * E, 4 * E)
                    for copy in native_copies(placed, final, slot_sems.at[s], False, rows):
                        act(copy)

                pl.when(parents_s[s, 0] >= 0)(one)

        each_covered(lambda copy: copy.start())
        plan.take_faces(recv, send_s, sums)
        planes = [n0, n1]

        def put(q, x, c, value):
            planes[q][pl.ds(c * E + x, S, stride=4 * E), :] = value

        add_layers(through, layer_cot, total, sums, put)
        copies = native_copies(planes, gradient, sems, False)
        for copy in copies:
            copy.start()
        for copy in copies:
            copy.wait()
        each_covered(lambda copy: copy.wait())

    gradient, final_fields = run(
        last_cot,
        "last_cot",
        [send, parents],
        [through1, layercot1, received8, (final_open,)],
        [(plan.native, True), (plan.native, True)],
        [vm(*plan.ff)] + native_planes + native_planes
        + [pair_of_sems, pltpu.SemaphoreType.DMA((S, 2))] + face_sums,
        aliases={5: 1},
    )
    return (final_fields.reshape(fields.shape), gradient.reshape(fields.shape))


def solution(mesh):
    placed = (
        P("blk", None, None, None),
        P("blk", None, None, None),
        P("blk"),
        P("blk", None, None),
        P("blk", None, None),
        P("blk", None, None),
        P("blk", None),
        P("blk", None),
    )
    return jax.shard_map(
        on_device,
        mesh=mesh,
        in_specs=placed,
        out_specs=(P("blk", None, None, None), P("blk", None, None, None)),
        check_vma=False,
    )
```

```python
import jax
import jax.numpy as jnp
import numpy as np
from jax import lax
from jax.experimental import pallas as pl
from jax.experimental.pallas import tpu as pltpu
from jax.sharding import PartitionSpec as P

sound_speed = 1.0
base_ratio = 0.04
speed_floor = 0.01
f32 = jnp.float32
bf16 = jnp.bfloat16


def half_map(extent):
    half = extent // 2
    square = extent * extent
    table = np.zeros((2, extent, extent, half, 2, half), np.float32)
    for group in range(2):
        for i in range(extent):
            for j in range(extent):
                table[group, i, j, i // 2, group, j // 2] = 0.25
    return table.reshape(2 * square, square // 2)


def dot2(values, table):
    high = values.astype(bf16)
    low = (values - high.astype(f32)).astype(bf16)
    return jnp.dot(high, table, preferred_element_type=f32) + jnp.dot(
        low, table, preferred_element_type=f32
    )


def roll(values, shift):
    lanes = values.shape[1]
    shift = shift % lanes
    return values if shift == 0 else pltpu.roll(values, shift, 1)


def flux_of(behind, beyond, normal, inv_behind, inv_beyond):
    v = behind[1 + normal] * inv_behind
    w = beyond[1 + normal] * inv_beyond
    c = sound_speed + jnp.sqrt(0.5 * (v * v + w * w) + speed_floor)
    result = [0.5 * ((behind[1 + normal] + beyond[1 + normal]) - c * (beyond[0] - behind[0]))]
    for k in range(1, 4):
        total = behind[k] * v + beyond[k] * w
        if k == 1 + normal:
            total = total + (sound_speed * sound_speed) * (behind[0] + beyond[0])
        result.append(0.5 * (total - c * (beyond[k] - behind[k])))
    return result


def flux_pull(behind, beyond, normal, inv_behind, inv_beyond, cot):
    v = behind[1 + normal] * inv_behind
    w = beyond[1 + normal] * inv_beyond
    inside = 0.5 * (v * v + w * w) + speed_floor
    root = jnp.sqrt(inside)
    c = sound_speed + root
    half_cot = [0.5 * part for part in cot]
    jump = half_cot[0] * (beyond[0] - behind[0])
    v_cot = half_cot[1] * behind[1]
    w_cot = half_cot[1] * beyond[1]
    for k in range(1, 4):
        jump = jump + half_cot[k] * (beyond[k] - behind[k])
        if k > 1:
            v_cot = v_cot + half_cot[k] * behind[k]
            w_cot = w_cot + half_cot[k] * beyond[k]
    scale = jump * (-0.5) / root
    v_cot = (v_cot + scale * v) * inv_behind
    w_cot = (w_cot + scale * w) * inv_beyond
    plus = v + c
    minus = w - c
    behind_cot = []
    beyond_cot = []
    pressure = (sound_speed * sound_speed) * half_cot[1 + normal]
    for k in range(4):
        if k == 0:
            behind_cot.append(c * half_cot[0] + pressure - v_cot * v)
            beyond_cot.append(pressure - c * half_cot[0] - w_cot * w)
        else:
            left = half_cot[k] * plus
            right = half_cot[k] * minus
            if k == 1 + normal:
                left = left + half_cot[0] + v_cot
                right = right + half_cot[0] + w_cot
            behind_cot.append(left)
            beyond_cot.append(right)
    return behind_cot, beyond_cot


class Plan:
    def __init__(self, slots, extent, peers):
        self.S = slots
        self.E = extent
        self.P = peers
        self.H = extent // 2
        self.COL = extent * extent // 2
        self.slab = (2, extent * 4 * slots, self.COL)
        self.ff = (2, 6 * 4 * slots, self.COL)
        self.fb = (2, 3 * slots * 8, self.COL)
        self.native = (slots * 4 * extent, 2 * self.COL)
        self.coarse = (slots * 16, self.COL)

    def lane(self, rows):
        return lax.broadcasted_iota(jnp.int32, (rows, self.COL), 1)

    def low(self, rows):
        return (self.lane(rows) & (self.E - 1)) < self.H

    def per_slot(self, scalar_of):
        sub = lax.broadcasted_iota(jnp.int32, (self.S, self.COL), 0)
        value = jnp.zeros((self.S, self.COL), jnp.int32)
        for s in range(self.S):
            value = jnp.where(sub == s, scalar_of(s), value)
        return value

    def ratio(self, levels):
        level = self.per_slot(lambda s: levels[s])
        degree = level.astype(f32)
        ratio = base_ratio * (1.0 + degree + 0.5 * degree * (degree - 1.0))
        return jnp.where(level >= 0, ratio, 0.0)

    def slab_at(self, ref):
        return lambda q, x, c: ref[q, (x * 4 + c) * self.S : (x * 4 + c + 1) * self.S, :]

    def native_at(self, planes):
        step = 4 * self.E
        return lambda q, x, c: planes[q][pl.ds(c * self.E + x, self.S, stride=step), :]

    def ff_at(self, ref):
        return lambda q, f, c: ref[q, (f * 4 + c) * self.S : (f * 4 + c + 1) * self.S, :]

    def fb_rows(self, f, c, swapped=False):
        side = f % 2
        half = 1 - side if swapped else side
        return pl.ds((f // 2) * self.S * 8 + half * 4 + c, self.S, stride=8)

    def extract(self, get, c):
        E, H, COL = self.E, self.H, self.COL
        lane = self.lane(self.S)
        group = lax.shift_right_logical(lane, E.bit_length() - 1)
        within = lane & (E - 1)
        faces = [[get(q, 0, c) for q in range(2)], [get(q, E - 1, c) for q in range(2)]]
        low_y, high_y, low_z, high_z = [], [], [], []
        for q in range(2):
            first, last, near, far = None, None, None, None
            for k in range(H):
                a = roll(get(0, q * H + k, c), E * k)
                b = roll(get(1, q * H + k, c), E * k - (COL - E))
                first = a if first is None else jnp.where(group == k, a, first)
                last = b if last is None else jnp.where(group == k, b, last)
            for x in range(E):
                source = get(q, x, c)
                a = roll(source, x)
                b = roll(source, x - (E - 1))
                near = a if near is None else jnp.where(within == x, a, near)
                far = b if far is None else jnp.where(within == x, b, far)
            low_y.append(first)
            high_y.append(last)
            low_z.append(near)
            high_z.append(far)
        return faces + [low_y, high_y, low_z, high_z]

    def spread(self, face, q, x, c):
        E, H, COL = self.E, self.H, self.COL
        lane = self.lane(self.S)
        within = lane & (E - 1)
        k = x % H
        y_face = face(x // H, 2 + q, c)
        if q == 0:
            total = jnp.where(lane < E, roll(y_face, -E * k), 0.0)
        else:
            total = jnp.where(lane >= COL - E, roll(y_face, (COL - E) - E * k), 0.0)
        near = roll(face(q, 4, c), -x)
        far = roll(face(q, 5, c), E - 1 - x)
        total = total + jnp.where(within == 0, near, jnp.where(within == E - 1, far, 0.0))
        if x == 0:
            total = total + face(q, 0, c)
        if x == E - 1:
            total = total + face(q, 1, c)
        return total

    def pack_faces(self, fb, send, out):
        sub = lax.broadcasted_iota(jnp.int32, (8, self.COL), 0)
        for axis in range(3):

            def one(peer, carry, axis=axis):
                slots = [jnp.maximum(send[peer, axis * 2 + side], 0) for side in range(2)]
                for q in range(2):
                    lo, hi = [
                        fb[q, pl.ds(pl.multiple_of((axis * self.S + slot) * 8, 8), 8), :]
                        for slot in slots
                    ]
                    row = axis * 16 + q * 8
                    out.ref[peer, row : row + 8, :] = jnp.where(sub < 4, lo, hi)
                return carry

            lax.fori_loop(0, self.P, one, 0, unroll=4)
            out.send(axis * 16, 16)

    def take_faces(self, packets, send, sums):
        def one(peer, carry):
            for f in range(6):
                slot = jnp.maximum(send[peer, f], 0)
                rows = pl.ds(pl.multiple_of(slot * 8, 8), 8)
                for q in range(2):
                    at = (f // 2) * 16 + q * 8
                    sums[f][q, rows, :] += packets[peer, at : at + 8, :]
            return carry

        for f in range(6):
            sums[f][...] = jnp.zeros(sums[f].shape, f32)
        lax.fori_loop(0, self.P, one, 0)

    def pack_averages(self, face, rb, send, out, row0, half):
        S, COL = self.S, self.COL
        rows = []
        for axis in range(3):
            for c in range(4):
                rows.append(
                    jnp.concatenate(
                        [face(q, 2 * axis + side, c) for side in range(2) for q in range(2)], axis=1
                    )
                )
        small = dot2(jnp.concatenate(rows, axis=0), half[...])
        for k in range(12):
            rb[pl.ds(k, S, stride=16), :] = small[k * S : (k + 1) * S]
        zero = jnp.zeros((S, COL), f32)
        for k in range(12, 16):
            rb[pl.ds(k, S, stride=16), :] = zero
        sub = lax.broadcasted_iota(jnp.int32, (8, COL), 0)
        low = self.low(8)

        def one(peer, carry):
            def part(f, at):
                slot = jnp.maximum(send[peer, f], 0)
                return rb[pl.ds(pl.multiple_of(slot * 16 + at, 8), 8), :]

            first = jnp.where(low, part(0, 0), part(1, 0))
            second = jnp.where(low, part(2, 0), part(3, 0))
            out[peer, row0 : row0 + 8, :] = jnp.where(sub < 4, first, second)
            out[peer, row0 + 8 : row0 + 16, :] = jnp.where(low, part(4, 8), part(5, 8))
            return carry

        lax.fori_loop(0, self.P, one, 0)

    def pack_quarters(self, fb, table, out, row0):
        E, H = self.E, self.H
        low = self.low(4)

        def clear(peer, carry):
            out[peer, row0 : row0 + 16, :] = jnp.zeros((16, self.COL), f32)
            return carry

        lax.fori_loop(0, self.P, clear, 0)
        for s in range(self.S):
            for f in range(6):
                base = (s * 6 + f) * 8

                def send_quarters(s=s, f=f, base=base):
                    axis, side = f // 2, f % 2
                    keep = low if side == 1 else jnp.logical_not(low)
                    row = (axis * self.S + s) * 8 + side * 4
                    at = row0 + axis * 4
                    for h in range(2):
                        values = fb[h, row : row + 4, :]
                        for g in range(2):
                            moved = roll(values, H * ((1 - side) - g))
                            peer = table[base + h * 2 + g]
                            out[peer, at : at + 4, :] += jnp.where(keep, moved, 0.0)

                pl.when(table[base + 4] == 2)(send_quarters)

    def take_quarters(self, packets, row0, send, sums, face_out, half_back):
        S, COL = self.S, self.COL

        def one(peer, carry):
            block = packets[peer, row0 : row0 + 16, :]
            for f in range(6):
                slot = jnp.maximum(send[peer, f], 0)
                rows = pl.ds(pl.multiple_of(slot * 16, 8), 16)
                sums[f][rows, :] += block
            return carry

        for f in range(6):
            sums[f][...] = jnp.zeros(sums[f].shape, f32)
        lax.fori_loop(0, self.P, one, 0)
        for f in range(6):
            axis, side = f // 2, f % 2
            rows = jnp.concatenate(
                [sums[f][pl.ds(axis * 4 + c, S, stride=16), :] for c in range(4)], axis=0
            )
            wide = dot2(rows, half_back[:, side * 2 * COL : (side + 1) * 2 * COL])
            for c in range(4):
                face_out(f, c, [wide[c * S : (c + 1) * S, q * COL : (q + 1) * COL] for q in range(2)])

    def ghosts(self, packets, table, planes, near, kinds, gb, half, half_back):
        S, COL, H = self.S, self.COL, self.H
        for s in range(S):
            for f in range(6):
                base = (s * 6 + f) * 8
                axis, half_row = f // 2, (1 - f % 2) * 4
                row = (axis * S + s) * 8 + half_row
                first = None
                for k in range(4):
                    peer = table[base + k]
                    got = []
                    for q in range(2):
                        at = axis * 16 + q * 8 + half_row
                        values = packets[peer, at : at + 4, :]
                        planes[k * 2 + q, row : row + 4, :] = values
                        got.append(values)
                    if k == 0:
                        first = got
                source = jnp.where(table[base + 5] == 1, first[1], first[0])
                source = jnp.where(table[base + 6] == 1, roll(source, -H), source)
                near[row : row + 4, :] = source
                kinds[row : row + 4, :] = jnp.full((4, COL), table[base + 4], jnp.int32)
        for axis in range(3):
            rows = slice(axis * S * 8, (axis + 1) * S * 8)
            kind = kinds[rows, :]
            coarse = 4.0 * dot2(near[rows, :], half_back[:, : 2 * COL])
            for h in range(2):
                parts = [planes[(h * 2 + g) * 2 + q, rows, :] for g in range(2) for q in range(2)]
                fine = dot2(jnp.concatenate(parts, axis=1), half[...])
                value = jnp.where(kind == 1, coarse[:, h * COL : (h + 1) * COL], planes[h, rows, :])
                gb[h, rows, :] = jnp.where(kind == 2, fine, value)

    def pack_ghost_cot(self, gb, table, wide, near, out, half, half_back):
        S, COL, H = self.S, self.COL, self.H
        low = self.low(4)

        def clear(peer, carry):
            out.ref[peer, 0:48, :] = jnp.zeros((48, COL), f32)
            return carry

        lax.fori_loop(0, self.P, clear, 0)
        for h in range(2):
            for g in range(2):
                spread = dot2(gb[h, :, :], half_back[:, g * 2 * COL : (g + 1) * 2 * COL])
                for q in range(2):
                    wide[(h * 2 + g) * 2 + q, :, :] = spread[:, q * COL : (q + 1) * COL]
        both = jnp.concatenate([gb[0, :, :], gb[1, :, :]], axis=1)
        near[...] = 4.0 * dot2(both, half[0 : 2 * COL, :])
        for f in range(6):
            for s in range(S):
                base = (s * 6 + f) * 8
                axis, half_row = f // 2, (1 - f % 2) * 4
                row = (axis * S + s) * 8 + half_row
                kind = table[base + 4]

                def same(base=base, axis=axis, half_row=half_row, row=row):
                    peer = table[base]
                    for q in range(2):
                        at = axis * 16 + q * 8 + half_row
                        out.ref[peer, at : at + 4, :] += gb[q, row : row + 4, :]

                def coarse(base=base, axis=axis, half_row=half_row, row=row):
                    peer = table[base]
                    values = near[row : row + 4, :]
                    values = jnp.where(table[base + 6] == 1, roll(values, H), values)
                    for q in range(2):
                        at = axis * 16 + q * 8 + half_row
                        out.ref[peer, at : at + 4, :] += jnp.where(table[base + 5] == q, values, 0.0)

                def fine(base=base, axis=axis, half_row=half_row, row=row):
                    for k in range(4):
                        peer = table[base + k]
                        for q in range(2):
                            at = axis * 16 + q * 8 + half_row
                            out.ref[peer, at : at + 4, :] += wide[k * 2 + q, row : row + 4, :]

                pl.when(kind == 0)(same)
                pl.when(kind == 1)(coarse)
                pl.when(kind == 2)(fine)
            if f % 2 == 1:
                out.send((f // 2) * 16, 16)

    def corrected(self, b_fb, packets, row0, table, out):
        H = self.H
        low = self.low(4)
        out[...] = b_fb[...]
        for s in range(self.S):
            for f in range(6):
                base = (s * 6 + f) * 8

                def replace(s=s, f=f, base=base):
                    axis, side = f // 2, f % 2
                    row = (axis * self.S + s) * 8 + side * 4
                    at = row0 + axis * 4
                    for h in range(2):
                        got = []
                        for g in range(2):
                            values = packets[table[base + h * 2 + g], at : at + 4, :]
                            got.append(roll(values, H * (g - (1 - side))))
                        out[h, row : row + 4, :] = jnp.where(low, got[0], got[1])

                pl.when(table[base + 4] == 2)(replace)

    def pack_octants(self, load, parents, out, row0):
        H = self.H
        low = self.low(4)
        for s in range(self.S):

            def send(s=s):
                for ox in range(2):
                    for oy in range(2):
                        peers = [parents[s, ox * 4 + oy * 2 + oz] for oz in range(2)]
                        for pair in range(H // 2):
                            x = ox * H + pair * 2
                            first, second = load(s, x, oy), load(s, x + 1, oy)
                            at = row0 + pair * 4
                            out[peers[0], at : at + 4, :] = jnp.where(low, first, roll(second, H))
                            out[peers[1], at : at + 4, :] = jnp.where(low, roll(first, -H), second)

            pl.when(parents[s, 0] >= 0)(send)

    def place_octants(self, packets, row0, parents, store):
        H = self.H
        low = self.low(4)
        for s in range(self.S):

            def place(s=s):
                for ox in range(2):
                    for oy in range(2):
                        peers = [parents[s, ox * 4 + oy * 2 + oz] for oz in range(2)]
                        for pair in range(H // 2):
                            x = ox * H + pair * 2
                            at = row0 + pair * 4
                            first = packets[peers[0], at : at + 4, :]
                            second = packets[peers[1], at : at + 4, :]
                            store(s, x, oy, jnp.where(low, first, roll(second, H)))
                            store(s, x + 1, oy, jnp.where(low, roll(first, -H), second))

            pl.when(parents[s, 0] >= 0)(place)

    def slab_rows(self, s, x):
        return pl.ds(x * 4 * self.S + s, 4, stride=self.S)

    def native_rows(self, s, x):
        return pl.ds(s * 4 * self.E + x, 4, stride=self.E)

    def average_blocks(self, get, cb, half):
        S = self.S
        rows = []
        for pair in range(self.E // 4):
            for c in range(4):
                x = 4 * pair
                rows.append(
                    jnp.concatenate(
                        [get(q, x + 2 * a, c) + get(q, x + 2 * a + 1, c) for a in range(2) for q in range(2)],
                        axis=1,
                    )
                )
        small = 0.5 * dot2(jnp.concatenate(rows, axis=0), half[...])
        for k in range(16):
            cb[pl.ds(k, S, stride=16), :] = small[k * S : (k + 1) * S]

    def pack_children(self, cb, children, out, row0):
        def one(peer, carry):
            slot = jnp.maximum(children[peer], 0)
            out[peer, row0 : row0 + 16, :] = cb[pl.ds(pl.multiple_of(slot * 16, 8), 16), :]
            return carry

        lax.fori_loop(0, self.P, one, 0)

    def upward(self, packets, row0, cc, children, parents, get, put, half_back):
        S, COL = self.S, self.COL
        cc[...] = jnp.zeros(cc.shape, f32)

        def one(peer, carry):
            child = children[peer]
            slot = jnp.where(child < 0, S, child)
            rows = pl.ds(pl.multiple_of(slot * 16, 8), 16)
            cc[rows, :] += jnp.where(child < 0, 0.0, packets[peer, row0 : row0 + 16, :])
            return carry

        lax.fori_loop(0, self.P, one, 0)
        rows = jnp.concatenate([cc[pl.ds(k, S, stride=16), :] for k in range(16)], axis=0)
        wide = 0.5 * dot2(rows, half_back[...])
        covered = self.per_slot(lambda s: parents[s, 0]) >= 0
        for x in range(self.E):
            for c in range(4):
                row = ((x // 4) * 4 + c) * S
                for q in range(2):
                    lane0 = ((x // 2) % 2 * 2 + q) * COL
                    added = wide[row : row + S, lane0 : lane0 + COL]
                    put(q, x, c, jnp.where(covered, 0.0, get(q, x, c)) + added)

    def shifted(self, planes, amount):
        COL = self.COL
        lane = self.lane(self.S)
        moved = [roll(values, amount) for values in planes]
        if amount > 0:
            return [jnp.where(lane < amount, moved[1 - q], moved[q]) for q in range(2)]
        return [jnp.where(lane >= COL + amount, moved[1 - q], moved[q]) for q in range(2)]

    def interior(self, get, levels, forward_put, cot_get=None, cot_put=None):
        S, E, COL = self.S, self.E, self.COL
        ratio = self.ratio(levels)
        lane = self.lane(S)
        y_inside = [lane >= 0, lane < COL - E]
        z_inside = (lane & (E - 1)) != E - 1
        zero = jnp.zeros((S, COL), f32)

        def row_of(x, c):
            return pl.ds(pl.multiple_of((x * 4 + c) * S, S), S)

        def one(x, carry):
            after = jnp.minimum(x + 1, E - 1)
            x_inside = x < E - 1
            here = [[get(q, row_of(x, c)) for c in range(4)] for q in range(2)]
            inverse = [1.0 / here[q][0] for q in range(2)]
            ahead = [[get(q, row_of(after, c)) for c in range(4)] for q in range(2)]
            ahead_inv = [1.0 / ahead[q][0] for q in range(2)]
            flux_carry, cot_carry = carry
            new_flux, new_cot = [], []
            change = [[None] * 4 for _ in range(2)]
            if cot_get is not None:
                weight = [[get_c(q, row_of(x, c)) for c in range(4)] for q in range(2)]
                scaled = [[ratio * weight[q][c] for c in range(4)] for q in range(2)]
                ahead_scaled = [
                    [ratio * get_c(q, row_of(after, c)) for c in range(4)] for q in range(2)
                ]
                back = [[weight[q][c] for c in range(4)] for q in range(2)]
            for q in range(2):
                if forward_put is not None:
                    flux = flux_of(here[q], ahead[q], 0, inverse[q], ahead_inv[q])
                    flux = [jnp.where(x_inside, part, 0.0) for part in flux]
                    change[q] = [flux[c] - flux_carry[q * 4 + c] for c in range(4)]
                    new_flux += flux
                if cot_get is not None:
                    cot = [
                        jnp.where(x_inside, ahead_scaled[q][c] - scaled[q][c], 0.0) for c in range(4)
                    ]
                    left, right = flux_pull(here[q], ahead[q], 0, inverse[q], ahead_inv[q], cot)
                    back[q] = [back[q][c] + left[c] + cot_carry[q * 4 + c] for c in range(4)]
                    new_cot += right
            for normal, step, inside in ((1, E, y_inside), (2, 1, [z_inside, z_inside])):
                turned = [self.shifted([here[q][c] for q in range(2)], -step) for c in range(4)]
                turned_inv = self.shifted(inverse, -step)
                beyond = [[turned[c][q] for c in range(4)] for q in range(2)]
                if forward_put is not None:
                    flux = []
                    for q in range(2):
                        got = flux_of(here[q], beyond[q], normal, inverse[q], turned_inv[q])
                        flux.append([jnp.where(inside[q], part, 0.0) for part in got])
                    for c in range(4):
                        behind = self.shifted([flux[q][c] for q in range(2)], step)
                        for q in range(2):
                            change[q][c] = change[q][c] + (flux[q][c] - behind[q])
                if cot_get is not None:
                    turned_w = [self.shifted([scaled[q][c] for q in range(2)], -step) for c in range(4)]
                    rights = []
                    for q in range(2):
                        cot = [
                            jnp.where(inside[q], turned_w[c][q] - scaled[q][c], 0.0) for c in range(4)
                        ]
                        left, right = flux_pull(here[q], beyond[q], normal, inverse[q], turned_inv[q], cot)
                        back[q] = [back[q][c] + left[c] for c in range(4)]
                        rights.append(right)
                    for c in range(4):
                        moved = self.shifted([rights[q][c] for q in range(2)], step)
                        for q in range(2):
                            back[q][c] = back[q][c] + moved[q]
            for q in range(2):
                for c in range(4):
                    if forward_put is not None:
                        forward_put(q, row_of(x, c), here[q][c] - ratio * change[q][c])
                    if cot_get is not None:
                        cot_put(q, row_of(x, c), back[q][c])
            return (new_flux, new_cot)

        get_c = cot_get
        start = (
            [zero] * 8 if forward_put is not None else [],
            [zero] * 8 if cot_get is not None else [],
        )
        lax.fori_loop(0, E, one, start)


class Arriving:
    def __init__(self, copies, ref):
        self.copies = copies
        self.ref = ref
        for copy in copies:
            copy.start()

    def get(self):
        for copy in self.copies:
            copy.wait()
        self.copies = []
        return self.ref


class Leaving:
    def __init__(self, ref, target, sems):
        self.ref = ref
        self.target = target
        self.sems = sems
        self.copies = []

    def send(self, first=None, count=None):
        near, far = self.ref, self.target
        if count is not None:
            near = near.at[:, pl.ds(first, count), :]
            far = far.at[:, pl.ds(first, count), :]
        copy = pltpu.make_async_copy(near, far, self.sems.at[len(self.copies)])
        copy.start()
        self.copies.append(copy)

    def finish(self):
        for copy in self.copies:
            copy.wait()


class Late:
    def __init__(self, array, native=False, raw=False):
        self.array = array
        self.native = native
        self.raw = raw


def run(body, name, scalars, arrays, outs, scratch, aliases=None):
    hbm = pltpu.MemorySpace.HBM
    specs = [pl.BlockSpec(memory_space=pltpu.SMEM) for _ in scalars]
    operands = list(scalars)
    extra = []
    arriving, leaving = {}, {}
    for index, item in enumerate(arrays):
        if isinstance(item, Late):
            specs.append(pl.BlockSpec(memory_space=hbm))
            operands.append(pltpu.with_memory_space_constraint(item.array, hbm))
            if not item.raw:
                shape = item.array.shape
                arriving[index] = (len(extra), item.native)
                if item.native:
                    half = (shape[0], shape[1] // 2)
                    extra += [pltpu.VMEM(half, f32), pltpu.VMEM(half, f32)]
                    extra.append(pltpu.SemaphoreType.DMA((2,)))
                else:
                    extra += [pltpu.VMEM(shape, f32), pltpu.SemaphoreType.DMA((1,))]
        else:
            specs.append(pl.BlockSpec(memory_space=pltpu.VMEM))
            operands.append(item)
    out_specs = []
    for index, (shape, mode) in enumerate(outs):
        out_specs.append(pl.BlockSpec(memory_space=hbm if mode else pltpu.VMEM))
        if mode == "late":
            leaving[index] = len(extra)
            extra += [pltpu.VMEM(shape, f32), pltpu.SemaphoreType.DMA((4,))]

    def wrapped(*refs):
        n_scalar, n_in, n_out = len(scalars), len(arrays), len(outs)
        scalar_refs = list(refs[:n_scalar])
        in_refs = list(refs[n_scalar : n_scalar + n_in])
        out_refs = list(refs[n_scalar + n_in : n_scalar + n_in + n_out])
        rest = refs[n_scalar + n_in + n_out :]
        own, late = rest[: len(scratch)], rest[len(scratch) :]
        for index, (at, native) in arriving.items():
            if native:
                planes = [late[at], late[at + 1]]
                copies = native_copies(planes, in_refs[index], late[at + 2], True)
                in_refs[index] = Arriving(copies, planes)
            else:
                copy = pltpu.make_async_copy(in_refs[index], late[at], late[at + 1].at[0])
                in_refs[index] = Arriving([copy], late[at])
        for index, at in leaving.items():
            out_refs[index] = Leaving(late[at], out_refs[index], late[at + 1])
        body(*scalar_refs, *in_refs, *out_refs, *own)
        for index in arriving:
            in_refs[index].get()
        for index in leaving:
            out_refs[index].finish()

    return pl.pallas_call(
        wrapped,
        name=name,
        in_specs=specs,
        out_specs=out_specs,
        out_shape=[
            hbm(shape, f32) if mode else jax.ShapeDtypeStruct(shape, f32) for shape, mode in outs
        ],
        scratch_shapes=list(scratch) + extra,
        input_output_aliases=aliases or {},
        compiler_params=pltpu.CompilerParams(vmem_limit_bytes=32 * 1024 * 1024),
    )(*operands)


def native_copies(planes, whole, sems, inward, rows=None):
    lanes = planes[0].shape[1]
    copies = []
    for q in range(2):
        part = whole.at[:, pl.ds(q * lanes, lanes)]
        near = planes[q]
        if rows is not None:
            part = whole.at[pl.ds(*rows), pl.ds(q * lanes, lanes)]
            near = planes[q].at[pl.ds(*rows), :]
        source, target = (part, near) if inward else (near, part)
        copies.append(pltpu.make_async_copy(source, target, sems.at[q]))
    return copies


def boundary_fluxes(plan, layers, ghost, emit):
    for f in range(6):
        result = []
        for q in range(2):
            inner = [layers(q, f, c) for c in range(4)]
            outer = [ghost(q, f, c) for c in range(4)]
            inner_inv, outer_inv = 1.0 / inner[0], 1.0 / outer[0]
            if f % 2 == 0:
                result.append(flux_of(outer, inner, f // 2, outer_inv, inner_inv))
            else:
                result.append(flux_of(inner, outer, f // 2, inner_inv, outer_inv))
        for c in range(4):
            emit(f, c, [result[q][c] for q in range(2)])


def boundary_pull(plan, layers, ghost, cot, emit):
    for f in range(6):
        result = []
        for q in range(2):
            inner = [layers(q, f, c) for c in range(4)]
            outer = [ghost(q, f, c) for c in range(4)]
            weight = [cot(q, f, c) for c in range(4)]
            inner_inv, outer_inv = 1.0 / inner[0], 1.0 / outer[0]
            if f % 2 == 0:
                out_cot, in_cot = flux_pull(outer, inner, f // 2, outer_inv, inner_inv, weight)
            else:
                in_cot, out_cot = flux_pull(inner, outer, f // 2, inner_inv, outer_inv, weight)
            result.append((in_cot, out_cot))
        for c in range(4):
            emit(f, c, [result[q][0][c] for q in range(2)], [result[q][1][c] for q in range(2)])


def on_device(fields, guidance, levels, send_faces, ghost_peer, ghost_code, child_send, parent_peer):
    slots, _, extent, square = fields.shape
    peers = send_faces.shape[1]
    plan = Plan(slots, extent, peers)
    S, E, COL = slots, extent, plan.COL
    half_np = half_map(extent)
    half = jnp.asarray(half_np, bf16)
    half_back = jnp.asarray(np.ascontiguousarray(half_np.T), bf16)

    first_map, second_map = ghost_code // 5, ghost_code % 5
    turned = (jnp.arange(6) >= 4)[None, :, None]
    major = jnp.where(turned, second_map, first_map)
    minor = jnp.where(turned, first_map, second_map)
    refined = ghost_peer[:, :, 1] >= 0
    quarter = (major - 3) * 2 + (minor - 3)
    chosen = jnp.maximum(ghost_peer, 0)
    columns = [
        jnp.where(refined, jnp.sum(jnp.where(quarter == k, chosen, 0), axis=2), chosen[:, :, 0])
        for k in range(4)
    ]
    coarser = ghost_code[:, :, 0] > 0
    kind = jnp.where(
        ghost_peer[:, :, 0] < 0, 3, jnp.where(refined, 2, jnp.where(coarser, 1, 0))
    )
    single = jnp.logical_and(coarser, jnp.logical_not(refined))
    columns += [
        kind,
        jnp.where(single, major[:, :, 0] - 1, 0),
        jnp.where(single, minor[:, :, 0] - 1, 0),
        jnp.zeros_like(kind),
    ]
    table = jnp.stack(columns, axis=-1).astype(jnp.int32).reshape(-1)
    send = send_faces.reshape(peers, 6)
    children = child_send.reshape(-1)
    parents = parent_peer
    native_fields = fields.reshape(plan.native)
    native_guidance = guidance.reshape(plan.native)

    def exchange(packets):
        return lax.all_to_all(packets, "blk", split_axis=0, concat_axis=0, tiled=True)

    def vm(*shape):
        return pltpu.VMEM(shape, f32)

    def occupied_of(levels_ref):
        return plan.per_slot(lambda s: levels_ref[s]) >= 0

    fb_scratch = vm(*plan.fb)
    kind_scratch = pltpu.VMEM((3 * S * 8, COL), jnp.int32)
    native_planes = [vm(S * 4 * E, COL), vm(S * 4 * E, COL)]
    pair_of_sems = pltpu.SemaphoreType.DMA((2,))
    quarter_sums = [vm(S * 16, COL) for _ in range(6)]
    face_sums = [vm(2, S * 8, COL) for _ in range(6)]
    signs = [1.0, -1.0, 1.0, -1.0, 1.0, -1.0]

    def layers_of(get, fb, ff):
        for c in range(4):
            faces = plan.extract(get, c)
            for f in range(6):
                for q in range(2):
                    if fb is not None:
                        fb[q, plan.fb_rows(f, c), :] = faces[f][q]
                    if ff is not None:
                        ff[q, (f * 4 + c) * S : (f * 4 + c + 1) * S, :] = faces[f][q]

    def corrected_cot_of(get, levels_ref, fb):
        ratio = plan.ratio(levels_ref)
        for c in range(4):
            faces = plan.extract(get, c)
            for f in range(6):
                for q in range(2):
                    fb[q, plan.fb_rows(f, c), :] = (signs[f] * ratio) * faces[f][q]

    def finished(partial, corr, levels_ref, put):
        ratio = plan.ratio(levels_ref)
        occupied = ratio > 0.0
        get = plan.slab_at(partial)

        def face(q, f, c):
            value = corr[q, plan.fb_rows(f, c), :]
            return jnp.where(occupied, (signs[f] * ratio) * value, 0.0)

        for x in range(E):
            for c in range(4):
                for q in range(2):
                    put(q, x, c, get(q, x, c) + plan.spread(face, q, x, c))

    def ghost_reader(gb, layers, levels_ref):
        occupied = occupied_of(levels_ref)
        return lambda q, f, c: jnp.where(
            occupied, gb[q, plan.fb_rows(f, c, True), :], layers(q, f, c)
        )

    def slab_put(ref):
        def put(q, x, c, value):
            ref[q, (x * 4 + c) * S : (x * 4 + c + 1) * S, :] = value

        return put

    def dyn_get(ref):
        return lambda q, rows: ref[q, rows, :]

    def dyn_put(ref):
        def put(q, rows, value):
            ref[q, rows, :] = value

        return put

    ghost_scratch = [vm(8, 3 * S * 8, COL), vm(3 * S * 8, COL), kind_scratch]

    def flux_cot_of(recv, row0, cot_fb, table_s, send_s, sums, kinds, flux_cot, back_r):
        for s in range(S):
            for f in range(6):
                row = ((f // 2) * S + s) * 8 + (f % 2) * 4
                kinds[row : row + 4, :] = jnp.full((4, COL), table_s[(s * 6 + f) * 8 + 4], jnp.int32)

        def face_out(f, c, wide):
            keep = kinds[plan.fb_rows(f, c), :] != 2
            for q in range(2):
                own = jnp.where(keep, cot_fb[q, plan.fb_rows(f, c), :], 0.0)
                flux_cot[q, (f * 4 + c) * S : (f * 4 + c + 1) * S, :] = own + wide[q]

        plan.take_quarters(recv, row0, send_s, sums, face_out, back_r)

    def flux_emitter(b_fb, ff):
        def emit(f, c, values):
            for q in range(2):
                b_fb[q, plan.fb_rows(f, c), :] = values[q]
                ff[q, (f * 4 + c) * S : (f * 4 + c + 1) * S, :] = values[q]

        return emit

    def cot_emitter(layer_cot, gcot):
        def emit(f, c, inner, outer):
            for q in range(2):
                layer_cot[q, (f * 4 + c) * S : (f * 4 + c + 1) * S, :] = inner[q]
                gcot[q, plan.fb_rows(f, c, True), :] = outer[q]

        return emit

    def carry_packets(source, out, row0):
        def one(peer, carry):
            out[peer, row0 : row0 + 16, :] = source[peer, :, :]
            return carry

        lax.fori_loop(0, peers, one, 0)

    def add_layers(through, layer_cot, total, sums, put):
        own = plan.ff_at(layer_cot)
        for f in range(6):
            for c in range(4):
                for q in range(2):
                    added = sums[f][q, pl.ds((f % 2) * 4 + c, S, stride=8), :]
                    total[q, (f * 4 + c) * S : (f * 4 + c + 1) * S, :] = own(q, f, c) + added
        get = plan.slab_at(through)
        summed = plan.ff_at(total)
        for x in range(E):
            for c in range(4):
                for q in range(2):
                    put(q, x, c, get(q, x, c) + plan.spread(summed, q, x, c))

    def first_pack(send_s, parents_s, fields_r, guide_r, volume, layers, packets, fb):
        get = plan.native_at(fields_r.get())
        for x in range(E):
            for c in range(4):
                for q in range(2):
                    volume.ref[q, (x * 4 + c) * S : (x * 4 + c + 1) * S, :] = get(q, x, c)
        volume.send()
        layers_of(plan.slab_at(volume.ref), fb, layers.ref)
        layers.send()
        plan.pack_faces(fb, send_s, packets)
        planes = guide_r.get()
        plan.pack_octants(
            lambda s, x, q: planes[q][plan.native_rows(s, x), :], parents_s, packets.ref, 48
        )
        packets.send(48, 16)

    volume1, layers1, packets = run(
        first_pack,
        "first_pack",
        [send, parents],
        [Late(native_fields, native=True), Late(native_guidance, native=True)],
        [(plan.slab, "late"), (plan.ff, "late"), ((peers, 64, COL), "late")],
        [fb_scratch],
    )
    received1 = exchange(packets)

    def interior_first(levels_s, volume, partial, done):
        plan.interior(dyn_get(volume.get()), levels_s, dyn_put(partial.ref))
        partial.send()
        done[...] = jnp.zeros(done.shape, f32)

    partial1, done1 = run(
        interior_first, "interior_first", [levels], [Late(volume1)],
        [(plan.slab, "late"), ((8, COL), None)], [],
    )

    def first_flux(levels_s, send_s, table_s, layers, after, recv, half_r, back_r, gb, b_fb, packets,
                   planes, near, kinds, ff, rb):
        del after
        plan.ghosts(recv, table_s, planes, near, kinds, gb.ref, half_r, back_r)
        gb.send()
        layer = plan.ff_at(layers.get())
        boundary_fluxes(plan, layer, ghost_reader(gb.ref, layer, levels_s), flux_emitter(b_fb.ref, ff))
        b_fb.send()
        plan.pack_averages(plan.ff_at(ff), rb, send_s, packets, 0, half_r)

    ghosts1, fluxes1, packets = run(
        first_flux,
        "first_flux",
        [levels, send, table],
        [Late(layers1), done1, received1, half, half_back],
        [(plan.fb, "late"), (plan.fb, "late"), ((peers, 16, COL), None)],
        ghost_scratch + [vm(*plan.ff), vm(*plan.coarse)],
    )
    received2 = exchange(packets)

    def upward_second(levels_s, table_s, children_s, parents_s, guide_r, recv, back_r, up, cot_fb,
                      packets, cc):
        planes = guide_r.get()
        plan.upward(recv, 48, cc, children_s, parents_s, plan.native_at(planes), slab_put(up.ref), back_r)
        up.send()
        corrected_cot_of(plan.slab_at(up.ref), levels_s, cot_fb.ref)
        cot_fb.send()
        plan.pack_quarters(cot_fb.ref, table_s, packets.ref, 0)
        packets.send()

    up2, corrcot2, quarters2 = run(
        upward_second,
        "upward_second",
        [levels, table, children, parents],
        [Late(native_guidance, native=True), received1, half_back],
        [(plan.slab, "late"), (plan.fb, "late"), ((peers, 16, COL), "late")],
        [vm((S + 1) * 16, COL)],
    )

    def first_update(levels_s, table_s, children_s, partial, b_fb, recv, quarters, half_r, updated,
                     packets, corr, cb):
        plan.corrected(b_fb.get(), recv, 0, table_s, corr)
        finished(partial.get(), corr, levels_s, slab_put(updated.ref))
        updated.send()
        plan.average_blocks(plan.slab_at(updated.ref), cb, half_r)
        plan.pack_children(cb, children_s, packets, 0)
        carry_packets(quarters.get(), packets, 16)

    updated1, packets = run(
        first_update,
        "first_update",
        [levels, table, children],
        [Late(partial1), Late(fluxes1), received2, Late(quarters2), half],
        [(plan.slab, "late"), ((peers, 32, COL), None)],
        [fb_scratch, vm(*plan.coarse)],
    )
    received3 = exchange(packets)

    def middle_pack(send_s, parents_s, updated, recv, volume, layers, packets, fb, sems):
        copy = pltpu.make_async_copy(updated, volume.ref, sems.at[0])
        copy.start()
        copy.wait()

        def store(s, x, q, value):
            volume.ref[q, plan.slab_rows(s, x), :] = value

        plan.place_octants(recv, 0, parents_s, store)
        volume.send()
        layers_of(plan.slab_at(volume.ref), fb, layers.ref)
        layers.send()
        plan.pack_faces(fb, send_s, packets)

    volume2, layers2, packets = run(
        middle_pack,
        "middle_pack",
        [send, parents],
        [Late(updated1, raw=True), received3],
        [(plan.slab, "late"), (plan.ff, "late"), ((peers, 48, COL), "late")],
        [fb_scratch, pair_of_sems],
    )
    received4 = exchange(packets)

    def flux_cot_second(send_s, table_s, cot_fb, recv, back_r, flux_cot, kinds, *sums):
        flux_cot_of(recv, 16, cot_fb.get(), table_s, send_s, sums, kinds, flux_cot.ref, back_r)
        flux_cot.send()

    (fluxcot2,) = run(
        flux_cot_second,
        "flux_cot_second",
        [send, table],
        [Late(corrcot2), received3, half_back],
        [(plan.ff, "late")],
        [kind_scratch] + quarter_sums,
    )

    def interior_both(levels_s, volume, cot, partial, through):
        plan.interior(
            dyn_get(volume.get()), levels_s, dyn_put(partial.ref), dyn_get(cot.get()), dyn_put(through.ref)
        )
        partial.send()
        through.send()

    partial2, through2 = run(
        interior_both, "interior_both", [levels], [Late(volume2), Late(up2)],
        [(plan.slab, "late"), (plan.slab, "late")], [],
    )

    def second_pull(levels_s, table_s, layers, recv, flux_cot, half_r, back_r, gb, layer_cot,
                    packets, planes, near, kinds, gcot):
        plan.ghosts(recv, table_s, planes, near, kinds, gb.ref, half_r, back_r)
        gb.send()
        layer = plan.ff_at(layers.get())
        boundary_pull(
            plan, layer, ghost_reader(gb.ref, layer, levels_s), plan.ff_at(flux_cot.get()),
            cot_emitter(layer_cot.ref, gcot),
        )
        layer_cot.send()
        plan.pack_ghost_cot(gcot, table_s, planes, near, packets, half_r, back_r)

    ghosts2, layercot2, packets = run(
        second_pull,
        "second_pull",
        [levels, table],
        [Late(layers2), received4, Late(fluxcot2), half, half_back],
        [(plan.fb, "late"), (plan.ff, "late"), ((peers, 48, COL), "late")],
        ghost_scratch + [fb_scratch],
    )
    received5 = exchange(packets)

    def second_flux(levels_s, send_s, layers, gb, half_r, b_fb, packets, ff, rb):
        layer = plan.ff_at(layers.get())
        boundary_fluxes(plan, layer, ghost_reader(gb.get(), layer, levels_s), flux_emitter(b_fb.ref, ff))
        b_fb.send()
        plan.pack_averages(plan.ff_at(ff), rb, send_s, packets.ref, 0, half_r)
        packets.send()

    fluxes2, averages2 = run(
        second_flux,
        "second_flux",
        [levels, send],
        [Late(layers2), Late(ghosts2), half],
        [(plan.fb, "late"), ((peers, 16, COL), "late")],
        [vm(*plan.ff), vm(*plan.coarse)],
    )

    def middle_cot(send_s, parents_s, through, layer_cot, recv, averages, inner, packets, total, *sums):
        plan.take_faces(recv, send_s, sums)
        carry_packets(averages.get(), packets, 16)
        add_layers(through.get(), layer_cot.get(), total, sums, slab_put(inner.ref))
        inner.send()
        plan.pack_octants(
            lambda s, x, q: inner.ref[q, plan.slab_rows(s, x), :], parents_s, packets, 0
        )

    inner_cot, packets = run(
        middle_cot,
        "middle_cot",
        [send, parents],
        [Late(through2), Late(layercot2), received5, Late(averages2)],
        [(plan.slab, "late"), ((peers, 32, COL), None)],
        [vm(*plan.ff)] + face_sums,
    )
    received6 = exchange(packets)

    def upward_first(levels_s, table_s, children_s, parents_s, inner, recv, back_r, up, cot_fb,
                     packets, cc):
        plan.upward(
            recv, 0, cc, children_s, parents_s, lambda q, x, c: plan.slab_at(inner.get())(q, x, c),
            slab_put(up.ref), back_r,
        )
        up.send()
        corrected_cot_of(plan.slab_at(up.ref), levels_s, cot_fb.ref)
        cot_fb.send()
        plan.pack_quarters(cot_fb.ref, table_s, packets, 0)

    up1, corrcot1, packets = run(
        upward_first,
        "upward_first",
        [levels, table, children, parents],
        [Late(inner_cot), received6, half_back],
        [(plan.slab, "late"), (plan.fb, "late"), ((peers, 16, COL), None)],
        [vm((S + 1) * 16, COL)],
    )
    received7 = exchange(packets)

    def second_update(levels_s, table_s, partial, b_fb, recv, half_r, final, cb, corr, updated, n0,
                      n1, sems):
        plan.corrected(b_fb.get(), recv, 16, table_s, corr)
        planes = [n0, n1]
        put_slab = slab_put(updated)

        def put(q, x, c, value):
            put_slab(q, x, c, value)
            planes[q][pl.ds(c * E + x, S, stride=4 * E), :] = value

        finished(partial.get(), corr, levels_s, put)
        copies = native_copies(planes, final, sems, False)
        for copy in copies:
            copy.start()
        plan.average_blocks(plan.slab_at(updated), cb, half_r)
        for copy in copies:
            copy.wait()

    final_open, coarse2 = run(
        second_update,
        "second_update",
        [levels, table],
        [Late(partial2), Late(fluxes2), received6, half],
        [(plan.native, "raw"), (plan.coarse, None)],
        [fb_scratch, vm(*plan.slab)] + native_planes + [pair_of_sems],
    )

    def interior_back(levels_s, volume, cot, through):
        plan.interior(
            dyn_get(volume.get()), levels_s, None, dyn_get(cot.get()), dyn_put(through.ref)
        )
        through.send()

    (through1,) = run(
        interior_back, "interior_back", [levels], [Late(volume1), Late(up1)],
        [(plan.slab, "late")], [],
    )

    def first_pull(levels_s, send_s, table_s, children_s, layers, gb, cot_fb, recv, coarse, half_r,
                   back_r, layer_cot, packets, planes, near, kinds, flux_cot, gcot, *sums):
        plan.pack_children(coarse, children_s, packets.ref, 48)
        packets.send(48, 16)
        flux_cot_of(recv, 0, cot_fb.get(), table_s, send_s, sums, kinds, flux_cot, back_r)
        layer = plan.ff_at(layers.get())
        boundary_pull(
            plan, layer, ghost_reader(gb.get(), layer, levels_s), plan.ff_at(flux_cot),
            cot_emitter(layer_cot.ref, gcot),
        )
        layer_cot.send()
        plan.pack_ghost_cot(gcot, table_s, planes, near, packets, half_r, back_r)

    layercot1, packets = run(
        first_pull,
        "first_pull",
        [levels, send, table, children],
        [Late(layers1), Late(ghosts1), Late(corrcot1), received7, coarse2, half, half_back],
        [(plan.ff, "late"), ((peers, 64, COL), "late")],
        ghost_scratch + [vm(*plan.ff), fb_scratch] + quarter_sums,
    )
    received8 = exchange(packets)

    def last_cot(send_s, parents_s, through, layer_cot, recv, open_r, gradient, final, total, n0, n1,
                 p0, p1, sems, slot_sems, *sums):
        del open_r
        placed = [p0, p1]

        def store(s, x, q, value):
            placed[q][plan.native_rows(s, x), :] = value

        plan.place_octants(recv, 48, parents_s, store)

        def each_covered(act):
            for s in range(S):

                def one(s=s):
                    rows = (s * 4 * E, 4 * E)
                    for copy in native_copies(placed, final, slot_sems.at[s], False, rows):
                        act(copy)

                pl.when(parents_s[s, 0] >= 0)(one)

        each_covered(lambda copy: copy.start())
        plan.take_faces(recv, send_s, sums)
        planes = [n0, n1]

        def put(q, x, c, value):
            planes[q][pl.ds(c * E + x, S, stride=4 * E), :] = value

        add_layers(through.get(), layer_cot.get(), total, sums, put)
        copies = native_copies(planes, gradient, sems, False)
        for copy in copies:
            copy.start()
        for copy in copies:
            copy.wait()
        each_covered(lambda copy: copy.wait())

    gradient, final_fields = run(
        last_cot,
        "last_cot",
        [send, parents],
        [Late(through1), Late(layercot1), received8, Late(final_open, raw=True)],
        [(plan.native, "raw"), (plan.native, "raw")],
        [vm(*plan.ff)] + native_planes + native_planes
        + [pair_of_sems, pltpu.SemaphoreType.DMA((S, 2))] + face_sums,
        aliases={5: 1},
    )
    return (final_fields.reshape(fields.shape), gradient.reshape(fields.shape))


def solution(mesh):
    placed = (
        P("blk", None, None, None),
        P("blk", None, None, None),
        P("blk"),
        P("blk", None, None),
        P("blk", None, None),
        P("blk", None, None),
        P("blk", None),
        P("blk", None),
    )
    return jax.shard_map(
        on_device,
        mesh=mesh,
        in_specs=placed,
        out_specs=(P("blk", None, None, None), P("blk", None, None, None)),
        check_vma=False,
    )
```

```python
import jax
import jax.numpy as jnp
import numpy as np
from jax import lax
from jax.experimental import pallas as pl
from jax.experimental.pallas import tpu as pltpu
from jax.sharding import PartitionSpec as P

sound_speed = 1.0
base_ratio = 0.04
speed_floor = 0.01
f32 = jnp.float32
bf16 = jnp.bfloat16


def half_map(extent):
    half = extent // 2
    square = extent * extent
    table = np.zeros((2, extent, extent, half, 2, half), np.float32)
    for group in range(2):
        for i in range(extent):
            for j in range(extent):
                table[group, i, j, i // 2, group, j // 2] = 0.25
    return table.reshape(2 * square, square // 2)


def dot2(values, table):
    high = values.astype(bf16)
    low = (values - high.astype(f32)).astype(bf16)
    return jnp.dot(high, table, preferred_element_type=f32) + jnp.dot(
        low, table, preferred_element_type=f32
    )


def roll(values, shift):
    lanes = values.shape[1]
    shift = shift % lanes
    return values if shift == 0 else pltpu.roll(values, shift, 1)


def tile(packets, peer, row):
    return packets.at[peer, row // 4] if len(packets.shape) == 4 else packets.at[peer, row : row + 4]


def flux_of(behind, beyond, normal, inv_behind, inv_beyond):
    v = behind[1 + normal] * inv_behind
    w = beyond[1 + normal] * inv_beyond
    c = sound_speed + jnp.sqrt(0.5 * (v * v + w * w) + speed_floor)
    result = [0.5 * ((behind[1 + normal] + beyond[1 + normal]) - c * (beyond[0] - behind[0]))]
    for k in range(1, 4):
        total = behind[k] * v + beyond[k] * w
        if k == 1 + normal:
            total = total + (sound_speed * sound_speed) * (behind[0] + beyond[0])
        result.append(0.5 * (total - c * (beyond[k] - behind[k])))
    return result


def flux_pull(behind, beyond, normal, inv_behind, inv_beyond, cot):
    v = behind[1 + normal] * inv_behind
    w = beyond[1 + normal] * inv_beyond
    inside = 0.5 * (v * v + w * w) + speed_floor
    root = jnp.sqrt(inside)
    c = sound_speed + root
    half_cot = [0.5 * part for part in cot]
    jump = half_cot[0] * (beyond[0] - behind[0])
    v_cot = half_cot[1] * behind[1]
    w_cot = half_cot[1] * beyond[1]
    for k in range(1, 4):
        jump = jump + half_cot[k] * (beyond[k] - behind[k])
        if k > 1:
            v_cot = v_cot + half_cot[k] * behind[k]
            w_cot = w_cot + half_cot[k] * beyond[k]
    scale = jump * (-0.5) / root
    v_cot = (v_cot + scale * v) * inv_behind
    w_cot = (w_cot + scale * w) * inv_beyond
    plus = v + c
    minus = w - c
    behind_cot = []
    beyond_cot = []
    pressure = (sound_speed * sound_speed) * half_cot[1 + normal]
    for k in range(4):
        if k == 0:
            behind_cot.append(c * half_cot[0] + pressure - v_cot * v)
            beyond_cot.append(pressure - c * half_cot[0] - w_cot * w)
        else:
            left = half_cot[k] * plus
            right = half_cot[k] * minus
            if k == 1 + normal:
                left = left + half_cot[0] + v_cot
                right = right + half_cot[0] + w_cot
            behind_cot.append(left)
            beyond_cot.append(right)
    return behind_cot, beyond_cot


class Plan:
    def __init__(self, slots, extent, peers):
        self.S = slots
        self.E = extent
        self.P = peers
        self.H = extent // 2
        self.COL = extent * extent // 2
        self.slab = (2, extent * 4 * slots, self.COL)
        self.ff = (2, 6 * 4 * slots, self.COL)
        self.fb = (2, 3 * slots * 8, self.COL)
        self.native = (slots * 4 * extent, 2 * self.COL)
        self.coarse = (slots * 32, self.COL)
        self.small = (slots * 24, self.COL)

    def lane(self, rows):
        return lax.broadcasted_iota(jnp.int32, (rows, self.COL), 1)

    def low(self, rows):
        return (self.lane(rows) & (self.E - 1)) < self.H

    def per_slot(self, scalar_of):
        sub = lax.broadcasted_iota(jnp.int32, (self.S, self.COL), 0)
        value = jnp.zeros((self.S, self.COL), jnp.int32)
        for s in range(self.S):
            value = jnp.where(sub == s, scalar_of(s), value)
        return value

    def ratio(self, levels):
        level = self.per_slot(lambda s: levels[s])
        degree = level.astype(f32)
        ratio = base_ratio * (1.0 + degree + 0.5 * degree * (degree - 1.0))
        return jnp.where(level >= 0, ratio, 0.0)

    def slab_at(self, ref):
        return lambda q, x, c: ref[q, (x * 4 + c) * self.S : (x * 4 + c + 1) * self.S, :]

    def native_at(self, planes):
        step = 4 * self.E
        return lambda q, x, c: planes[q][pl.ds(c * self.E + x, self.S, stride=step), :]

    def ff_at(self, ref):
        return lambda q, f, c: ref[q, (f * 4 + c) * self.S : (f * 4 + c + 1) * self.S, :]

    def fb_rows(self, f, c, swapped=False):
        side = f % 2
        half = 1 - side if swapped else side
        return pl.ds((f // 2) * self.S * 8 + half * 4 + c, self.S, stride=8)

    def extract(self, get, c):
        E, H, COL = self.E, self.H, self.COL
        lane = self.lane(self.S)
        group = lax.shift_right_logical(lane, E.bit_length() - 1)
        within = lane & (E - 1)
        faces = [[get(q, 0, c) for q in range(2)], [get(q, E - 1, c) for q in range(2)]]
        low_y, high_y, low_z, high_z = [], [], [], []
        for q in range(2):
            first, last, near, far = None, None, None, None
            for k in range(H):
                a = roll(get(0, q * H + k, c), E * k)
                b = roll(get(1, q * H + k, c), E * k - (COL - E))
                first = a if first is None else jnp.where(group == k, a, first)
                last = b if last is None else jnp.where(group == k, b, last)
            for x in range(E):
                source = get(q, x, c)
                a = roll(source, x)
                b = roll(source, x - (E - 1))
                near = a if near is None else jnp.where(within == x, a, near)
                far = b if far is None else jnp.where(within == x, b, far)
            low_y.append(first)
            high_y.append(last)
            low_z.append(near)
            high_z.append(far)
        return faces + [low_y, high_y, low_z, high_z]

    def spread(self, face, q, x, c):
        E, H, COL = self.E, self.H, self.COL
        lane = self.lane(self.S)
        within = lane & (E - 1)
        k = x % H
        y_face = face(x // H, 2 + q, c)
        if q == 0:
            total = jnp.where(lane < E, roll(y_face, -E * k), 0.0)
        else:
            total = jnp.where(lane >= COL - E, roll(y_face, (COL - E) - E * k), 0.0)
        near = roll(face(q, 4, c), -x)
        far = roll(face(q, 5, c), E - 1 - x)
        total = total + jnp.where(within == 0, near, jnp.where(within == E - 1, far, 0.0))
        if x == 0:
            total = total + face(q, 0, c)
        if x == E - 1:
            total = total + face(q, 1, c)
        return total

    def pack_faces(self, fb, send, out):
        sub = lax.broadcasted_iota(jnp.int32, (8, self.COL), 0)
        for axis in range(3):

            def one(peer, carry, axis=axis):
                slots = [jnp.maximum(send[peer, axis * 2 + side], 0) for side in range(2)]
                for q in range(2):
                    lo, hi = [
                        fb[q, pl.ds(pl.multiple_of((axis * self.S + slot) * 8, 8), 8), :]
                        for slot in slots
                    ]
                    row = axis * 16 + q * 8
                    out.ref[peer, row : row + 8, :] = jnp.where(sub < 4, lo, hi)
                return carry

            lax.fori_loop(0, self.P, one, 0, unroll=4)
            out.send(axis * 16, 16)

    def take_faces(self, packets, send, sums):
        def one(peer, carry):
            for f in range(6):
                slot = jnp.maximum(send[peer, f], 0)
                rows = pl.ds(pl.multiple_of(slot * 8, 8), 8)
                for q in range(2):
                    at = (f // 2) * 16 + q * 8
                    sums[f][q, rows, :] += packets[peer, at : at + 8, :]
            return carry

        for f in range(6):
            sums[f][...] = jnp.zeros(sums[f].shape, f32)
        lax.fori_loop(0, self.P, one, 0)

    def pack_averages(self, face, rb, send, out, row0, half):
        S, COL = self.S, self.COL
        rows = []
        for axis in range(3):
            for c in range(4):
                rows.append(
                    jnp.concatenate(
                        [face(q, 2 * axis + side, c) for side in range(2) for q in range(2)], axis=1
                    )
                )
        small = dot2(jnp.concatenate(rows, axis=0), half[...])
        for k in range(12):
            rb[pl.ds((k // 4) * 8 + k % 4, S, stride=24), :] = small[k * S : (k + 1) * S]
        low = self.low(4)

        def one(peer, carry):
            for axis in range(3):
                lo, hi = [
                    rb[pl.ds(pl.multiple_of(slot * 24 + axis * 8, 8), 4), :]
                    for slot in [jnp.maximum(send[peer, axis * 2 + side], 0) for side in range(2)]
                ]
                tile(out, peer, row0 + axis * 4)[...] = jnp.where(low, lo, hi)
            return carry

        lax.fori_loop(0, self.P, one, 0)

    def pack_quarters(self, fb, table, out, row0):
        E, H = self.E, self.H
        low = self.low(4)

        def clear(peer, carry):
            for axis in range(3):
                tile(out, peer, row0 + axis * 4)[...] = jnp.zeros((4, self.COL), f32)
            return carry

        lax.fori_loop(0, self.P, clear, 0)
        for s in range(self.S):
            for f in range(6):
                base = (s * 6 + f) * 8

                def send_quarters(s=s, f=f, base=base):
                    axis, side = f // 2, f % 2
                    keep = low if side == 1 else jnp.logical_not(low)
                    row = (axis * self.S + s) * 8 + side * 4
                    at = row0 + axis * 4
                    for h in range(2):
                        values = fb[h, row : row + 4, :]
                        for g in range(2):
                            moved = roll(values, H * ((1 - side) - g))
                            peer = table[base + h * 2 + g]
                            tile(out, peer, at)[...] += jnp.where(keep, moved, 0.0)

                pl.when(table[base + 4] == 2)(send_quarters)

    def take_quarters(self, packets, row0, send, sums, face_out, half_back):
        S, COL = self.S, self.COL

        def one(peer, carry):
            for axis in range(3):
                block = tile(packets, peer, row0 + axis * 4)[...]
                for f in (axis * 2, axis * 2 + 1):
                    slot = jnp.maximum(send[peer, f], 0)
                    sums[f][pl.ds(pl.multiple_of(slot * 8, 8), 4), :] += block
            return carry

        for f in range(6):
            sums[f][...] = jnp.zeros(sums[f].shape, f32)
        lax.fori_loop(0, self.P, one, 0)
        for f in range(6):
            side = f % 2
            rows = jnp.concatenate(
                [sums[f][pl.ds(c, S, stride=8), :] for c in range(4)], axis=0
            )
            wide = dot2(rows, half_back[:, side * 2 * COL : (side + 1) * 2 * COL])
            for c in range(4):
                face_out(f, c, [wide[c * S : (c + 1) * S, q * COL : (q + 1) * COL] for q in range(2)])

    def ghosts(self, packets, table, planes, near, kinds, gb, half, half_back):
        S, COL, H = self.S, self.COL, self.H
        for s in range(S):
            for f in range(6):
                base = (s * 6 + f) * 8
                axis, half_row = f // 2, (1 - f % 2) * 4
                row = (axis * S + s) * 8 + half_row
                first = None
                for k in range(4):
                    peer = table[base + k]
                    got = []
                    for q in range(2):
                        at = axis * 16 + q * 8 + half_row
                        values = packets[peer, at : at + 4, :]
                        planes[k * 2 + q, row : row + 4, :] = values
                        got.append(values)
                    if k == 0:
                        first = got
                source = jnp.where(table[base + 5] == 1, first[1], first[0])
                source = jnp.where(table[base + 6] == 1, roll(source, -H), source)
                near[row : row + 4, :] = source
                kinds[row : row + 4, :] = jnp.full((4, COL), table[base + 4], jnp.int32)
        for axis in range(3):
            rows = slice(axis * S * 8, (axis + 1) * S * 8)
            kind = kinds[rows, :]
            coarse = 4.0 * dot2(near[rows, :], half_back[:, : 2 * COL])
            for h in range(2):
                parts = [planes[(h * 2 + g) * 2 + q, rows, :] for g in range(2) for q in range(2)]
                fine = dot2(jnp.concatenate(parts, axis=1), half[...])
                value = jnp.where(kind == 1, coarse[:, h * COL : (h + 1) * COL], planes[h, rows, :])
                gb[h, rows, :] = jnp.where(kind == 2, fine, value)

    def pack_ghost_cot(self, gb, table, wide, near, out, half, half_back):
        S, COL, H = self.S, self.COL, self.H
        low = self.low(4)

        def clear(peer, carry):
            out.ref[peer, 0:48, :] = jnp.zeros((48, COL), f32)
            return carry

        lax.fori_loop(0, self.P, clear, 0)
        for h in range(2):
            for g in range(2):
                spread = dot2(gb[h, :, :], half_back[:, g * 2 * COL : (g + 1) * 2 * COL])
                for q in range(2):
                    wide[(h * 2 + g) * 2 + q, :, :] = spread[:, q * COL : (q + 1) * COL]
        both = jnp.concatenate([gb[0, :, :], gb[1, :, :]], axis=1)
        near[...] = 4.0 * dot2(both, half[0 : 2 * COL, :])
        for f in range(6):
            for s in range(S):
                base = (s * 6 + f) * 8
                axis, half_row = f // 2, (1 - f % 2) * 4
                row = (axis * S + s) * 8 + half_row
                kind = table[base + 4]

                def same(base=base, axis=axis, half_row=half_row, row=row):
                    peer = table[base]
                    for q in range(2):
                        at = axis * 16 + q * 8 + half_row
                        out.ref[peer, at : at + 4, :] += gb[q, row : row + 4, :]

                def coarse(base=base, axis=axis, half_row=half_row, row=row):
                    peer = table[base]
                    values = near[row : row + 4, :]
                    values = jnp.where(table[base + 6] == 1, roll(values, H), values)
                    for q in range(2):
                        at = axis * 16 + q * 8 + half_row
                        out.ref[peer, at : at + 4, :] += jnp.where(table[base + 5] == q, values, 0.0)

                def fine(base=base, axis=axis, half_row=half_row, row=row):
                    for k in range(4):
                        peer = table[base + k]
                        for q in range(2):
                            at = axis * 16 + q * 8 + half_row
                            out.ref[peer, at : at + 4, :] += wide[k * 2 + q, row : row + 4, :]

                pl.when(kind == 0)(same)
                pl.when(kind == 1)(coarse)
                pl.when(kind == 2)(fine)
            if f % 2 == 1:
                out.send((f // 2) * 16, 16)

    def corrected(self, b_fb, packets, row0, table, out):
        H = self.H
        low = self.low(4)
        out[...] = b_fb[...]
        for s in range(self.S):
            for f in range(6):
                base = (s * 6 + f) * 8

                def replace(s=s, f=f, base=base):
                    axis, side = f // 2, f % 2
                    row = (axis * self.S + s) * 8 + side * 4
                    at = row0 + axis * 4
                    for h in range(2):
                        got = []
                        for g in range(2):
                            values = tile(packets, table[base + h * 2 + g], at)[...]
                            got.append(roll(values, H * (g - (1 - side))))
                        out[h, row : row + 4, :] = jnp.where(low, got[0], got[1])

                pl.when(table[base + 4] == 2)(replace)

    def pack_octants(self, load, parents, out, row0):
        H = self.H
        low = self.low(4)
        for s in range(self.S):

            def send(s=s):
                for ox in range(2):
                    for oy in range(2):
                        peers = [parents[s, ox * 4 + oy * 2 + oz] for oz in range(2)]
                        for pair in range(H // 2):
                            x = ox * H + pair * 2
                            first, second = load(s, x, oy), load(s, x + 1, oy)
                            at = row0 + pair * 4
                            tile(out, peers[0], at)[...] = jnp.where(low, first, roll(second, H))
                            tile(out, peers[1], at)[...] = jnp.where(low, roll(first, -H), second)

            pl.when(parents[s, 0] >= 0)(send)

    def place_octants(self, packets, row0, parents, store):
        H = self.H
        low = self.low(4)
        for s in range(self.S):

            def place(s=s):
                for ox in range(2):
                    for oy in range(2):
                        peers = [parents[s, ox * 4 + oy * 2 + oz] for oz in range(2)]
                        for pair in range(H // 2):
                            x = ox * H + pair * 2
                            at = row0 + pair * 4
                            first = tile(packets, peers[0], at)[...]
                            second = tile(packets, peers[1], at)[...]
                            store(s, x, oy, jnp.where(low, first, roll(second, H)))
                            store(s, x + 1, oy, jnp.where(low, roll(first, -H), second))

            pl.when(parents[s, 0] >= 0)(place)

    def slab_rows(self, s, x):
        return pl.ds(x * 4 * self.S + s, 4, stride=self.S)

    def native_rows(self, s, x):
        return pl.ds(s * 4 * self.E + x, 4, stride=self.E)

    def average_blocks(self, get, cb, half):
        S = self.S
        rows = []
        for pair in range(self.E // 4):
            for c in range(4):
                x = 4 * pair
                rows.append(
                    jnp.concatenate(
                        [get(q, x + 2 * a, c) + get(q, x + 2 * a + 1, c) for a in range(2) for q in range(2)],
                        axis=1,
                    )
                )
        small = 0.5 * dot2(jnp.concatenate(rows, axis=0), half[...])
        for k in range(16):
            cb[pl.ds((k // 4) * 8 + k % 4, S, stride=32), :] = small[k * S : (k + 1) * S]

    def pack_children(self, cb, children, out, row0):
        def one(peer, carry):
            slot = jnp.maximum(children[peer], 0)
            for part in range(4):
                rows = pl.ds(pl.multiple_of(slot * 32 + part * 8, 8), 4)
                tile(out, peer, row0 + part * 4)[...] = cb[rows, :]
            return carry

        lax.fori_loop(0, self.P, one, 0)

    def upward(self, packets, row0, cc, children, parents, get, put, half_back):
        S, COL = self.S, self.COL
        cc[...] = jnp.zeros(cc.shape, f32)

        def one(peer, carry):
            child = children[peer]
            slot = jnp.where(child < 0, S, child)
            for part in range(4):
                rows = pl.ds(pl.multiple_of(slot * 32 + part * 8, 8), 4)
                cc[rows, :] += tile(packets, peer, row0 + part * 4)[...]
            return carry

        lax.fori_loop(0, self.P, one, 0)
        rows = jnp.concatenate(
            [cc[pl.ds((k // 4) * 8 + k % 4, S, stride=32), :] for k in range(16)], axis=0
        )
        wide = 0.5 * dot2(rows, half_back[...])
        covered = self.per_slot(lambda s: parents[s, 0]) >= 0
        for x in range(self.E):
            for c in range(4):
                row = ((x // 4) * 4 + c) * S
                for q in range(2):
                    lane0 = ((x // 2) % 2 * 2 + q) * COL
                    added = wide[row : row + S, lane0 : lane0 + COL]
                    put(q, x, c, jnp.where(covered, 0.0, get(q, x, c)) + added)

    def shifted(self, planes, amount):
        COL = self.COL
        lane = self.lane(self.S)
        moved = [roll(values, amount) for values in planes]
        if amount > 0:
            return [jnp.where(lane < amount, moved[1 - q], moved[q]) for q in range(2)]
        return [jnp.where(lane >= COL + amount, moved[1 - q], moved[q]) for q in range(2)]

    def interior(self, get, levels, forward_put, cot_get=None, cot_put=None):
        S, E, COL = self.S, self.E, self.COL
        ratio = self.ratio(levels)
        lane = self.lane(S)
        y_inside = [lane >= 0, lane < COL - E]
        z_inside = (lane & (E - 1)) != E - 1
        zero = jnp.zeros((S, COL), f32)

        def row_of(x, c):
            return pl.ds(pl.multiple_of((x * 4 + c) * S, S), S)

        def one(x, carry):
            after = jnp.minimum(x + 1, E - 1)
            x_inside = x < E - 1
            here = [[get(q, row_of(x, c)) for c in range(4)] for q in range(2)]
            inverse = [1.0 / here[q][0] for q in range(2)]
            ahead = [[get(q, row_of(after, c)) for c in range(4)] for q in range(2)]
            ahead_inv = [1.0 / ahead[q][0] for q in range(2)]
            flux_carry, cot_carry = carry
            new_flux, new_cot = [], []
            change = [[None] * 4 for _ in range(2)]
            if cot_get is not None:
                weight = [[get_c(q, row_of(x, c)) for c in range(4)] for q in range(2)]
                scaled = [[ratio * weight[q][c] for c in range(4)] for q in range(2)]
                ahead_scaled = [
                    [ratio * get_c(q, row_of(after, c)) for c in range(4)] for q in range(2)
                ]
                back = [[weight[q][c] for c in range(4)] for q in range(2)]
            for q in range(2):
                if forward_put is not None:
                    flux = flux_of(here[q], ahead[q], 0, inverse[q], ahead_inv[q])
                    flux = [jnp.where(x_inside, part, 0.0) for part in flux]
                    change[q] = [flux[c] - flux_carry[q * 4 + c] for c in range(4)]
                    new_flux += flux
                if cot_get is not None:
                    cot = [
                        jnp.where(x_inside, ahead_scaled[q][c] - scaled[q][c], 0.0) for c in range(4)
                    ]
                    left, right = flux_pull(here[q], ahead[q], 0, inverse[q], ahead_inv[q], cot)
                    back[q] = [back[q][c] + left[c] + cot_carry[q * 4 + c] for c in range(4)]
                    new_cot += right
            for normal, step, inside in ((1, E, y_inside), (2, 1, [z_inside, z_inside])):
                turned = [self.shifted([here[q][c] for q in range(2)], -step) for c in range(4)]
                turned_inv = self.shifted(inverse, -step)
                beyond = [[turned[c][q] for c in range(4)] for q in range(2)]
                if forward_put is not None:
                    flux = []
                    for q in range(2):
                        got = flux_of(here[q], beyond[q], normal, inverse[q], turned_inv[q])
                        flux.append([jnp.where(inside[q], part, 0.0) for part in got])
                    for c in range(4):
                        behind = self.shifted([flux[q][c] for q in range(2)], step)
                        for q in range(2):
                            change[q][c] = change[q][c] + (flux[q][c] - behind[q])
                if cot_get is not None:
                    turned_w = [self.shifted([scaled[q][c] for q in range(2)], -step) for c in range(4)]
                    rights = []
                    for q in range(2):
                        cot = [
                            jnp.where(inside[q], turned_w[c][q] - scaled[q][c], 0.0) for c in range(4)
                        ]
                        left, right = flux_pull(here[q], beyond[q], normal, inverse[q], turned_inv[q], cot)
                        back[q] = [back[q][c] + left[c] for c in range(4)]
                        rights.append(right)
                    for c in range(4):
                        moved = self.shifted([rights[q][c] for q in range(2)], step)
                        for q in range(2):
                            back[q][c] = back[q][c] + moved[q]
            for q in range(2):
                for c in range(4):
                    if forward_put is not None:
                        forward_put(q, row_of(x, c), here[q][c] - ratio * change[q][c])
                    if cot_get is not None:
                        cot_put(q, row_of(x, c), back[q][c])
            return (new_flux, new_cot)

        get_c = cot_get
        start = (
            [zero] * 8 if forward_put is not None else [],
            [zero] * 8 if cot_get is not None else [],
        )
        lax.fori_loop(0, E, one, start)


class Arriving:
    def __init__(self, copies, ref):
        self.copies = copies
        self.ref = ref
        for copy in copies:
            copy.start()

    def get(self):
        for copy in self.copies:
            copy.wait()
        self.copies = []
        return self.ref


class Leaving:
    def __init__(self, ref, target, sems):
        self.ref = ref
        self.target = target
        self.sems = sems
        self.copies = []

    def send(self, first=None, count=None):
        near, far = self.ref, self.target
        if count is not None:
            near = near.at[:, pl.ds(first, count), :]
            far = far.at[:, pl.ds(first, count), :]
        copy = pltpu.make_async_copy(near, far, self.sems.at[len(self.copies)])
        copy.start()
        self.copies.append(copy)

    def finish(self):
        for copy in self.copies:
            copy.wait()


class Late:
    def __init__(self, array, native=False, raw=False):
        self.array = array
        self.native = native
        self.raw = raw


def run(body, name, scalars, arrays, outs, scratch, aliases=None):
    hbm = pltpu.MemorySpace.HBM
    specs = [pl.BlockSpec(memory_space=pltpu.SMEM) for _ in scalars]
    operands = list(scalars)
    extra = []
    arriving, leaving = {}, {}
    for index, item in enumerate(arrays):
        if isinstance(item, Late):
            specs.append(pl.BlockSpec(memory_space=hbm))
            operands.append(pltpu.with_memory_space_constraint(item.array, hbm))
            if not item.raw:
                shape = item.array.shape
                arriving[index] = (len(extra), item.native)
                if item.native:
                    half = (shape[0], shape[1] // 2)
                    extra += [pltpu.VMEM(half, f32), pltpu.VMEM(half, f32)]
                    extra.append(pltpu.SemaphoreType.DMA((2,)))
                else:
                    extra += [pltpu.VMEM(shape, f32), pltpu.SemaphoreType.DMA((1,))]
        else:
            specs.append(pl.BlockSpec(memory_space=pltpu.VMEM))
            operands.append(item)
    out_specs = []
    for index, (shape, mode) in enumerate(outs):
        out_specs.append(pl.BlockSpec(memory_space=hbm if mode else pltpu.VMEM))
        if mode == "late":
            leaving[index] = len(extra)
            extra += [pltpu.VMEM(shape, f32), pltpu.SemaphoreType.DMA((4,))]

    def wrapped(*refs):
        n_scalar, n_in, n_out = len(scalars), len(arrays), len(outs)
        scalar_refs = list(refs[:n_scalar])
        in_refs = list(refs[n_scalar : n_scalar + n_in])
        out_refs = list(refs[n_scalar + n_in : n_scalar + n_in + n_out])
        rest = refs[n_scalar + n_in + n_out :]
        own, late = rest[: len(scratch)], rest[len(scratch) :]
        for index, (at, native) in arriving.items():
            if native:
                planes = [late[at], late[at + 1]]
                copies = native_copies(planes, in_refs[index], late[at + 2], True)
                in_refs[index] = Arriving(copies, planes)
            else:
                copy = pltpu.make_async_copy(in_refs[index], late[at], late[at + 1].at[0])
                in_refs[index] = Arriving([copy], late[at])
        for index, at in leaving.items():
            out_refs[index] = Leaving(late[at], out_refs[index], late[at + 1])
        body(*scalar_refs, *in_refs, *out_refs, *own)
        for index in arriving:
            in_refs[index].get()
        for index in leaving:
            out_refs[index].finish()

    return pl.pallas_call(
        wrapped,
        name=name,
        in_specs=specs,
        out_specs=out_specs,
        out_shape=[
            hbm(shape, f32) if mode else jax.ShapeDtypeStruct(shape, f32) for shape, mode in outs
        ],
        scratch_shapes=list(scratch) + extra,
        input_output_aliases=aliases or {},
        compiler_params=pltpu.CompilerParams(vmem_limit_bytes=32 * 1024 * 1024),
    )(*operands)


def native_copies(planes, whole, sems, inward, rows=None):
    lanes = planes[0].shape[1]
    copies = []
    for q in range(2):
        part = whole.at[:, pl.ds(q * lanes, lanes)]
        near = planes[q]
        if rows is not None:
            part = whole.at[pl.ds(*rows), pl.ds(q * lanes, lanes)]
            near = planes[q].at[pl.ds(*rows), :]
        source, target = (part, near) if inward else (near, part)
        copies.append(pltpu.make_async_copy(source, target, sems.at[q]))
    return copies


def boundary_fluxes(plan, layers, ghost, emit):
    for f in range(6):
        result = []
        for q in range(2):
            inner = [layers(q, f, c) for c in range(4)]
            outer = [ghost(q, f, c) for c in range(4)]
            inner_inv, outer_inv = 1.0 / inner[0], 1.0 / outer[0]
            if f % 2 == 0:
                result.append(flux_of(outer, inner, f // 2, outer_inv, inner_inv))
            else:
                result.append(flux_of(inner, outer, f // 2, inner_inv, outer_inv))
        for c in range(4):
            emit(f, c, [result[q][c] for q in range(2)])


def boundary_pull(plan, layers, ghost, cot, emit):
    for f in range(6):
        result = []
        for q in range(2):
            inner = [layers(q, f, c) for c in range(4)]
            outer = [ghost(q, f, c) for c in range(4)]
            weight = [cot(q, f, c) for c in range(4)]
            inner_inv, outer_inv = 1.0 / inner[0], 1.0 / outer[0]
            if f % 2 == 0:
                out_cot, in_cot = flux_pull(outer, inner, f // 2, outer_inv, inner_inv, weight)
            else:
                in_cot, out_cot = flux_pull(inner, outer, f // 2, inner_inv, outer_inv, weight)
            result.append((in_cot, out_cot))
        for c in range(4):
            emit(f, c, [result[q][0][c] for q in range(2)], [result[q][1][c] for q in range(2)])


def on_device(fields, guidance, levels, send_faces, ghost_peer, ghost_code, child_send, parent_peer):
    slots, _, extent, square = fields.shape
    peers = send_faces.shape[1]
    plan = Plan(slots, extent, peers)
    S, E, COL = slots, extent, plan.COL
    half_np = half_map(extent)
    half = jnp.asarray(half_np, bf16)
    half_back = jnp.asarray(np.ascontiguousarray(half_np.T), bf16)

    first_map, second_map = ghost_code // 5, ghost_code % 5
    turned = (jnp.arange(6) >= 4)[None, :, None]
    major = jnp.where(turned, second_map, first_map)
    minor = jnp.where(turned, first_map, second_map)
    refined = ghost_peer[:, :, 1] >= 0
    quarter = (major - 3) * 2 + (minor - 3)
    chosen = jnp.maximum(ghost_peer, 0)
    columns = [
        jnp.where(refined, jnp.sum(jnp.where(quarter == k, chosen, 0), axis=2), chosen[:, :, 0])
        for k in range(4)
    ]
    coarser = ghost_code[:, :, 0] > 0
    kind = jnp.where(
        ghost_peer[:, :, 0] < 0, 3, jnp.where(refined, 2, jnp.where(coarser, 1, 0))
    )
    single = jnp.logical_and(coarser, jnp.logical_not(refined))
    columns += [
        kind,
        jnp.where(single, major[:, :, 0] - 1, 0),
        jnp.where(single, minor[:, :, 0] - 1, 0),
        jnp.zeros_like(kind),
    ]
    table = jnp.stack(columns, axis=-1).astype(jnp.int32).reshape(-1)
    send = send_faces.reshape(peers, 6)
    children = child_send.reshape(-1)
    parents = parent_peer
    native_fields = fields.reshape(plan.native)
    native_guidance = guidance.reshape(plan.native)

    def exchange(packets):
        return lax.all_to_all(packets, "blk", split_axis=0, concat_axis=0, tiled=True)

    def vm(*shape):
        return pltpu.VMEM(shape, f32)

    def occupied_of(levels_ref):
        return plan.per_slot(lambda s: levels_ref[s]) >= 0

    fb_scratch = vm(*plan.fb)
    kind_scratch = pltpu.VMEM((3 * S * 8, COL), jnp.int32)
    native_planes = [vm(S * 4 * E, COL), vm(S * 4 * E, COL)]
    pair_of_sems = pltpu.SemaphoreType.DMA((2,))
    quarter_sums = [vm(S * 8, COL) for _ in range(6)]
    face_sums = [vm(2, S * 8, COL) for _ in range(6)]
    signs = [1.0, -1.0, 1.0, -1.0, 1.0, -1.0]

    def layers_of(get, fb, ff):
        for c in range(4):
            faces = plan.extract(get, c)
            for f in range(6):
                for q in range(2):
                    if fb is not None:
                        fb[q, plan.fb_rows(f, c), :] = faces[f][q]
                    if ff is not None:
                        ff[q, (f * 4 + c) * S : (f * 4 + c + 1) * S, :] = faces[f][q]

    def corrected_cot_of(get, levels_ref, fb):
        ratio = plan.ratio(levels_ref)
        for c in range(4):
            faces = plan.extract(get, c)
            for f in range(6):
                for q in range(2):
                    fb[q, plan.fb_rows(f, c), :] = (signs[f] * ratio) * faces[f][q]

    def finished(partial, corr, levels_ref, put):
        ratio = plan.ratio(levels_ref)
        occupied = ratio > 0.0
        get = plan.slab_at(partial)

        def face(q, f, c):
            value = corr[q, plan.fb_rows(f, c), :]
            return jnp.where(occupied, (signs[f] * ratio) * value, 0.0)

        for x in range(E):
            for c in range(4):
                for q in range(2):
                    put(q, x, c, get(q, x, c) + plan.spread(face, q, x, c))

    def ghost_reader(gb, layers, levels_ref):
        occupied = occupied_of(levels_ref)
        return lambda q, f, c: jnp.where(
            occupied, gb[q, plan.fb_rows(f, c, True), :], layers(q, f, c)
        )

    def slab_put(ref):
        def put(q, x, c, value):
            ref[q, (x * 4 + c) * S : (x * 4 + c + 1) * S, :] = value

        return put

    def dyn_get(ref):
        return lambda q, rows: ref[q, rows, :]

    def dyn_put(ref):
        def put(q, rows, value):
            ref[q, rows, :] = value

        return put

    ghost_scratch = [vm(8, 3 * S * 8, COL), vm(3 * S * 8, COL), kind_scratch]

    def flux_cot_of(recv, row0, cot_fb, table_s, send_s, sums, kinds, flux_cot, back_r):
        for s in range(S):
            for f in range(6):
                row = ((f // 2) * S + s) * 8 + (f % 2) * 4
                kinds[row : row + 4, :] = jnp.full((4, COL), table_s[(s * 6 + f) * 8 + 4], jnp.int32)

        def face_out(f, c, wide):
            keep = kinds[plan.fb_rows(f, c), :] != 2
            for q in range(2):
                own = jnp.where(keep, cot_fb[q, plan.fb_rows(f, c), :], 0.0)
                flux_cot[q, (f * 4 + c) * S : (f * 4 + c + 1) * S, :] = own + wide[q]

        plan.take_quarters(recv, row0, send_s, sums, face_out, back_r)

    def flux_emitter(b_fb, ff):
        def emit(f, c, values):
            for q in range(2):
                b_fb[q, plan.fb_rows(f, c), :] = values[q]
                ff[q, (f * 4 + c) * S : (f * 4 + c + 1) * S, :] = values[q]

        return emit

    def cot_emitter(layer_cot, gcot):
        def emit(f, c, inner, outer):
            for q in range(2):
                layer_cot[q, (f * 4 + c) * S : (f * 4 + c + 1) * S, :] = inner[q]
                gcot[q, plan.fb_rows(f, c, True), :] = outer[q]

        return emit

    def carry_packets(source, out, row0):
        def one(peer, carry):
            for axis in range(3):
                tile(out, peer, row0 + axis * 4)[...] = tile(source, peer, axis * 4)[...]
            return carry

        lax.fori_loop(0, peers, one, 0)

    def add_layers(through, layer_cot, total, sums, put):
        own = plan.ff_at(layer_cot)
        for f in range(6):
            for c in range(4):
                for q in range(2):
                    added = sums[f][q, pl.ds((f % 2) * 4 + c, S, stride=8), :]
                    total[q, (f * 4 + c) * S : (f * 4 + c + 1) * S, :] = own(q, f, c) + added
        get = plan.slab_at(through)
        summed = plan.ff_at(total)
        for x in range(E):
            for c in range(4):
                for q in range(2):
                    put(q, x, c, get(q, x, c) + plan.spread(summed, q, x, c))

    def first_pack(send_s, parents_s, fields_r, guide_r, volume, layers, packets, fb):
        get = plan.native_at(fields_r.get())
        for x in range(E):
            for c in range(4):
                for q in range(2):
                    volume.ref[q, (x * 4 + c) * S : (x * 4 + c + 1) * S, :] = get(q, x, c)
        volume.send()
        layers_of(plan.slab_at(volume.ref), fb, layers.ref)
        layers.send()
        plan.pack_faces(fb, send_s, packets)
        planes = guide_r.get()
        plan.pack_octants(
            lambda s, x, q: planes[q][plan.native_rows(s, x), :], parents_s, packets.ref, 48
        )
        packets.send(48, 16)

    volume1, layers1, packets = run(
        first_pack,
        "first_pack",
        [send, parents],
        [Late(native_fields, native=True), Late(native_guidance, native=True)],
        [(plan.slab, "late"), (plan.ff, "late"), ((peers, 64, COL), "late")],
        [fb_scratch],
    )
    received1 = exchange(packets)

    def interior_first(levels_s, volume, partial, done):
        plan.interior(dyn_get(volume.get()), levels_s, dyn_put(partial.ref))
        partial.send()
        done[...] = jnp.zeros(done.shape, f32)

    partial1, done1 = run(
        interior_first, "interior_first", [levels], [Late(volume1)],
        [(plan.slab, "late"), ((8, COL), None)], [],
    )

    def first_flux(levels_s, send_s, table_s, layers, after, recv, half_r, back_r, gb, b_fb, packets,
                   planes, near, kinds, ff, rb):
        del after
        plan.ghosts(recv, table_s, planes, near, kinds, gb.ref, half_r, back_r)
        gb.send()
        layer = plan.ff_at(layers)
        boundary_fluxes(plan, layer, ghost_reader(gb.ref, layer, levels_s), flux_emitter(b_fb.ref, ff))
        b_fb.send()
        plan.pack_averages(plan.ff_at(ff), rb, send_s, packets, 0, half_r)

    ghosts1, fluxes1, packets = run(
        first_flux,
        "first_flux",
        [levels, send, table],
        [layers1, done1, received1, half, half_back],
        [(plan.fb, "late"), (plan.fb, "late"), ((peers, 3, 4, COL), None)],
        ghost_scratch + [vm(*plan.ff), vm(*plan.small)],
    )
    received2 = exchange(packets)

    def upward_second(levels_s, table_s, children_s, parents_s, guide_r, recv, back_r, up, cot_fb,
                      packets, cc):
        planes = guide_r.get()
        plan.upward(recv, 48, cc, children_s, parents_s, plan.native_at(planes), slab_put(up.ref), back_r)
        up.send()
        corrected_cot_of(plan.slab_at(up.ref), levels_s, cot_fb.ref)
        cot_fb.send()
        plan.pack_quarters(cot_fb.ref, table_s, packets.ref, 0)
        packets.send()

    up2, corrcot2, quarters2 = run(
        upward_second,
        "upward_second",
        [levels, table, children, parents],
        [Late(native_guidance, native=True), received1, half_back],
        [(plan.slab, "late"), (plan.fb, "late"), ((peers, 3, 4, COL), "late")],
        [vm((S + 1) * 32, COL)],
    )

    def first_update(levels_s, table_s, children_s, partial, b_fb, recv, quarters, half_r, updated,
                     packets, corr, cb):
        plan.corrected(b_fb, recv, 0, table_s, corr)
        finished(partial, corr, levels_s, slab_put(updated))
        plan.average_blocks(plan.slab_at(updated), cb, half_r)
        plan.pack_children(cb, children_s, packets, 0)
        carry_packets(quarters.get(), packets, 16)

    updated1, packets = run(
        first_update,
        "first_update",
        [levels, table, children],
        [partial1, fluxes1, received2, Late(quarters2), half],
        [(plan.slab, None), ((peers, 7, 4, COL), None)],
        [fb_scratch, vm(*plan.coarse)],
    )
    received3 = exchange(packets)

    def middle_pack(send_s, parents_s, updated, recv, volume, layers, packets, fb):
        volume.ref[...] = updated[...]

        def store(s, x, q, value):
            volume.ref[q, plan.slab_rows(s, x), :] = value

        plan.place_octants(recv, 0, parents_s, store)
        volume.send()
        layers_of(plan.slab_at(volume.ref), fb, layers.ref)
        layers.send()
        plan.pack_faces(fb, send_s, packets)

    volume2, layers2, packets = run(
        middle_pack,
        "middle_pack",
        [send, parents],
        [updated1, received3],
        [(plan.slab, "late"), (plan.ff, "late"), ((peers, 48, COL), "late")],
        [fb_scratch],
    )
    received4 = exchange(packets)

    def flux_cot_second(send_s, table_s, cot_fb, recv, back_r, flux_cot, kinds, *sums):
        flux_cot_of(recv, 16, cot_fb.get(), table_s, send_s, sums, kinds, flux_cot.ref, back_r)
        flux_cot.send()

    (fluxcot2,) = run(
        flux_cot_second,
        "flux_cot_second",
        [send, table],
        [Late(corrcot2), received3, half_back],
        [(plan.ff, "late")],
        [kind_scratch] + quarter_sums,
    )

    def interior_both(levels_s, volume, cot, partial, through):
        plan.interior(
            dyn_get(volume.get()), levels_s, dyn_put(partial.ref), dyn_get(cot.get()), dyn_put(through.ref)
        )
        partial.send()
        through.send()

    partial2, through2 = run(
        interior_both, "interior_both", [levels], [Late(volume2), Late(up2)],
        [(plan.slab, "late"), (plan.slab, "late")], [],
    )

    def second_pull(levels_s, table_s, layers, recv, flux_cot, half_r, back_r, gb, layer_cot,
                    packets, planes, near, kinds, gcot):
        plan.ghosts(recv, table_s, planes, near, kinds, gb.ref, half_r, back_r)
        gb.send()
        layer = plan.ff_at(layers)
        boundary_pull(
            plan, layer, ghost_reader(gb.ref, layer, levels_s), plan.ff_at(flux_cot.get()),
            cot_emitter(layer_cot.ref, gcot),
        )
        layer_cot.send()
        plan.pack_ghost_cot(gcot, table_s, planes, near, packets, half_r, back_r)

    ghosts2, layercot2, packets = run(
        second_pull,
        "second_pull",
        [levels, table],
        [layers2, received4, Late(fluxcot2), half, half_back],
        [(plan.fb, "late"), (plan.ff, "late"), ((peers, 48, COL), "late")],
        ghost_scratch + [fb_scratch],
    )
    received5 = exchange(packets)

    def second_flux(levels_s, send_s, layers, gb, half_r, b_fb, packets, ff, rb):
        layer = plan.ff_at(layers.get())
        boundary_fluxes(plan, layer, ghost_reader(gb.get(), layer, levels_s), flux_emitter(b_fb.ref, ff))
        b_fb.send()
        plan.pack_averages(plan.ff_at(ff), rb, send_s, packets.ref, 0, half_r)
        packets.send()

    fluxes2, averages2 = run(
        second_flux,
        "second_flux",
        [levels, send],
        [Late(layers2), Late(ghosts2), half],
        [(plan.fb, "late"), ((peers, 3, 4, COL), "late")],
        [vm(*plan.ff), vm(*plan.small)],
    )

    def middle_cot(send_s, parents_s, through, layer_cot, recv, averages, inner, packets, total, *sums):
        plan.take_faces(recv, send_s, sums)
        carry_packets(averages.get(), packets, 16)
        add_layers(through.get(), layer_cot.get(), total, sums, slab_put(inner))
        plan.pack_octants(
            lambda s, x, q: inner[q, plan.slab_rows(s, x), :], parents_s, packets, 0
        )

    inner_cot, packets = run(
        middle_cot,
        "middle_cot",
        [send, parents],
        [Late(through2), Late(layercot2), received5, Late(averages2)],
        [(plan.slab, None), ((peers, 7, 4, COL), None)],
        [vm(*plan.ff)] + face_sums,
    )
    received6 = exchange(packets)

    def upward_first(levels_s, table_s, children_s, parents_s, inner, recv, back_r, up, cot_fb,
                     packets, cc):
        plan.upward(
            recv, 0, cc, children_s, parents_s, plan.slab_at(inner), slab_put(up.ref), back_r
        )
        up.send()
        corrected_cot_of(plan.slab_at(up.ref), levels_s, cot_fb.ref)
        cot_fb.send()
        plan.pack_quarters(cot_fb.ref, table_s, packets, 0)

    up1, corrcot1, packets = run(
        upward_first,
        "upward_first",
        [levels, table, children, parents],
        [inner_cot, received6, half_back],
        [(plan.slab, "late"), (plan.fb, "late"), ((peers, 3, 4, COL), None)],
        [vm((S + 1) * 32, COL)],
    )
    received7 = exchange(packets)

    def second_update(levels_s, table_s, partial, b_fb, recv, half_r, final, cb, corr, updated, n0,
                      n1, sems):
        plan.corrected(b_fb.get(), recv, 16, table_s, corr)
        planes = [n0, n1]
        put_slab = slab_put(updated)

        def put(q, x, c, value):
            put_slab(q, x, c, value)
            planes[q][pl.ds(c * E + x, S, stride=4 * E), :] = value

        finished(partial.get(), corr, levels_s, put)
        copies = native_copies(planes, final, sems, False)
        for copy in copies:
            copy.start()
        plan.average_blocks(plan.slab_at(updated), cb, half_r)
        for copy in copies:
            copy.wait()

    final_open, coarse2 = run(
        second_update,
        "second_update",
        [levels, table],
        [Late(partial2), Late(fluxes2), received6, half],
        [(plan.native, "raw"), (plan.coarse, None)],
        [fb_scratch, vm(*plan.slab)] + native_planes + [pair_of_sems],
    )

    def interior_back(levels_s, volume, cot, through):
        plan.interior(
            dyn_get(volume.get()), levels_s, None, dyn_get(cot.get()), dyn_put(through.ref)
        )
        through.send()

    (through1,) = run(
        interior_back, "interior_back", [levels], [Late(volume1), Late(up1)],
        [(plan.slab, "late")], [],
    )

    def first_pull(levels_s, send_s, table_s, children_s, layers, gb, cot_fb, recv, coarse, half_r,
                   back_r, layer_cot, packets, planes, near, kinds, flux_cot, gcot, *sums):
        plan.pack_children(coarse, children_s, packets.ref, 48)
        packets.send(48, 16)
        flux_cot_of(recv, 0, cot_fb, table_s, send_s, sums, kinds, flux_cot, back_r)
        layer = plan.ff_at(layers)
        boundary_pull(
            plan, layer, ghost_reader(gb, layer, levels_s), plan.ff_at(flux_cot),
            cot_emitter(layer_cot.ref, gcot),
        )
        layer_cot.send()
        plan.pack_ghost_cot(gcot, table_s, planes, near, packets, half_r, back_r)

    layercot1, packets = run(
        first_pull,
        "first_pull",
        [levels, send, table, children],
        [layers1, ghosts1, corrcot1, received7, coarse2, half, half_back],
        [(plan.ff, "late"), ((peers, 64, COL), "late")],
        ghost_scratch + [vm(*plan.ff), fb_scratch] + quarter_sums,
    )
    received8 = exchange(packets)

    def last_cot(send_s, parents_s, through, layer_cot, recv, open_r, gradient, final, total, n0, n1,
                 p0, p1, sems, slot_sems, *sums):
        del open_r
        placed = [p0, p1]

        def store(s, x, q, value):
            placed[q][plan.native_rows(s, x), :] = value

        plan.place_octants(recv, 48, parents_s, store)

        def each_covered(act):
            for s in range(S):

                def one(s=s):
                    rows = (s * 4 * E, 4 * E)
                    for copy in native_copies(placed, final, slot_sems.at[s], False, rows):
                        act(copy)

                pl.when(parents_s[s, 0] >= 0)(one)

        each_covered(lambda copy: copy.start())
        plan.take_faces(recv, send_s, sums)
        planes = [n0, n1]

        def put(q, x, c, value):
            planes[q][pl.ds(c * E + x, S, stride=4 * E), :] = value

        add_layers(through.get(), layer_cot.get(), total, sums, put)
        copies = native_copies(planes, gradient, sems, False)
        for copy in copies:
            copy.start()
        for copy in copies:
            copy.wait()
        each_covered(lambda copy: copy.wait())

    gradient, final_fields = run(
        last_cot,
        "last_cot",
        [send, parents],
        [Late(through1), Late(layercot1), received8, Late(final_open, raw=True)],
        [(plan.native, "raw"), (plan.native, "raw")],
        [vm(*plan.ff)] + native_planes + native_planes
        + [pair_of_sems, pltpu.SemaphoreType.DMA((S, 2))] + face_sums,
        aliases={5: 1},
    )
    return (final_fields.reshape(fields.shape), gradient.reshape(fields.shape))


def solution(mesh):
    placed = (
        P("blk", None, None, None),
        P("blk", None, None, None),
        P("blk"),
        P("blk", None, None),
        P("blk", None, None),
        P("blk", None, None),
        P("blk", None),
        P("blk", None),
    )
    return jax.shard_map(
        on_device,
        mesh=mesh,
        in_specs=placed,
        out_specs=(P("blk", None, None, None), P("blk", None, None, None)),
        check_vma=False,
    )
```

```python
import jax
import jax.numpy as jnp
import numpy as np
from jax import lax
from jax.experimental import pallas as pl
from jax.experimental.pallas import tpu as pltpu
from jax.sharding import PartitionSpec as P

sound_speed = 1.0
base_ratio = 0.04
speed_floor = 0.01
f32 = jnp.float32
bf16 = jnp.bfloat16


def half_map(extent):
    half = extent // 2
    square = extent * extent
    table = np.zeros((2, extent, extent, half, 2, half), np.float32)
    for group in range(2):
        for i in range(extent):
            for j in range(extent):
                table[group, i, j, i // 2, group, j // 2] = 0.25
    return table.reshape(2 * square, square // 2)


def dot2(values, table):
    high = values.astype(bf16)
    low = (values - high.astype(f32)).astype(bf16)
    return jnp.dot(high, table, preferred_element_type=f32) + jnp.dot(
        low, table, preferred_element_type=f32
    )


def roll(values, shift):
    lanes = values.shape[1]
    shift = shift % lanes
    return values if shift == 0 else pltpu.roll(values, shift, 1)


def tile(packets, peer, row):
    return packets.at[peer, row // 4] if len(packets.shape) == 4 else packets.at[peer, row : row + 4]


def flux_of(behind, beyond, normal, inv_behind, inv_beyond):
    v = behind[1 + normal] * inv_behind
    w = beyond[1 + normal] * inv_beyond
    c = sound_speed + jnp.sqrt(0.5 * (v * v + w * w) + speed_floor)
    result = [0.5 * ((behind[1 + normal] + beyond[1 + normal]) - c * (beyond[0] - behind[0]))]
    for k in range(1, 4):
        total = behind[k] * v + beyond[k] * w
        if k == 1 + normal:
            total = total + (sound_speed * sound_speed) * (behind[0] + beyond[0])
        result.append(0.5 * (total - c * (beyond[k] - behind[k])))
    return result


def flux_pull(behind, beyond, normal, inv_behind, inv_beyond, cot):
    v = behind[1 + normal] * inv_behind
    w = beyond[1 + normal] * inv_beyond
    inside = 0.5 * (v * v + w * w) + speed_floor
    root = jnp.sqrt(inside)
    c = sound_speed + root
    half_cot = [0.5 * part for part in cot]
    jump = half_cot[0] * (beyond[0] - behind[0])
    v_cot = half_cot[1] * behind[1]
    w_cot = half_cot[1] * beyond[1]
    for k in range(1, 4):
        jump = jump + half_cot[k] * (beyond[k] - behind[k])
        if k > 1:
            v_cot = v_cot + half_cot[k] * behind[k]
            w_cot = w_cot + half_cot[k] * beyond[k]
    scale = jump * (-0.5) / root
    v_cot = (v_cot + scale * v) * inv_behind
    w_cot = (w_cot + scale * w) * inv_beyond
    plus = v + c
    minus = w - c
    behind_cot = []
    beyond_cot = []
    pressure = (sound_speed * sound_speed) * half_cot[1 + normal]
    for k in range(4):
        if k == 0:
            behind_cot.append(c * half_cot[0] + pressure - v_cot * v)
            beyond_cot.append(pressure - c * half_cot[0] - w_cot * w)
        else:
            left = half_cot[k] * plus
            right = half_cot[k] * minus
            if k == 1 + normal:
                left = left + half_cot[0] + v_cot
                right = right + half_cot[0] + w_cot
            behind_cot.append(left)
            beyond_cot.append(right)
    return behind_cot, beyond_cot


class Plan:
    def __init__(self, slots, extent, peers):
        self.S = slots
        self.E = extent
        self.P = peers
        self.H = extent // 2
        self.COL = extent * extent // 2
        self.slab = (2, extent * 4 * slots, self.COL)
        self.ff = (2, 6 * 4 * slots, self.COL)
        self.fb = (2, 3 * slots * 8, self.COL)
        self.native = (slots * 4 * extent, 2 * self.COL)
        self.coarse = (slots * 32, self.COL)
        self.small = (slots * 24, self.COL)

    def lane(self, rows):
        return lax.broadcasted_iota(jnp.int32, (rows, self.COL), 1)

    def low(self, rows):
        return (self.lane(rows) & (self.E - 1)) < self.H

    def per_slot(self, scalar_of):
        sub = lax.broadcasted_iota(jnp.int32, (self.S, self.COL), 0)
        value = jnp.zeros((self.S, self.COL), jnp.int32)
        for s in range(self.S):
            value = jnp.where(sub == s, scalar_of(s), value)
        return value

    def ratio(self, levels):
        level = self.per_slot(lambda s: levels[s])
        degree = level.astype(f32)
        ratio = base_ratio * (1.0 + degree + 0.5 * degree * (degree - 1.0))
        return jnp.where(level >= 0, ratio, 0.0)

    def slab_at(self, ref):
        return lambda q, x, c: ref[q, (x * 4 + c) * self.S : (x * 4 + c + 1) * self.S, :]

    def native_at(self, planes):
        step = 4 * self.E
        return lambda q, x, c: planes[q][pl.ds(c * self.E + x, self.S, stride=step), :]

    def ff_at(self, ref):
        return lambda q, f, c: ref[q, (f * 4 + c) * self.S : (f * 4 + c + 1) * self.S, :]

    def fb_rows(self, f, c, swapped=False):
        side = f % 2
        half = 1 - side if swapped else side
        return pl.ds((f // 2) * self.S * 8 + half * 4 + c, self.S, stride=8)

    def extract(self, get, c):
        E, H, COL = self.E, self.H, self.COL
        lane = self.lane(self.S)
        group = lax.shift_right_logical(lane, E.bit_length() - 1)
        within = lane & (E - 1)
        faces = [[get(q, 0, c) for q in range(2)], [get(q, E - 1, c) for q in range(2)]]
        low_y, high_y, low_z, high_z = [], [], [], []
        for q in range(2):
            first, last, near, far = None, None, None, None
            for k in range(H):
                a = roll(get(0, q * H + k, c), E * k)
                b = roll(get(1, q * H + k, c), E * k - (COL - E))
                first = a if first is None else jnp.where(group == k, a, first)
                last = b if last is None else jnp.where(group == k, b, last)
            for x in range(E):
                source = get(q, x, c)
                a = roll(source, x)
                b = roll(source, x - (E - 1))
                near = a if near is None else jnp.where(within == x, a, near)
                far = b if far is None else jnp.where(within == x, b, far)
            low_y.append(first)
            high_y.append(last)
            low_z.append(near)
            high_z.append(far)
        return faces + [low_y, high_y, low_z, high_z]

    def spread(self, face, q, x, c):
        E, H, COL = self.E, self.H, self.COL
        lane = self.lane(self.S)
        within = lane & (E - 1)
        k = x % H
        y_face = face(x // H, 2 + q, c)
        if q == 0:
            total = jnp.where(lane < E, roll(y_face, -E * k), 0.0)
        else:
            total = jnp.where(lane >= COL - E, roll(y_face, (COL - E) - E * k), 0.0)
        near = roll(face(q, 4, c), -x)
        far = roll(face(q, 5, c), E - 1 - x)
        total = total + jnp.where(within == 0, near, jnp.where(within == E - 1, far, 0.0))
        if x == 0:
            total = total + face(q, 0, c)
        if x == E - 1:
            total = total + face(q, 1, c)
        return total

    def pack_faces(self, fb, send, out):
        sub = lax.broadcasted_iota(jnp.int32, (8, self.COL), 0)
        for axis in range(3):

            def one(peer, carry, axis=axis):
                slots = [jnp.maximum(send[peer, axis * 2 + side], 0) for side in range(2)]
                for q in range(2):
                    lo, hi = [
                        fb[q, pl.ds(pl.multiple_of((axis * self.S + slot) * 8, 8), 8), :]
                        for slot in slots
                    ]
                    row = axis * 16 + q * 8
                    out.ref[peer, row : row + 8, :] = jnp.where(sub < 4, lo, hi)
                return carry

            lax.fori_loop(0, self.P, one, 0, unroll=4)
            out.send(axis * 16, 16)

    def take_faces(self, packets, send, sums):
        def one(peer, carry):
            for f in range(6):
                slot = jnp.maximum(send[peer, f], 0)
                rows = pl.ds(pl.multiple_of(slot * 8, 8), 8)
                for q in range(2):
                    at = (f // 2) * 16 + q * 8
                    sums[f * 2 + q][rows, :] += packets[peer, at : at + 8, :]
            return carry

        for part in sums:
            part[...] = jnp.zeros(part.shape, f32)
        lax.fori_loop(0, self.P, one, 0, unroll=4)

    def pack_averages(self, face, rb, send, out, row0, half):
        S, COL = self.S, self.COL
        rows = []
        for axis in range(3):
            for c in range(4):
                rows.append(
                    jnp.concatenate(
                        [face(q, 2 * axis + side, c) for side in range(2) for q in range(2)], axis=1
                    )
                )
        small = dot2(jnp.concatenate(rows, axis=0), half[...])
        for k in range(12):
            rb[pl.ds((k // 4) * 8 + k % 4, S, stride=24), :] = small[k * S : (k + 1) * S]
        low = self.low(4)

        def one(peer, carry):
            for axis in range(3):
                lo, hi = [
                    rb[pl.ds(pl.multiple_of(slot * 24 + axis * 8, 8), 4), :]
                    for slot in [jnp.maximum(send[peer, axis * 2 + side], 0) for side in range(2)]
                ]
                tile(out, peer, row0 + axis * 4)[...] = jnp.where(low, lo, hi)
            return carry

        lax.fori_loop(0, self.P, one, 0, unroll=4)

    def pack_quarters(self, fb, table, out, row0):
        E, H = self.E, self.H
        low = self.low(4)

        def clear(peer, carry):
            for axis in range(3):
                tile(out, peer, row0 + axis * 4)[...] = jnp.zeros((4, self.COL), f32)
            return carry

        lax.fori_loop(0, self.P, clear, 0, unroll=4)
        for s in range(self.S):
            for f in range(6):
                base = (s * 6 + f) * 8

                def send_quarters(s=s, f=f, base=base):
                    axis, side = f // 2, f % 2
                    keep = low if side == 1 else jnp.logical_not(low)
                    row = (axis * self.S + s) * 8 + side * 4
                    at = row0 + axis * 4
                    for h in range(2):
                        values = fb[h, row : row + 4, :]
                        for g in range(2):
                            moved = roll(values, H * ((1 - side) - g))
                            peer = table[base + h * 2 + g]
                            tile(out, peer, at)[...] += jnp.where(keep, moved, 0.0)

                pl.when(table[base + 4] == 2)(send_quarters)

    def take_quarters(self, packets, row0, send, sums, face_out, half_back):
        S, COL = self.S, self.COL

        def one(peer, carry):
            for axis in range(3):
                block = tile(packets, peer, row0 + axis * 4)[...]
                for f in (axis * 2, axis * 2 + 1):
                    slot = jnp.maximum(send[peer, f], 0)
                    sums[f][pl.ds(pl.multiple_of(slot * 8, 8), 4), :] += block
            return carry

        for f in range(6):
            sums[f][...] = jnp.zeros(sums[f].shape, f32)
        lax.fori_loop(0, self.P, one, 0, unroll=4)
        for f in range(6):
            side = f % 2
            rows = jnp.concatenate(
                [sums[f][pl.ds(c, S, stride=8), :] for c in range(4)], axis=0
            )
            wide = dot2(rows, half_back[:, side * 2 * COL : (side + 1) * 2 * COL])
            for c in range(4):
                face_out(f, c, [wide[c * S : (c + 1) * S, q * COL : (q + 1) * COL] for q in range(2)])

    def ghosts(self, packets, table, planes, near, kinds, gb, half, half_back):
        S, COL, H = self.S, self.COL, self.H
        for s in range(S):
            for f in range(6):
                base = (s * 6 + f) * 8
                axis, half_row = f // 2, (1 - f % 2) * 4
                row = (axis * S + s) * 8 + half_row
                first = None
                for k in range(4):
                    peer = table[base + k]
                    got = []
                    for q in range(2):
                        at = axis * 16 + q * 8 + half_row
                        values = packets[peer, at : at + 4, :]
                        planes[k * 2 + q, row : row + 4, :] = values
                        got.append(values)
                    if k == 0:
                        first = got
                source = jnp.where(table[base + 5] == 1, first[1], first[0])
                source = jnp.where(table[base + 6] == 1, roll(source, -H), source)
                near[row : row + 4, :] = source
                kinds[row : row + 4, :] = jnp.full((4, COL), table[base + 4], jnp.int32)
        for axis in range(3):
            rows = slice(axis * S * 8, (axis + 1) * S * 8)
            kind = kinds[rows, :]
            coarse = 4.0 * dot2(near[rows, :], half_back[:, : 2 * COL])
            for h in range(2):
                parts = [planes[(h * 2 + g) * 2 + q, rows, :] for g in range(2) for q in range(2)]
                fine = dot2(jnp.concatenate(parts, axis=1), half[...])
                value = jnp.where(kind == 1, coarse[:, h * COL : (h + 1) * COL], planes[h, rows, :])
                gb[h, rows, :] = jnp.where(kind == 2, fine, value)

    def pack_ghost_cot(self, gb, table, wide, near, out, parts, half, half_back):
        S, COL, H = self.S, self.COL, self.H
        low = self.low(4)

        def clear(peer, carry):
            for part in parts:
                part[peer, :, :] = jnp.zeros((24, COL), f32)
            return carry

        lax.fori_loop(0, self.P, clear, 0, unroll=4)
        for h in range(2):
            for g in range(2):
                spread = dot2(gb[h, :, :], half_back[:, g * 2 * COL : (g + 1) * 2 * COL])
                for q in range(2):
                    wide[(h * 2 + g) * 2 + q, :, :] = spread[:, q * COL : (q + 1) * COL]
        both = jnp.concatenate([gb[0, :, :], gb[1, :, :]], axis=1)
        near[...] = 4.0 * dot2(both, half[0 : 2 * COL, :])
        for f in range(6):
            for s in range(S):
                base = (s * 6 + f) * 8
                axis, half_row = f // 2, (1 - f % 2) * 4
                row = (axis * S + s) * 8 + half_row
                kind = table[base + 4]

                def same(base=base, axis=axis, half_row=half_row, row=row):
                    peer = table[base]
                    for q in range(2):
                        at = axis * 8 + half_row
                        parts[q][peer, at : at + 4, :] += gb[q, row : row + 4, :]

                def coarse(base=base, axis=axis, half_row=half_row, row=row):
                    peer = table[base]
                    values = near[row : row + 4, :]
                    values = jnp.where(table[base + 6] == 1, roll(values, H), values)
                    for q in range(2):
                        at = axis * 8 + half_row
                        parts[q][peer, at : at + 4, :] += jnp.where(table[base + 5] == q, values, 0.0)

                def fine(base=base, axis=axis, half_row=half_row, row=row):
                    for k in range(4):
                        peer = table[base + k]
                        for q in range(2):
                            at = axis * 8 + half_row
                            parts[q][peer, at : at + 4, :] += wide[k * 2 + q, row : row + 4, :]

                pl.when(kind == 0)(same)
                pl.when(kind == 1)(coarse)
                pl.when(kind == 2)(fine)
            if f % 2 == 1:
                for q in range(2):
                    out.send((f // 2) * 16 + q * 8, 8, parts[q], (f // 2) * 8)

    def corrected(self, b_fb, packets, row0, table, out):
        H = self.H
        low = self.low(4)
        out[...] = b_fb[...]
        for s in range(self.S):
            for f in range(6):
                base = (s * 6 + f) * 8

                def replace(s=s, f=f, base=base):
                    axis, side = f // 2, f % 2
                    row = (axis * self.S + s) * 8 + side * 4
                    at = row0 + axis * 4
                    for h in range(2):
                        got = []
                        for g in range(2):
                            values = tile(packets, table[base + h * 2 + g], at)[...]
                            got.append(roll(values, H * (g - (1 - side))))
                        out[h, row : row + 4, :] = jnp.where(low, got[0], got[1])

                pl.when(table[base + 4] == 2)(replace)

    def pack_octants(self, load, parents, out, row0):
        H = self.H
        low = self.low(4)
        for s in range(self.S):

            def send(s=s):
                for ox in range(2):
                    for oy in range(2):
                        peers = [parents[s, ox * 4 + oy * 2 + oz] for oz in range(2)]
                        for pair in range(H // 2):
                            x = ox * H + pair * 2
                            first, second = load(s, x, oy), load(s, x + 1, oy)
                            at = row0 + pair * 4
                            tile(out, peers[0], at)[...] = jnp.where(low, first, roll(second, H))
                            tile(out, peers[1], at)[...] = jnp.where(low, roll(first, -H), second)

            pl.when(parents[s, 0] >= 0)(send)

    def place_octants(self, packets, row0, parents, store):
        H = self.H
        low = self.low(4)
        for s in range(self.S):

            def place(s=s):
                for ox in range(2):
                    for oy in range(2):
                        peers = [parents[s, ox * 4 + oy * 2 + oz] for oz in range(2)]
                        for pair in range(H // 2):
                            x = ox * H + pair * 2
                            at = row0 + pair * 4
                            first = tile(packets, peers[0], at)[...]
                            second = tile(packets, peers[1], at)[...]
                            store(s, x, oy, jnp.where(low, first, roll(second, H)))
                            store(s, x + 1, oy, jnp.where(low, roll(first, -H), second))

            pl.when(parents[s, 0] >= 0)(place)

    def slab_rows(self, s, x):
        return pl.ds(x * 4 * self.S + s, 4, stride=self.S)

    def native_rows(self, s, x):
        return pl.ds(s * 4 * self.E + x, 4, stride=self.E)

    def average_blocks(self, get, cb, half):
        S = self.S
        rows = []
        for pair in range(self.E // 4):
            for c in range(4):
                x = 4 * pair
                rows.append(
                    jnp.concatenate(
                        [get(q, x + 2 * a, c) + get(q, x + 2 * a + 1, c) for a in range(2) for q in range(2)],
                        axis=1,
                    )
                )
        small = 0.5 * dot2(jnp.concatenate(rows, axis=0), half[...])
        for k in range(16):
            cb[pl.ds((k // 4) * 8 + k % 4, S, stride=32), :] = small[k * S : (k + 1) * S]

    def pack_children(self, cb, children, out, row0):
        def one(peer, carry):
            slot = jnp.maximum(children[peer], 0)
            for part in range(4):
                rows = pl.ds(pl.multiple_of(slot * 32 + part * 8, 8), 4)
                tile(out, peer, row0 + part * 4)[...] = cb[rows, :]
            return carry

        lax.fori_loop(0, self.P, one, 0, unroll=4)

    def upward(self, packets, row0, cc, children, parents, get, put, half_back):
        S, COL = self.S, self.COL
        cc[...] = jnp.zeros(cc.shape, f32)

        def one(peer, carry):
            child = children[peer]
            slot = jnp.where(child < 0, S, child)
            for part in range(4):
                rows = pl.ds(pl.multiple_of(slot * 32 + part * 8, 8), 4)
                cc[rows, :] += tile(packets, peer, row0 + part * 4)[...]
            return carry

        lax.fori_loop(0, self.P, one, 0, unroll=4)
        rows = jnp.concatenate(
            [cc[pl.ds((k // 4) * 8 + k % 4, S, stride=32), :] for k in range(16)], axis=0
        )
        wide = 0.5 * dot2(rows, half_back[...])
        covered = self.per_slot(lambda s: parents[s, 0]) >= 0
        for x in range(self.E):
            for c in range(4):
                row = ((x // 4) * 4 + c) * S
                for q in range(2):
                    lane0 = ((x // 2) % 2 * 2 + q) * COL
                    added = wide[row : row + S, lane0 : lane0 + COL]
                    put(q, x, c, jnp.where(covered, 0.0, get(q, x, c)) + added)

    def shifted(self, planes, amount):
        COL = self.COL
        lane = self.lane(self.S)
        moved = [roll(values, amount) for values in planes]
        if amount > 0:
            return [jnp.where(lane < amount, moved[1 - q], moved[q]) for q in range(2)]
        return [jnp.where(lane >= COL + amount, moved[1 - q], moved[q]) for q in range(2)]

    def interior(self, get, levels, forward_put, cot_get=None, cot_put=None):
        S, E, COL = self.S, self.E, self.COL
        ratio = self.ratio(levels)
        lane = self.lane(S)
        y_inside = [lane >= 0, lane < COL - E]
        z_inside = (lane & (E - 1)) != E - 1
        zero = jnp.zeros((S, COL), f32)

        def row_of(x, c):
            return pl.ds(pl.multiple_of((x * 4 + c) * S, S), S)

        def one(x, carry):
            after = jnp.minimum(x + 1, E - 1)
            x_inside = x < E - 1
            here = [[get(q, row_of(x, c)) for c in range(4)] for q in range(2)]
            inverse = [1.0 / here[q][0] for q in range(2)]
            ahead = [[get(q, row_of(after, c)) for c in range(4)] for q in range(2)]
            ahead_inv = [1.0 / ahead[q][0] for q in range(2)]
            flux_carry, cot_carry = carry
            new_flux, new_cot = [], []
            change = [[None] * 4 for _ in range(2)]
            if cot_get is not None:
                weight = [[get_c(q, row_of(x, c)) for c in range(4)] for q in range(2)]
                scaled = [[ratio * weight[q][c] for c in range(4)] for q in range(2)]
                ahead_scaled = [
                    [ratio * get_c(q, row_of(after, c)) for c in range(4)] for q in range(2)
                ]
                back = [[weight[q][c] for c in range(4)] for q in range(2)]
            for q in range(2):
                if forward_put is not None:
                    flux = flux_of(here[q], ahead[q], 0, inverse[q], ahead_inv[q])
                    flux = [jnp.where(x_inside, part, 0.0) for part in flux]
                    change[q] = [flux[c] - flux_carry[q * 4 + c] for c in range(4)]
                    new_flux += flux
                if cot_get is not None:
                    cot = [
                        jnp.where(x_inside, ahead_scaled[q][c] - scaled[q][c], 0.0) for c in range(4)
                    ]
                    left, right = flux_pull(here[q], ahead[q], 0, inverse[q], ahead_inv[q], cot)
                    back[q] = [back[q][c] + left[c] + cot_carry[q * 4 + c] for c in range(4)]
                    new_cot += right
            for normal, step, inside in ((1, E, y_inside), (2, 1, [z_inside, z_inside])):
                turned = [self.shifted([here[q][c] for q in range(2)], -step) for c in range(4)]
                turned_inv = self.shifted(inverse, -step)
                beyond = [[turned[c][q] for c in range(4)] for q in range(2)]
                if forward_put is not None:
                    flux = []
                    for q in range(2):
                        got = flux_of(here[q], beyond[q], normal, inverse[q], turned_inv[q])
                        flux.append([jnp.where(inside[q], part, 0.0) for part in got])
                    for c in range(4):
                        behind = self.shifted([flux[q][c] for q in range(2)], step)
                        for q in range(2):
                            change[q][c] = change[q][c] + (flux[q][c] - behind[q])
                if cot_get is not None:
                    turned_w = [self.shifted([scaled[q][c] for q in range(2)], -step) for c in range(4)]
                    rights = []
                    for q in range(2):
                        cot = [
                            jnp.where(inside[q], turned_w[c][q] - scaled[q][c], 0.0) for c in range(4)
                        ]
                        left, right = flux_pull(here[q], beyond[q], normal, inverse[q], turned_inv[q], cot)
                        back[q] = [back[q][c] + left[c] for c in range(4)]
                        rights.append(right)
                    for c in range(4):
                        moved = self.shifted([rights[q][c] for q in range(2)], step)
                        for q in range(2):
                            back[q][c] = back[q][c] + moved[q]
            for q in range(2):
                for c in range(4):
                    if forward_put is not None:
                        forward_put(q, row_of(x, c), here[q][c] - ratio * change[q][c])
                    if cot_get is not None:
                        cot_put(q, row_of(x, c), back[q][c])
            return (new_flux, new_cot)

        get_c = cot_get
        start = (
            [zero] * 8 if forward_put is not None else [],
            [zero] * 8 if cot_get is not None else [],
        )
        lax.fori_loop(0, E, one, start)


class Arriving:
    def __init__(self, copies, ref):
        self.copies = copies
        self.ref = ref
        for copy in copies:
            copy.start()

    def get(self):
        for copy in self.copies:
            copy.wait()
        self.copies = []
        return self.ref


class Leaving:
    def __init__(self, ref, target, sems):
        self.ref = ref
        self.target = target
        self.sems = sems
        self.copies = []

    def send(self, first=None, count=None, ref=None, start=None):
        near, far = self.ref if ref is None else ref, self.target
        if count is not None:
            near = near.at[:, pl.ds(first if start is None else start, count), :]
            far = far.at[:, pl.ds(first, count), :]
        copy = pltpu.make_async_copy(near, far, self.sems.at[len(self.copies)])
        copy.start()
        self.copies.append(copy)

    def finish(self):
        for copy in self.copies:
            copy.wait()


class Late:
    def __init__(self, array, native=False, raw=False):
        self.array = array
        self.native = native
        self.raw = raw


def run(body, name, scalars, arrays, outs, scratch, aliases=None):
    hbm = pltpu.MemorySpace.HBM
    specs = [pl.BlockSpec(memory_space=pltpu.SMEM) for _ in scalars]
    operands = list(scalars)
    extra = []
    arriving, leaving = {}, {}
    for index, item in enumerate(arrays):
        if isinstance(item, Late):
            specs.append(pl.BlockSpec(memory_space=hbm))
            operands.append(pltpu.with_memory_space_constraint(item.array, hbm))
            if not item.raw:
                shape = item.array.shape
                arriving[index] = (len(extra), item.native)
                if item.native:
                    half = (shape[0], shape[1] // 2)
                    extra += [pltpu.VMEM(half, f32), pltpu.VMEM(half, f32)]
                    extra.append(pltpu.SemaphoreType.DMA((2,)))
                else:
                    extra += [pltpu.VMEM(shape, f32), pltpu.SemaphoreType.DMA((1,))]
        else:
            specs.append(pl.BlockSpec(memory_space=pltpu.VMEM))
            operands.append(item)
    out_specs = []
    for index, (shape, mode) in enumerate(outs):
        out_specs.append(pl.BlockSpec(memory_space=hbm if mode else pltpu.VMEM))
        if mode == "late":
            leaving[index] = len(extra)
            extra += [pltpu.VMEM(shape, f32), pltpu.SemaphoreType.DMA((8,))]

    def wrapped(*refs):
        n_scalar, n_in, n_out = len(scalars), len(arrays), len(outs)
        scalar_refs = list(refs[:n_scalar])
        in_refs = list(refs[n_scalar : n_scalar + n_in])
        out_refs = list(refs[n_scalar + n_in : n_scalar + n_in + n_out])
        rest = refs[n_scalar + n_in + n_out :]
        own, late = rest[: len(scratch)], rest[len(scratch) :]
        for index, (at, native) in arriving.items():
            if native:
                planes = [late[at], late[at + 1]]
                copies = native_copies(planes, in_refs[index], late[at + 2], True)
                in_refs[index] = Arriving(copies, planes)
            else:
                copy = pltpu.make_async_copy(in_refs[index], late[at], late[at + 1].at[0])
                in_refs[index] = Arriving([copy], late[at])
        for index, at in leaving.items():
            out_refs[index] = Leaving(late[at], out_refs[index], late[at + 1])
        body(*scalar_refs, *in_refs, *out_refs, *own)
        for index in arriving:
            in_refs[index].get()
        for index in leaving:
            out_refs[index].finish()

    return pl.pallas_call(
        wrapped,
        name=name,
        in_specs=specs,
        out_specs=out_specs,
        out_shape=[
            hbm(shape, f32) if mode else jax.ShapeDtypeStruct(shape, f32) for shape, mode in outs
        ],
        scratch_shapes=list(scratch) + extra,
        input_output_aliases=aliases or {},
        compiler_params=pltpu.CompilerParams(vmem_limit_bytes=32 * 1024 * 1024),
    )(*operands)


def native_copies(planes, whole, sems, inward, rows=None):
    lanes = planes[0].shape[1]
    copies = []
    for q in range(2):
        part = whole.at[:, pl.ds(q * lanes, lanes)]
        near = planes[q]
        if rows is not None:
            part = whole.at[pl.ds(*rows), pl.ds(q * lanes, lanes)]
            near = planes[q].at[pl.ds(*rows), :]
        source, target = (part, near) if inward else (near, part)
        copies.append(pltpu.make_async_copy(source, target, sems.at[q]))
    return copies


def boundary_fluxes(plan, layers, ghost, emit):
    for f in range(6):
        result = []
        for q in range(2):
            inner = [layers(q, f, c) for c in range(4)]
            outer = [ghost(q, f, c) for c in range(4)]
            inner_inv, outer_inv = 1.0 / inner[0], 1.0 / outer[0]
            if f % 2 == 0:
                result.append(flux_of(outer, inner, f // 2, outer_inv, inner_inv))
            else:
                result.append(flux_of(inner, outer, f // 2, inner_inv, outer_inv))
        for c in range(4):
            emit(f, c, [result[q][c] for q in range(2)])


def boundary_pull(plan, layers, ghost, cot, emit):
    for f in range(6):
        result = []
        for q in range(2):
            inner = [layers(q, f, c) for c in range(4)]
            outer = [ghost(q, f, c) for c in range(4)]
            weight = [cot(q, f, c) for c in range(4)]
            inner_inv, outer_inv = 1.0 / inner[0], 1.0 / outer[0]
            if f % 2 == 0:
                out_cot, in_cot = flux_pull(outer, inner, f // 2, outer_inv, inner_inv, weight)
            else:
                in_cot, out_cot = flux_pull(inner, outer, f // 2, inner_inv, outer_inv, weight)
            result.append((in_cot, out_cot))
        for c in range(4):
            emit(f, c, [result[q][0][c] for q in range(2)], [result[q][1][c] for q in range(2)])


def on_device(fields, guidance, levels, send_faces, ghost_peer, ghost_code, child_send, parent_peer):
    slots, _, extent, square = fields.shape
    peers = send_faces.shape[1]
    plan = Plan(slots, extent, peers)
    S, E, COL = slots, extent, plan.COL
    half_np = half_map(extent)
    half = jnp.asarray(half_np, bf16)
    half_back = jnp.asarray(np.ascontiguousarray(half_np.T), bf16)

    first_map, second_map = ghost_code // 5, ghost_code % 5
    turned = (jnp.arange(6) >= 4)[None, :, None]
    major = jnp.where(turned, second_map, first_map)
    minor = jnp.where(turned, first_map, second_map)
    refined = ghost_peer[:, :, 1] >= 0
    quarter = (major - 3) * 2 + (minor - 3)
    chosen = jnp.maximum(ghost_peer, 0)
    columns = [
        jnp.where(refined, jnp.sum(jnp.where(quarter == k, chosen, 0), axis=2), chosen[:, :, 0])
        for k in range(4)
    ]
    coarser = ghost_code[:, :, 0] > 0
    kind = jnp.where(
        ghost_peer[:, :, 0] < 0, 3, jnp.where(refined, 2, jnp.where(coarser, 1, 0))
    )
    single = jnp.logical_and(coarser, jnp.logical_not(refined))
    columns += [
        kind,
        jnp.where(single, major[:, :, 0] - 1, 0),
        jnp.where(single, minor[:, :, 0] - 1, 0),
        jnp.zeros_like(kind),
    ]
    table = jnp.stack(columns, axis=-1).astype(jnp.int32).reshape(-1)
    send = send_faces.reshape(peers, 6)
    children = child_send.reshape(-1)
    parents = parent_peer
    native_fields = fields.reshape(plan.native)
    native_guidance = guidance.reshape(plan.native)

    def exchange(packets):
        return lax.all_to_all(packets, "blk", split_axis=0, concat_axis=0, tiled=True)

    def vm(*shape):
        return pltpu.VMEM(shape, f32)

    def occupied_of(levels_ref):
        return plan.per_slot(lambda s: levels_ref[s]) >= 0

    fb_scratch = vm(*plan.fb)
    kind_scratch = pltpu.VMEM((3 * S * 8, COL), jnp.int32)
    native_planes = [vm(S * 4 * E, COL), vm(S * 4 * E, COL)]
    pair_of_sems = pltpu.SemaphoreType.DMA((2,))
    quarter_sums = [vm(S * 8, COL) for _ in range(6)]
    face_sums = [vm(S * 8, COL) for _ in range(12)]
    cot_halves = [vm(peers, 24, COL) for _ in range(2)]
    signs = [1.0, -1.0, 1.0, -1.0, 1.0, -1.0]

    def layers_of(get, fb, ff):
        for c in range(4):
            faces = plan.extract(get, c)
            for f in range(6):
                for q in range(2):
                    if fb is not None:
                        fb[q, plan.fb_rows(f, c), :] = faces[f][q]
                    if ff is not None:
                        ff[q, (f * 4 + c) * S : (f * 4 + c + 1) * S, :] = faces[f][q]

    def corrected_cot_of(get, levels_ref, fb):
        ratio = plan.ratio(levels_ref)
        for c in range(4):
            faces = plan.extract(get, c)
            for f in range(6):
                for q in range(2):
                    fb[q, plan.fb_rows(f, c), :] = (signs[f] * ratio) * faces[f][q]

    def finished(partial, corr, levels_ref, put):
        ratio = plan.ratio(levels_ref)
        occupied = ratio > 0.0
        get = plan.slab_at(partial)

        def face(q, f, c):
            value = corr[q, plan.fb_rows(f, c), :]
            return jnp.where(occupied, (signs[f] * ratio) * value, 0.0)

        for x in range(E):
            for c in range(4):
                for q in range(2):
                    put(q, x, c, get(q, x, c) + plan.spread(face, q, x, c))

    def ghost_reader(gb, layers, levels_ref):
        occupied = occupied_of(levels_ref)
        return lambda q, f, c: jnp.where(
            occupied, gb[q, plan.fb_rows(f, c, True), :], layers(q, f, c)
        )

    def slab_put(ref):
        def put(q, x, c, value):
            ref[q, (x * 4 + c) * S : (x * 4 + c + 1) * S, :] = value

        return put

    def dyn_get(ref):
        return lambda q, rows: ref[q, rows, :]

    def dyn_put(ref):
        def put(q, rows, value):
            ref[q, rows, :] = value

        return put

    ghost_scratch = [vm(8, 3 * S * 8, COL), vm(3 * S * 8, COL), kind_scratch]

    def flux_cot_of(recv, row0, cot_fb, table_s, send_s, sums, kinds, flux_cot, back_r):
        for s in range(S):
            for f in range(6):
                row = ((f // 2) * S + s) * 8 + (f % 2) * 4
                kinds[row : row + 4, :] = jnp.full((4, COL), table_s[(s * 6 + f) * 8 + 4], jnp.int32)

        def face_out(f, c, wide):
            keep = kinds[plan.fb_rows(f, c), :] != 2
            for q in range(2):
                own = jnp.where(keep, cot_fb[q, plan.fb_rows(f, c), :], 0.0)
                flux_cot[q, (f * 4 + c) * S : (f * 4 + c + 1) * S, :] = own + wide[q]

        plan.take_quarters(recv, row0, send_s, sums, face_out, back_r)

    def flux_emitter(b_fb, ff):
        def emit(f, c, values):
            for q in range(2):
                b_fb[q, plan.fb_rows(f, c), :] = values[q]
                ff[q, (f * 4 + c) * S : (f * 4 + c + 1) * S, :] = values[q]

        return emit

    def cot_emitter(layer_cot, gcot):
        def emit(f, c, inner, outer):
            for q in range(2):
                layer_cot[q, (f * 4 + c) * S : (f * 4 + c + 1) * S, :] = inner[q]
                gcot[q, plan.fb_rows(f, c, True), :] = outer[q]

        return emit

    def carry_packets(source, out, row0):
        def one(peer, carry):
            for axis in range(3):
                tile(out, peer, row0 + axis * 4)[...] = tile(source, peer, axis * 4)[...]
            return carry

        lax.fori_loop(0, peers, one, 0, unroll=4)

    def add_layers(through, layer_cot, total, sums, put):
        own = plan.ff_at(layer_cot)
        for f in range(6):
            for c in range(4):
                for q in range(2):
                    added = sums[f * 2 + q][pl.ds((f % 2) * 4 + c, S, stride=8), :]
                    total[q, (f * 4 + c) * S : (f * 4 + c + 1) * S, :] = own(q, f, c) + added
        get = plan.slab_at(through)
        summed = plan.ff_at(total)
        for x in range(E):
            for c in range(4):
                for q in range(2):
                    put(q, x, c, get(q, x, c) + plan.spread(summed, q, x, c))

    def first_pack(send_s, parents_s, fields_r, guide_r, volume, layers, packets, fb):
        get = plan.native_at(fields_r.get())
        for x in range(E):
            for c in range(4):
                for q in range(2):
                    volume[q, (x * 4 + c) * S : (x * 4 + c + 1) * S, :] = get(q, x, c)
        layers_of(plan.slab_at(volume), fb, layers.ref)
        layers.send()
        plan.pack_faces(fb, send_s, packets)
        planes = guide_r.get()
        plan.pack_octants(
            lambda s, x, q: planes[q][plan.native_rows(s, x), :], parents_s, packets.ref, 48
        )
        packets.send(48, 16)

    state1, layers1, packets = run(
        first_pack,
        "first_pack",
        [send, parents],
        [Late(native_fields, native=True), Late(native_guidance, native=True)],
        [(plan.slab, None), (plan.ff, "late"), ((peers, 64, COL), "late")],
        [fb_scratch],
    )
    received1 = exchange(packets)

    def interior_first(levels_s, volume, guide_r, partial, kept, guide_slab, done, sems):
        copy = pltpu.make_async_copy(volume, kept, sems.at[0])
        copy.start()
        get = plan.native_at(guide_r.get())
        put = slab_put(guide_slab.ref)
        for x in range(E):
            for c in range(4):
                for q in range(2):
                    put(q, x, c, get(q, x, c))
        guide_slab.send()
        plan.interior(dyn_get(volume), levels_s, dyn_put(partial.ref))
        partial.send()
        done[...] = jnp.zeros(done.shape, f32)
        copy.wait()

    partial1, volume1, guide1, done1 = run(
        interior_first, "interior_first", [levels],
        [state1, Late(native_guidance, native=True)],
        [(plan.slab, "late"), (plan.slab, "raw"), (plan.slab, "late"), ((8, COL), None)],
        [pair_of_sems],
    )

    def first_flux(levels_s, send_s, table_s, layers, after, recv, half_r, back_r, gb, b_fb, packets,
                   planes, near, kinds, ff, rb):
        del after
        plan.ghosts(recv, table_s, planes, near, kinds, gb.ref, half_r, back_r)
        gb.send()
        layer = plan.ff_at(layers)
        boundary_fluxes(plan, layer, ghost_reader(gb.ref, layer, levels_s), flux_emitter(b_fb.ref, ff))
        b_fb.send()
        plan.pack_averages(plan.ff_at(ff), rb, send_s, packets, 0, half_r)

    ghosts1, fluxes1, packets = run(
        first_flux,
        "first_flux",
        [levels, send, table],
        [layers1, done1, received1, half, half_back],
        [(plan.fb, "late"), (plan.fb, "late"), ((peers, 3, 4, COL), None)],
        ghost_scratch + [vm(*plan.ff), vm(*plan.small)],
    )
    received2 = exchange(packets)

    def upward_second(levels_s, table_s, children_s, parents_s, guide_r, recv, back_r, up, cot_fb,
                      packets, cc):
        plan.upward(recv, 48, cc, children_s, parents_s, plan.slab_at(guide_r), slab_put(up.ref), back_r)
        up.send()
        corrected_cot_of(plan.slab_at(up.ref), levels_s, cot_fb.ref)
        cot_fb.send()
        plan.pack_quarters(cot_fb.ref, table_s, packets.ref, 0)
        packets.send()

    up2, corrcot2, quarters2 = run(
        upward_second,
        "upward_second",
        [levels, table, children, parents],
        [guide1, received1, half_back],
        [(plan.slab, "late"), (plan.fb, "late"), ((peers, 3, 4, COL), "late")],
        [vm((S + 1) * 32, COL)],
    )

    def first_update(levels_s, table_s, children_s, partial, b_fb, recv, quarters, half_r, updated,
                     packets, corr, cb):
        plan.corrected(b_fb, recv, 0, table_s, corr)
        finished(partial, corr, levels_s, slab_put(updated))
        plan.average_blocks(plan.slab_at(updated), cb, half_r)
        plan.pack_children(cb, children_s, packets, 0)
        carry_packets(quarters.get(), packets, 16)

    updated1, packets = run(
        first_update,
        "first_update",
        [levels, table, children],
        [partial1, fluxes1, received2, Late(quarters2), half],
        [(plan.slab, None), ((peers, 7, 4, COL), None)],
        [fb_scratch, vm(*plan.coarse)],
    )
    received3 = exchange(packets)

    def middle_pack(send_s, parents_s, updated, recv, volume, layers, packets, fb):
        volume[...] = updated[...]

        def store(s, x, q, value):
            volume[q, plan.slab_rows(s, x), :] = value

        plan.place_octants(recv, 0, parents_s, store)
        layers_of(plan.slab_at(volume), fb, layers.ref)
        layers.send()
        plan.pack_faces(fb, send_s, packets)

    volume2, layers2, packets = run(
        middle_pack,
        "middle_pack",
        [send, parents],
        [updated1, received3],
        [(plan.slab, None), (plan.ff, "late"), ((peers, 48, COL), "late")],
        [fb_scratch],
    )
    received4 = exchange(packets)

    def flux_cot_second(send_s, table_s, cot_fb, recv, back_r, flux_cot, kinds, *sums):
        flux_cot_of(recv, 16, cot_fb.get(), table_s, send_s, sums, kinds, flux_cot.ref, back_r)
        flux_cot.send()

    (fluxcot2,) = run(
        flux_cot_second,
        "flux_cot_second",
        [send, table],
        [Late(corrcot2), received3, half_back],
        [(plan.ff, "late")],
        [kind_scratch] + quarter_sums,
    )

    def interior_both(levels_s, volume, cot, partial, through, done):
        plan.interior(
            dyn_get(volume), levels_s, dyn_put(partial.ref), dyn_get(cot.get()), dyn_put(through.ref)
        )
        partial.send()
        through.send()
        done[...] = jnp.zeros(done.shape, f32)

    partial2, through2, done2 = run(
        interior_both, "interior_both", [levels], [volume2, Late(up2)],
        [(plan.slab, "late"), (plan.slab, "late"), ((8, COL), None)], [],
    )

    def second_pull(levels_s, table_s, layers, after, recv, flux_cot, half_r, back_r, gb, layer_cot,
                    packets, planes, near, kinds, gcot, *parts):
        del after
        plan.ghosts(recv, table_s, planes, near, kinds, gb.ref, half_r, back_r)
        gb.send()
        layer = plan.ff_at(layers)
        boundary_pull(
            plan, layer, ghost_reader(gb.ref, layer, levels_s), plan.ff_at(flux_cot.get()),
            cot_emitter(layer_cot.ref, gcot),
        )
        layer_cot.send()
        plan.pack_ghost_cot(gcot, table_s, planes, near, packets, parts, half_r, back_r)

    ghosts2, layercot2, packets = run(
        second_pull,
        "second_pull",
        [levels, table],
        [layers2, done2, received4, Late(fluxcot2), half, half_back],
        [(plan.fb, "late"), (plan.ff, "late"), ((peers, 48, COL), "late")],
        ghost_scratch + [fb_scratch] + cot_halves,
    )
    received5 = exchange(packets)

    def second_flux(levels_s, send_s, layers, gb, half_r, b_fb, packets, ff, rb):
        layer = plan.ff_at(layers.get())
        boundary_fluxes(plan, layer, ghost_reader(gb.get(), layer, levels_s), flux_emitter(b_fb.ref, ff))
        b_fb.send()
        plan.pack_averages(plan.ff_at(ff), rb, send_s, packets.ref, 0, half_r)
        packets.send()

    fluxes2, averages2 = run(
        second_flux,
        "second_flux",
        [levels, send],
        [Late(layers2), Late(ghosts2), half],
        [(plan.fb, "late"), ((peers, 3, 4, COL), "late")],
        [vm(*plan.ff), vm(*plan.small)],
    )

    def middle_cot(send_s, parents_s, through, layer_cot, recv, averages, inner, packets, total, *sums):
        plan.take_faces(recv, send_s, sums)
        carry_packets(averages.get(), packets, 16)
        add_layers(through.get(), layer_cot.get(), total, sums, slab_put(inner))
        plan.pack_octants(
            lambda s, x, q: inner[q, plan.slab_rows(s, x), :], parents_s, packets, 0
        )

    inner_cot, packets = run(
        middle_cot,
        "middle_cot",
        [send, parents],
        [Late(through2), Late(layercot2), received5, Late(averages2)],
        [(plan.slab, None), ((peers, 7, 4, COL), None)],
        [vm(*plan.ff)] + face_sums,
    )
    received6 = exchange(packets)

    def upward_first(levels_s, table_s, children_s, parents_s, inner, recv, back_r, up, cot_fb,
                     packets, cc):
        plan.upward(
            recv, 0, cc, children_s, parents_s, plan.slab_at(inner), slab_put(up.ref), back_r
        )
        up.send()
        corrected_cot_of(plan.slab_at(up.ref), levels_s, cot_fb.ref)
        cot_fb.send()
        plan.pack_quarters(cot_fb.ref, table_s, packets, 0)

    up1, corrcot1, packets = run(
        upward_first,
        "upward_first",
        [levels, table, children, parents],
        [inner_cot, received6, half_back],
        [(plan.slab, "late"), (plan.fb, "late"), ((peers, 3, 4, COL), None)],
        [vm((S + 1) * 32, COL)],
    )
    received7 = exchange(packets)

    def second_update(levels_s, table_s, partial, b_fb, recv, half_r, final, cb, corr, updated, n0,
                      n1, sems):
        plan.corrected(b_fb.get(), recv, 16, table_s, corr)
        planes = [n0, n1]
        put_slab = slab_put(updated)

        def put(q, x, c, value):
            put_slab(q, x, c, value)
            planes[q][pl.ds(c * E + x, S, stride=4 * E), :] = value

        finished(partial.get(), corr, levels_s, put)
        copies = native_copies(planes, final, sems, False)
        for copy in copies:
            copy.start()
        plan.average_blocks(plan.slab_at(updated), cb, half_r)
        for copy in copies:
            copy.wait()

    final_open, coarse2 = run(
        second_update,
        "second_update",
        [levels, table],
        [Late(partial2), Late(fluxes2), received6, half],
        [(plan.native, "raw"), (plan.coarse, None)],
        [fb_scratch, vm(*plan.slab)] + native_planes + [pair_of_sems],
    )

    def interior_back(levels_s, volume, cot, through):
        plan.interior(
            dyn_get(volume.get()), levels_s, None, dyn_get(cot.get()), dyn_put(through.ref)
        )
        through.send()

    (through1,) = run(
        interior_back, "interior_back", [levels], [Late(volume1), Late(up1)],
        [(plan.slab, "late")], [],
    )

    def first_pull(levels_s, send_s, table_s, children_s, layers, gb, cot_fb, recv, coarse, half_r,
                   back_r, layer_cot, packets, planes, near, kinds, flux_cot, gcot, *late):
        parts, sums = late[:2], late[2:]
        plan.pack_children(coarse, children_s, packets.ref, 48)
        packets.send(48, 16)
        flux_cot_of(recv, 0, cot_fb, table_s, send_s, sums, kinds, flux_cot, back_r)
        layer = plan.ff_at(layers)
        boundary_pull(
            plan, layer, ghost_reader(gb, layer, levels_s), plan.ff_at(flux_cot),
            cot_emitter(layer_cot.ref, gcot),
        )
        layer_cot.send()
        plan.pack_ghost_cot(gcot, table_s, planes, near, packets, parts, half_r, back_r)

    layercot1, packets = run(
        first_pull,
        "first_pull",
        [levels, send, table, children],
        [layers1, ghosts1, corrcot1, received7, coarse2, half, half_back],
        [(plan.ff, "late"), ((peers, 64, COL), "late")],
        ghost_scratch + [vm(*plan.ff), fb_scratch] + cot_halves + quarter_sums,
    )
    received8 = exchange(packets)

    def last_cot(send_s, parents_s, through, layer_cot, recv, open_r, gradient, final, total, n0, n1,
                 p0, p1, sems, slot_sems, *sums):
        del open_r
        placed = [p0, p1]

        def store(s, x, q, value):
            placed[q][plan.native_rows(s, x), :] = value

        plan.place_octants(recv, 48, parents_s, store)

        def each_covered(act):
            for s in range(S):

                def one(s=s):
                    rows = (s * 4 * E, 4 * E)
                    for copy in native_copies(placed, final, slot_sems.at[s], False, rows):
                        act(copy)

                pl.when(parents_s[s, 0] >= 0)(one)

        each_covered(lambda copy: copy.start())
        plan.take_faces(recv, send_s, sums)
        planes = [n0, n1]

        def put(q, x, c, value):
            planes[q][pl.ds(c * E + x, S, stride=4 * E), :] = value

        add_layers(through.get(), layer_cot.get(), total, sums, put)
        copies = native_copies(planes, gradient, sems, False)
        for copy in copies:
            copy.start()
        for copy in copies:
            copy.wait()
        each_covered(lambda copy: copy.wait())

    gradient, final_fields = run(
        last_cot,
        "last_cot",
        [send, parents],
        [Late(through1), Late(layercot1), received8, Late(final_open, raw=True)],
        [(plan.native, "raw"), (plan.native, "raw")],
        [vm(*plan.ff)] + native_planes + native_planes
        + [pair_of_sems, pltpu.SemaphoreType.DMA((S, 2))] + face_sums,
        aliases={5: 1},
    )
    return (final_fields.reshape(fields.shape), gradient.reshape(fields.shape))


def solution(mesh):
    placed = (
        P("blk", None, None, None),
        P("blk", None, None, None),
        P("blk"),
        P("blk", None, None),
        P("blk", None, None),
        P("blk", None, None),
        P("blk", None),
        P("blk", None),
    )
    return jax.shard_map(
        on_device,
        mesh=mesh,
        in_specs=placed,
        out_specs=(P("blk", None, None, None), P("blk", None, None, None)),
        check_vma=False,
    )
```

```python
import jax
import jax.numpy as jnp
import numpy as np
from jax import lax
from jax.experimental import pallas as pl
from jax.experimental.pallas import tpu as pltpu
from jax.sharding import PartitionSpec as P

sound_speed = 1.0
base_ratio = 0.04
speed_floor = 0.01
f32 = jnp.float32
bf16 = jnp.bfloat16


def half_map(extent):
    half = extent // 2
    square = extent * extent
    table = np.zeros((2, extent, extent, half, 2, half), np.float32)
    for group in range(2):
        for i in range(extent):
            for j in range(extent):
                table[group, i, j, i // 2, group, j // 2] = 0.25
    return table.reshape(2 * square, square // 2)


def dot2(values, table):
    high = values.astype(bf16)
    low = (values - high.astype(f32)).astype(bf16)
    return jnp.dot(high, table, preferred_element_type=f32) + jnp.dot(
        low, table, preferred_element_type=f32
    )


def roll(values, shift):
    lanes = values.shape[1]
    shift = shift % lanes
    return values if shift == 0 else pltpu.roll(values, shift, 1)


def tile(packets, peer, row):
    return packets.at[peer, row // 4] if len(packets.shape) == 4 else packets.at[peer, row : row + 4]


def flux_of(behind, beyond, normal, inv_behind, inv_beyond):
    v = behind[1 + normal] * inv_behind
    w = beyond[1 + normal] * inv_beyond
    c = sound_speed + jnp.sqrt(0.5 * (v * v + w * w) + speed_floor)
    result = [0.5 * ((behind[1 + normal] + beyond[1 + normal]) - c * (beyond[0] - behind[0]))]
    for k in range(1, 4):
        total = behind[k] * v + beyond[k] * w
        if k == 1 + normal:
            total = total + (sound_speed * sound_speed) * (behind[0] + beyond[0])
        result.append(0.5 * (total - c * (beyond[k] - behind[k])))
    return result


def flux_pull(behind, beyond, normal, inv_behind, inv_beyond, cot):
    v = behind[1 + normal] * inv_behind
    w = beyond[1 + normal] * inv_beyond
    inside = 0.5 * (v * v + w * w) + speed_floor
    root = jnp.sqrt(inside)
    c = sound_speed + root
    half_cot = [0.5 * part for part in cot]
    jump = half_cot[0] * (beyond[0] - behind[0])
    v_cot = half_cot[1] * behind[1]
    w_cot = half_cot[1] * beyond[1]
    for k in range(1, 4):
        jump = jump + half_cot[k] * (beyond[k] - behind[k])
        if k > 1:
            v_cot = v_cot + half_cot[k] * behind[k]
            w_cot = w_cot + half_cot[k] * beyond[k]
    scale = jump * (-0.5) / root
    v_cot = (v_cot + scale * v) * inv_behind
    w_cot = (w_cot + scale * w) * inv_beyond
    plus = v + c
    minus = w - c
    behind_cot = []
    beyond_cot = []
    pressure = (sound_speed * sound_speed) * half_cot[1 + normal]
    for k in range(4):
        if k == 0:
            behind_cot.append(c * half_cot[0] + pressure - v_cot * v)
            beyond_cot.append(pressure - c * half_cot[0] - w_cot * w)
        else:
            left = half_cot[k] * plus
            right = half_cot[k] * minus
            if k == 1 + normal:
                left = left + half_cot[0] + v_cot
                right = right + half_cot[0] + w_cot
            behind_cot.append(left)
            beyond_cot.append(right)
    return behind_cot, beyond_cot


class Plan:
    def __init__(self, slots, extent, peers):
        self.S = slots
        self.E = extent
        self.P = peers
        self.H = extent // 2
        self.COL = extent * extent // 2
        self.slab = (2, extent * 4 * slots, self.COL)
        self.ff = (2, 6 * 4 * slots, self.COL)
        self.fb = (2, 3 * slots * 8, self.COL)
        self.native = (slots * 4 * extent, 2 * self.COL)
        self.coarse = (slots * 32, self.COL)
        self.small = (slots * 24, self.COL)

    def lane(self, rows):
        return lax.broadcasted_iota(jnp.int32, (rows, self.COL), 1)

    def low(self, rows):
        return (self.lane(rows) & (self.E - 1)) < self.H

    def per_slot(self, scalar_of):
        sub = lax.broadcasted_iota(jnp.int32, (self.S, self.COL), 0)
        value = jnp.zeros((self.S, self.COL), jnp.int32)
        for s in range(self.S):
            value = jnp.where(sub == s, scalar_of(s), value)
        return value

    def ratio(self, levels):
        level = self.per_slot(lambda s: levels[s])
        degree = level.astype(f32)
        ratio = base_ratio * (1.0 + degree + 0.5 * degree * (degree - 1.0))
        return jnp.where(level >= 0, ratio, 0.0)

    def slab_at(self, ref):
        return lambda q, x, c: ref[q, (x * 4 + c) * self.S : (x * 4 + c + 1) * self.S, :]

    def native_at(self, planes):
        step = 4 * self.E
        return lambda q, x, c: planes[q][pl.ds(c * self.E + x, self.S, stride=step), :]

    def ff_at(self, ref):
        return lambda q, f, c: ref[q, (f * 4 + c) * self.S : (f * 4 + c + 1) * self.S, :]

    def fb_rows(self, f, c, swapped=False):
        side = f % 2
        half = 1 - side if swapped else side
        return pl.ds((f // 2) * self.S * 8 + half * 4 + c, self.S, stride=8)

    def extract(self, get, c):
        E, H, COL = self.E, self.H, self.COL
        lane = self.lane(self.S)
        group = lax.shift_right_logical(lane, E.bit_length() - 1)
        within = lane & (E - 1)
        faces = [[get(q, 0, c) for q in range(2)], [get(q, E - 1, c) for q in range(2)]]
        low_y, high_y, low_z, high_z = [], [], [], []
        for q in range(2):
            first, last, near, far = None, None, None, None
            for k in range(H):
                a = roll(get(0, q * H + k, c), E * k)
                b = roll(get(1, q * H + k, c), E * k - (COL - E))
                first = a if first is None else jnp.where(group == k, a, first)
                last = b if last is None else jnp.where(group == k, b, last)
            for x in range(E):
                source = get(q, x, c)
                a = roll(source, x)
                b = roll(source, x - (E - 1))
                near = a if near is None else jnp.where(within == x, a, near)
                far = b if far is None else jnp.where(within == x, b, far)
            low_y.append(first)
            high_y.append(last)
            low_z.append(near)
            high_z.append(far)
        return faces + [low_y, high_y, low_z, high_z]

    def spread(self, face, q, x, c):
        E, H, COL = self.E, self.H, self.COL
        lane = self.lane(self.S)
        within = lane & (E - 1)
        k = x % H
        y_face = face(x // H, 2 + q, c)
        if q == 0:
            total = jnp.where(lane < E, roll(y_face, -E * k), 0.0)
        else:
            total = jnp.where(lane >= COL - E, roll(y_face, (COL - E) - E * k), 0.0)
        near = roll(face(q, 4, c), -x)
        far = roll(face(q, 5, c), E - 1 - x)
        total = total + jnp.where(within == 0, near, jnp.where(within == E - 1, far, 0.0))
        if x == 0:
            total = total + face(q, 0, c)
        if x == E - 1:
            total = total + face(q, 1, c)
        return total

    def pack_faces(self, fb, send, out):
        sub = lax.broadcasted_iota(jnp.int32, (8, self.COL), 0)
        for axis in range(3):

            def one(peer, carry, axis=axis):
                slots = [jnp.maximum(send[axis * 2 + side, 0, peer], 0) for side in range(2)]
                for q in range(2):
                    lo, hi = [
                        fb[q, pl.ds(pl.multiple_of((axis * self.S + slot) * 8, 8), 8), :]
                        for slot in slots
                    ]
                    row = axis * 16 + q * 8
                    out.ref[peer, row : row + 8, :] = jnp.where(sub < 4, lo, hi)
                return carry

            lax.fori_loop(0, self.P, one, 0, unroll=4)
            out.send(axis * 16, 16)

    def take_faces(self, packets, send, sums):
        def one(peer, carry):
            for f in range(6):
                slot = jnp.maximum(send[f, 0, peer], 0)
                rows = pl.ds(pl.multiple_of(slot * 8, 8), 8)
                for q in range(2):
                    at = (f // 2) * 16 + q * 8
                    sums[f * 2 + q][rows, :] += packets[peer, at : at + 8, :]
            return carry

        for part in sums:
            part[...] = jnp.zeros(part.shape, f32)
        lax.fori_loop(0, self.P, one, 0, unroll=4)

    def pack_averages(self, face, rb, send, out, row0, half):
        S, COL = self.S, self.COL
        rows = []
        for axis in range(3):
            for c in range(4):
                rows.append(
                    jnp.concatenate(
                        [face(q, 2 * axis + side, c) for side in range(2) for q in range(2)], axis=1
                    )
                )
        small = dot2(jnp.concatenate(rows, axis=0), half[...])
        for k in range(12):
            rb[pl.ds((k // 4) * 8 + k % 4, S, stride=24), :] = small[k * S : (k + 1) * S]
        low = self.low(4)

        def one(peer, carry):
            for axis in range(3):
                lo, hi = [
                    rb[pl.ds(pl.multiple_of(slot * 24 + axis * 8, 8), 4), :]
                    for slot in [jnp.maximum(send[axis * 2 + side, 0, peer], 0) for side in range(2)]
                ]
                tile(out, peer, row0 + axis * 4)[...] = jnp.where(low, lo, hi)
            return carry

        lax.fori_loop(0, self.P, one, 0, unroll=4)

    def pack_quarters(self, fb, table, out, row0):
        E, H = self.E, self.H
        low = self.low(4)

        def clear(peer, carry):
            for axis in range(3):
                tile(out, peer, row0 + axis * 4)[...] = jnp.zeros((4, self.COL), f32)
            return carry

        lax.fori_loop(0, self.P, clear, 0, unroll=4)
        for s in range(self.S):
            for f in range(6):
                base = (s * 6 + f) * 8

                def send_quarters(s=s, f=f, base=base):
                    axis, side = f // 2, f % 2
                    keep = low if side == 1 else jnp.logical_not(low)
                    row = (axis * self.S + s) * 8 + side * 4
                    at = row0 + axis * 4
                    for h in range(2):
                        values = fb[h, row : row + 4, :]
                        for g in range(2):
                            moved = roll(values, H * ((1 - side) - g))
                            peer = table[base + h * 2 + g]
                            tile(out, peer, at)[...] += jnp.where(keep, moved, 0.0)

                pl.when(table[base + 4] == 2)(send_quarters)

    def take_quarters(self, packets, row0, send, sums, face_out, half_back):
        S, COL = self.S, self.COL

        def one(peer, carry):
            for axis in range(3):
                block = tile(packets, peer, row0 + axis * 4)[...]
                for f in (axis * 2, axis * 2 + 1):
                    slot = jnp.maximum(send[f, 0, peer], 0)
                    sums[f][pl.ds(pl.multiple_of(slot * 8, 8), 4), :] += block
            return carry

        for f in range(6):
            sums[f][...] = jnp.zeros(sums[f].shape, f32)
        lax.fori_loop(0, self.P, one, 0, unroll=4)
        for f in range(6):
            side = f % 2
            rows = jnp.concatenate(
                [sums[f][pl.ds(c, S, stride=8), :] for c in range(4)], axis=0
            )
            wide = dot2(rows, half_back[:, side * 2 * COL : (side + 1) * 2 * COL])
            for c in range(4):
                face_out(f, c, [wide[c * S : (c + 1) * S, q * COL : (q + 1) * COL] for q in range(2)])

    def ghosts(self, packets, table, planes, near, kinds, gb, half, half_back):
        S, COL, H = self.S, self.COL, self.H
        for s in range(S):
            for f in range(6):
                base = (s * 6 + f) * 8
                axis, half_row = f // 2, (1 - f % 2) * 4
                row = (axis * S + s) * 8 + half_row
                first = None
                for k in range(4):
                    peer = table[base + k]
                    got = []
                    for q in range(2):
                        at = axis * 16 + q * 8 + half_row
                        values = packets[peer, at : at + 4, :]
                        planes[k * 2 + q, row : row + 4, :] = values
                        got.append(values)
                    if k == 0:
                        first = got
                source = jnp.where(table[base + 5] == 1, first[1], first[0])
                source = jnp.where(table[base + 6] == 1, roll(source, -H), source)
                near[row : row + 4, :] = source
                kinds[row : row + 4, :] = jnp.full((4, COL), table[base + 4], jnp.int32)
        for axis in range(3):
            rows = slice(axis * S * 8, (axis + 1) * S * 8)
            kind = kinds[rows, :]
            coarse = 4.0 * dot2(near[rows, :], half_back[:, : 2 * COL])
            for h in range(2):
                parts = [planes[(h * 2 + g) * 2 + q, rows, :] for g in range(2) for q in range(2)]
                fine = dot2(jnp.concatenate(parts, axis=1), half[...])
                value = jnp.where(kind == 1, coarse[:, h * COL : (h + 1) * COL], planes[h, rows, :])
                gb[h, rows, :] = jnp.where(kind == 2, fine, value)

    def pack_ghost_cot(self, gb, table, wide, near, out, parts, half, half_back):
        S, COL, H = self.S, self.COL, self.H
        low = self.low(4)

        def clear(peer, carry):
            for part in parts:
                part[peer, :, :] = jnp.zeros((24, COL), f32)
            return carry

        lax.fori_loop(0, self.P, clear, 0, unroll=4)
        for h in range(2):
            for g in range(2):
                spread = dot2(gb[h, :, :], half_back[:, g * 2 * COL : (g + 1) * 2 * COL])
                for q in range(2):
                    wide[(h * 2 + g) * 2 + q, :, :] = spread[:, q * COL : (q + 1) * COL]
        both = jnp.concatenate([gb[0, :, :], gb[1, :, :]], axis=1)
        near[...] = 4.0 * dot2(both, half[0 : 2 * COL, :])
        for f in range(6):
            for s in range(S):
                base = (s * 6 + f) * 8
                axis, half_row = f // 2, (1 - f % 2) * 4
                row = (axis * S + s) * 8 + half_row
                kind = table[base + 4]

                def same(base=base, axis=axis, half_row=half_row, row=row):
                    peer = table[base]
                    for q in range(2):
                        at = axis * 8 + half_row
                        parts[q][peer, at : at + 4, :] += gb[q, row : row + 4, :]

                def coarse(base=base, axis=axis, half_row=half_row, row=row):
                    peer = table[base]
                    values = near[row : row + 4, :]
                    values = jnp.where(table[base + 6] == 1, roll(values, H), values)
                    for q in range(2):
                        at = axis * 8 + half_row
                        parts[q][peer, at : at + 4, :] += jnp.where(table[base + 5] == q, values, 0.0)

                def fine(base=base, axis=axis, half_row=half_row, row=row):
                    for k in range(4):
                        peer = table[base + k]
                        for q in range(2):
                            at = axis * 8 + half_row
                            parts[q][peer, at : at + 4, :] += wide[k * 2 + q, row : row + 4, :]

                pl.when(kind == 0)(same)
                pl.when(kind == 1)(coarse)
                pl.when(kind == 2)(fine)
            if f % 2 == 1:
                for q in range(2):
                    out.send((f // 2) * 16 + q * 8, 8, parts[q], (f // 2) * 8)

    def corrected(self, b_fb, packets, row0, table, out):
        H = self.H
        low = self.low(4)
        out[...] = b_fb[...]
        for s in range(self.S):
            for f in range(6):
                base = (s * 6 + f) * 8

                def replace(s=s, f=f, base=base):
                    axis, side = f // 2, f % 2
                    row = (axis * self.S + s) * 8 + side * 4
                    at = row0 + axis * 4
                    for h in range(2):
                        got = []
                        for g in range(2):
                            values = tile(packets, table[base + h * 2 + g], at)[...]
                            got.append(roll(values, H * (g - (1 - side))))
                        out[h, row : row + 4, :] = jnp.where(low, got[0], got[1])

                pl.when(table[base + 4] == 2)(replace)

    def pack_octants(self, load, parents, out, row0):
        H = self.H
        low = self.low(4)
        for s in range(self.S):

            def send(s=s):
                for ox in range(2):
                    for oy in range(2):
                        peers = [parents[s, ox * 4 + oy * 2 + oz] for oz in range(2)]
                        for pair in range(H // 2):
                            x = ox * H + pair * 2
                            first, second = load(s, x, oy), load(s, x + 1, oy)
                            at = row0 + pair * 4
                            tile(out, peers[0], at)[...] = jnp.where(low, first, roll(second, H))
                            tile(out, peers[1], at)[...] = jnp.where(low, roll(first, -H), second)

            pl.when(parents[s, 0] >= 0)(send)

    def place_octants(self, packets, row0, parents, store):
        H = self.H
        low = self.low(4)
        for s in range(self.S):

            def place(s=s):
                for ox in range(2):
                    for oy in range(2):
                        peers = [parents[s, ox * 4 + oy * 2 + oz] for oz in range(2)]
                        for pair in range(H // 2):
                            x = ox * H + pair * 2
                            at = row0 + pair * 4
                            first = tile(packets, peers[0], at)[...]
                            second = tile(packets, peers[1], at)[...]
                            store(s, x, oy, jnp.where(low, first, roll(second, H)))
                            store(s, x + 1, oy, jnp.where(low, roll(first, -H), second))

            pl.when(parents[s, 0] >= 0)(place)

    def slab_rows(self, s, x):
        return pl.ds(x * 4 * self.S + s, 4, stride=self.S)

    def native_rows(self, s, x):
        return pl.ds(s * 4 * self.E + x, 4, stride=self.E)

    def average_blocks(self, get, cb, half):
        S = self.S
        rows = []
        for pair in range(self.E // 4):
            for c in range(4):
                x = 4 * pair
                rows.append(
                    jnp.concatenate(
                        [get(q, x + 2 * a, c) + get(q, x + 2 * a + 1, c) for a in range(2) for q in range(2)],
                        axis=1,
                    )
                )
        small = 0.5 * dot2(jnp.concatenate(rows, axis=0), half[...])
        for k in range(16):
            cb[pl.ds((k // 4) * 8 + k % 4, S, stride=32), :] = small[k * S : (k + 1) * S]

    def pack_children(self, cb, children, out, row0):
        def one(peer, carry):
            slot = jnp.maximum(children[peer], 0)
            for part in range(4):
                rows = pl.ds(pl.multiple_of(slot * 32 + part * 8, 8), 4)
                tile(out, peer, row0 + part * 4)[...] = cb[rows, :]
            return carry

        lax.fori_loop(0, self.P, one, 0, unroll=4)

    def upward(self, packets, row0, cc, children, parents, get, put, half_back):
        S, COL = self.S, self.COL
        cc[...] = jnp.zeros(cc.shape, f32)

        def one(peer, carry):
            child = children[peer]
            slot = jnp.where(child < 0, S, child)
            for part in range(4):
                rows = pl.ds(pl.multiple_of(slot * 32 + part * 8, 8), 4)
                cc[rows, :] += tile(packets, peer, row0 + part * 4)[...]
            return carry

        lax.fori_loop(0, self.P, one, 0, unroll=4)
        rows = jnp.concatenate(
            [cc[pl.ds((k // 4) * 8 + k % 4, S, stride=32), :] for k in range(16)], axis=0
        )
        wide = 0.5 * dot2(rows, half_back[...])
        covered = self.per_slot(lambda s: parents[s, 0]) >= 0
        for x in range(self.E):
            for c in range(4):
                row = ((x // 4) * 4 + c) * S
                for q in range(2):
                    lane0 = ((x // 2) % 2 * 2 + q) * COL
                    added = wide[row : row + S, lane0 : lane0 + COL]
                    put(q, x, c, jnp.where(covered, 0.0, get(q, x, c)) + added)

    def shifted(self, planes, amount):
        COL = self.COL
        lane = self.lane(self.S)
        moved = [roll(values, amount) for values in planes]
        if amount > 0:
            return [jnp.where(lane < amount, moved[1 - q], moved[q]) for q in range(2)]
        return [jnp.where(lane >= COL + amount, moved[1 - q], moved[q]) for q in range(2)]

    def interior(self, get, levels, forward_put, cot_get=None, cot_put=None):
        S, E, COL = self.S, self.E, self.COL
        ratio = self.ratio(levels)
        lane = self.lane(S)
        y_inside = [lane >= 0, lane < COL - E]
        z_inside = (lane & (E - 1)) != E - 1
        zero = jnp.zeros((S, COL), f32)

        def row_of(x, c):
            return pl.ds(pl.multiple_of((x * 4 + c) * S, S), S)

        def one(x, carry):
            after = jnp.minimum(x + 1, E - 1)
            x_inside = x < E - 1
            here = [[get(q, row_of(x, c)) for c in range(4)] for q in range(2)]
            inverse = [1.0 / here[q][0] for q in range(2)]
            ahead = [[get(q, row_of(after, c)) for c in range(4)] for q in range(2)]
            ahead_inv = [1.0 / ahead[q][0] for q in range(2)]
            flux_carry, cot_carry = carry
            new_flux, new_cot = [], []
            change = [[None] * 4 for _ in range(2)]
            if cot_get is not None:
                weight = [[get_c(q, row_of(x, c)) for c in range(4)] for q in range(2)]
                scaled = [[ratio * weight[q][c] for c in range(4)] for q in range(2)]
                ahead_scaled = [
                    [ratio * get_c(q, row_of(after, c)) for c in range(4)] for q in range(2)
                ]
                back = [[weight[q][c] for c in range(4)] for q in range(2)]
            for q in range(2):
                if forward_put is not None:
                    flux = flux_of(here[q], ahead[q], 0, inverse[q], ahead_inv[q])
                    flux = [jnp.where(x_inside, part, 0.0) for part in flux]
                    change[q] = [flux[c] - flux_carry[q * 4 + c] for c in range(4)]
                    new_flux += flux
                if cot_get is not None:
                    cot = [
                        jnp.where(x_inside, ahead_scaled[q][c] - scaled[q][c], 0.0) for c in range(4)
                    ]
                    left, right = flux_pull(here[q], ahead[q], 0, inverse[q], ahead_inv[q], cot)
                    back[q] = [back[q][c] + left[c] + cot_carry[q * 4 + c] for c in range(4)]
                    new_cot += right
            for normal, step, inside in ((1, E, y_inside), (2, 1, [z_inside, z_inside])):
                turned = [self.shifted([here[q][c] for q in range(2)], -step) for c in range(4)]
                turned_inv = self.shifted(inverse, -step)
                beyond = [[turned[c][q] for c in range(4)] for q in range(2)]
                if forward_put is not None:
                    flux = []
                    for q in range(2):
                        got = flux_of(here[q], beyond[q], normal, inverse[q], turned_inv[q])
                        flux.append([jnp.where(inside[q], part, 0.0) for part in got])
                    for c in range(4):
                        behind = self.shifted([flux[q][c] for q in range(2)], step)
                        for q in range(2):
                            change[q][c] = change[q][c] + (flux[q][c] - behind[q])
                if cot_get is not None:
                    turned_w = [self.shifted([scaled[q][c] for q in range(2)], -step) for c in range(4)]
                    rights = []
                    for q in range(2):
                        cot = [
                            jnp.where(inside[q], turned_w[c][q] - scaled[q][c], 0.0) for c in range(4)
                        ]
                        left, right = flux_pull(here[q], beyond[q], normal, inverse[q], turned_inv[q], cot)
                        back[q] = [back[q][c] + left[c] for c in range(4)]
                        rights.append(right)
                    for c in range(4):
                        moved = self.shifted([rights[q][c] for q in range(2)], step)
                        for q in range(2):
                            back[q][c] = back[q][c] + moved[q]
            for q in range(2):
                for c in range(4):
                    if forward_put is not None:
                        forward_put(q, row_of(x, c), here[q][c] - ratio * change[q][c])
                    if cot_get is not None:
                        cot_put(q, row_of(x, c), back[q][c])
            return (new_flux, new_cot)

        get_c = cot_get
        start = (
            [zero] * 8 if forward_put is not None else [],
            [zero] * 8 if cot_get is not None else [],
        )
        lax.fori_loop(0, E, one, start)


class Arriving:
    def __init__(self, copies, ref):
        self.copies = copies
        self.ref = ref
        for copy in copies:
            copy.start()

    def get(self):
        for copy in self.copies:
            copy.wait()
        self.copies = []
        return self.ref


class Leaving:
    def __init__(self, ref, target, sems):
        self.ref = ref
        self.target = target
        self.sems = sems
        self.copies = []

    def send(self, first=None, count=None, ref=None, start=None):
        near, far = self.ref if ref is None else ref, self.target
        if count is not None:
            near = near.at[:, pl.ds(first if start is None else start, count), :]
            far = far.at[:, pl.ds(first, count), :]
        copy = pltpu.make_async_copy(near, far, self.sems.at[len(self.copies)])
        copy.start()
        self.copies.append(copy)

    def finish(self):
        for copy in self.copies:
            copy.wait()


class Late:
    def __init__(self, array, native=False, raw=False):
        self.array = array
        self.native = native
        self.raw = raw


def run(body, name, scalars, arrays, outs, scratch, aliases=None):
    hbm = pltpu.MemorySpace.HBM
    specs = [pl.BlockSpec(memory_space=pltpu.SMEM) for _ in scalars]
    operands = list(scalars)
    extra = []
    arriving, leaving = {}, {}
    for index, item in enumerate(arrays):
        if isinstance(item, Late):
            specs.append(pl.BlockSpec(memory_space=hbm))
            operands.append(pltpu.with_memory_space_constraint(item.array, hbm))
            if not item.raw:
                shape = item.array.shape
                arriving[index] = (len(extra), item.native)
                if item.native:
                    half = (shape[0], shape[1] // 2)
                    extra += [pltpu.VMEM(half, f32), pltpu.VMEM(half, f32)]
                    extra.append(pltpu.SemaphoreType.DMA((2,)))
                else:
                    extra += [pltpu.VMEM(shape, f32), pltpu.SemaphoreType.DMA((1,))]
        else:
            specs.append(pl.BlockSpec(memory_space=pltpu.VMEM))
            operands.append(item)
    out_specs = []
    for index, (shape, mode) in enumerate(outs):
        out_specs.append(pl.BlockSpec(memory_space=hbm if mode else pltpu.VMEM))
        if mode == "late":
            leaving[index] = len(extra)
            extra += [pltpu.VMEM(shape, f32), pltpu.SemaphoreType.DMA((8,))]

    def wrapped(*refs):
        n_scalar, n_in, n_out = len(scalars), len(arrays), len(outs)
        scalar_refs = list(refs[:n_scalar])
        in_refs = list(refs[n_scalar : n_scalar + n_in])
        out_refs = list(refs[n_scalar + n_in : n_scalar + n_in + n_out])
        rest = refs[n_scalar + n_in + n_out :]
        own, late = rest[: len(scratch)], rest[len(scratch) :]
        for index, (at, native) in arriving.items():
            if native:
                planes = [late[at], late[at + 1]]
                copies = native_copies(planes, in_refs[index], late[at + 2], True)
                in_refs[index] = Arriving(copies, planes)
            else:
                copy = pltpu.make_async_copy(in_refs[index], late[at], late[at + 1].at[0])
                in_refs[index] = Arriving([copy], late[at])
        for index, at in leaving.items():
            out_refs[index] = Leaving(late[at], out_refs[index], late[at + 1])
        body(*scalar_refs, *in_refs, *out_refs, *own)
        for index in arriving:
            in_refs[index].get()
        for index in leaving:
            out_refs[index].finish()

    return pl.pallas_call(
        wrapped,
        name=name,
        in_specs=specs,
        out_specs=out_specs,
        out_shape=[
            hbm(shape, f32) if mode else jax.ShapeDtypeStruct(shape, f32) for shape, mode in outs
        ],
        scratch_shapes=list(scratch) + extra,
        input_output_aliases=aliases or {},
        compiler_params=pltpu.CompilerParams(vmem_limit_bytes=32 * 1024 * 1024),
    )(*operands)


def native_copies(planes, whole, sems, inward, rows=None):
    lanes = planes[0].shape[1]
    copies = []
    for q in range(2):
        part = whole.at[:, pl.ds(q * lanes, lanes)]
        near = planes[q]
        if rows is not None:
            part = whole.at[pl.ds(*rows), pl.ds(q * lanes, lanes)]
            near = planes[q].at[pl.ds(*rows), :]
        source, target = (part, near) if inward else (near, part)
        copies.append(pltpu.make_async_copy(source, target, sems.at[q]))
    return copies


def boundary_fluxes(plan, layers, ghost, emit):
    for f in range(6):
        result = []
        for q in range(2):
            inner = [layers(q, f, c) for c in range(4)]
            outer = [ghost(q, f, c) for c in range(4)]
            inner_inv, outer_inv = 1.0 / inner[0], 1.0 / outer[0]
            if f % 2 == 0:
                result.append(flux_of(outer, inner, f // 2, outer_inv, inner_inv))
            else:
                result.append(flux_of(inner, outer, f // 2, inner_inv, outer_inv))
        for c in range(4):
            emit(f, c, [result[q][c] for q in range(2)])


def boundary_pull(plan, layers, ghost, cot, emit):
    for f in range(6):
        result = []
        for q in range(2):
            inner = [layers(q, f, c) for c in range(4)]
            outer = [ghost(q, f, c) for c in range(4)]
            weight = [cot(q, f, c) for c in range(4)]
            inner_inv, outer_inv = 1.0 / inner[0], 1.0 / outer[0]
            if f % 2 == 0:
                out_cot, in_cot = flux_pull(outer, inner, f // 2, outer_inv, inner_inv, weight)
            else:
                in_cot, out_cot = flux_pull(inner, outer, f // 2, inner_inv, outer_inv, weight)
            result.append((in_cot, out_cot))
        for c in range(4):
            emit(f, c, [result[q][0][c] for q in range(2)], [result[q][1][c] for q in range(2)])


def on_device(fields, guidance, levels, send_faces, ghost_peer, ghost_code, child_send, parent_peer):
    slots, _, extent, square = fields.shape
    peers = send_faces.shape[1]
    plan = Plan(slots, extent, peers)
    S, E, COL = slots, extent, plan.COL
    half_np = half_map(extent)
    half = jnp.asarray(half_np, bf16)
    half_back = jnp.asarray(np.ascontiguousarray(half_np.T), bf16)

    first_map, second_map = ghost_code // 5, ghost_code % 5
    turned = (jnp.arange(6) >= 4)[None, :, None]
    major = jnp.where(turned, second_map, first_map)
    minor = jnp.where(turned, first_map, second_map)
    refined = ghost_peer[:, :, 1] >= 0
    quarter = (major - 3) * 2 + (minor - 3)
    chosen = jnp.maximum(ghost_peer, 0)
    columns = [
        jnp.where(refined, jnp.sum(jnp.where(quarter == k, chosen, 0), axis=2), chosen[:, :, 0])
        for k in range(4)
    ]
    coarser = ghost_code[:, :, 0] > 0
    kind = jnp.where(
        ghost_peer[:, :, 0] < 0, 3, jnp.where(refined, 2, jnp.where(coarser, 1, 0))
    )
    single = jnp.logical_and(coarser, jnp.logical_not(refined))
    columns += [
        kind,
        jnp.where(single, major[:, :, 0] - 1, 0),
        jnp.where(single, minor[:, :, 0] - 1, 0),
        jnp.zeros_like(kind),
    ]
    table = jnp.stack(columns, axis=-1).astype(jnp.int32).reshape(-1)
    send = jnp.transpose(send_faces, (2, 0, 1))
    children = child_send.reshape(-1)
    parents = parent_peer
    native_fields = fields.reshape(plan.native)
    native_guidance = guidance.reshape(plan.native)

    def exchange(packets):
        return lax.all_to_all(packets, "blk", split_axis=0, concat_axis=0, tiled=True)

    def vm(*shape):
        return pltpu.VMEM(shape, f32)

    def occupied_of(levels_ref):
        return plan.per_slot(lambda s: levels_ref[s]) >= 0

    fb_scratch = vm(*plan.fb)
    kind_scratch = pltpu.VMEM((3 * S * 8, COL), jnp.int32)
    native_planes = [vm(S * 4 * E, COL), vm(S * 4 * E, COL)]
    pair_of_sems = pltpu.SemaphoreType.DMA((2,))
    quarter_sums = [vm(S * 8, COL) for _ in range(6)]
    face_sums = [vm(S * 8, COL) for _ in range(12)]
    cot_halves = [vm(peers, 24, COL) for _ in range(2)]
    signs = [1.0, -1.0, 1.0, -1.0, 1.0, -1.0]

    def layers_of(get, fb, ff):
        for c in range(4):
            faces = plan.extract(get, c)
            for f in range(6):
                for q in range(2):
                    if fb is not None:
                        fb[q, plan.fb_rows(f, c), :] = faces[f][q]
                    if ff is not None:
                        ff[q, (f * 4 + c) * S : (f * 4 + c + 1) * S, :] = faces[f][q]

    def corrected_cot_of(get, levels_ref, fb):
        ratio = plan.ratio(levels_ref)
        for c in range(4):
            faces = plan.extract(get, c)
            for f in range(6):
                for q in range(2):
                    fb[q, plan.fb_rows(f, c), :] = (signs[f] * ratio) * faces[f][q]

    def finished(partial, corr, levels_ref, put):
        ratio = plan.ratio(levels_ref)
        occupied = ratio > 0.0
        get = plan.slab_at(partial)

        def face(q, f, c):
            value = corr[q, plan.fb_rows(f, c), :]
            return jnp.where(occupied, (signs[f] * ratio) * value, 0.0)

        for x in range(E):
            for c in range(4):
                for q in range(2):
                    put(q, x, c, get(q, x, c) + plan.spread(face, q, x, c))

    def ghost_reader(gb, layers, levels_ref):
        occupied = occupied_of(levels_ref)
        return lambda q, f, c: jnp.where(
            occupied, gb[q, plan.fb_rows(f, c, True), :], layers(q, f, c)
        )

    def slab_put(ref):
        def put(q, x, c, value):
            ref[q, (x * 4 + c) * S : (x * 4 + c + 1) * S, :] = value

        return put

    def dyn_get(ref):
        return lambda q, rows: ref[q, rows, :]

    def dyn_put(ref):
        def put(q, rows, value):
            ref[q, rows, :] = value

        return put

    ghost_scratch = [vm(8, 3 * S * 8, COL), vm(3 * S * 8, COL), kind_scratch]

    def flux_cot_of(recv, row0, cot_fb, table_s, send_s, sums, kinds, flux_cot, back_r):
        for s in range(S):
            for f in range(6):
                row = ((f // 2) * S + s) * 8 + (f % 2) * 4
                kinds[row : row + 4, :] = jnp.full((4, COL), table_s[(s * 6 + f) * 8 + 4], jnp.int32)

        def face_out(f, c, wide):
            keep = kinds[plan.fb_rows(f, c), :] != 2
            for q in range(2):
                own = jnp.where(keep, cot_fb[q, plan.fb_rows(f, c), :], 0.0)
                flux_cot[q, (f * 4 + c) * S : (f * 4 + c + 1) * S, :] = own + wide[q]

        plan.take_quarters(recv, row0, send_s, sums, face_out, back_r)

    def flux_emitter(b_fb, ff):
        def emit(f, c, values):
            for q in range(2):
                b_fb[q, plan.fb_rows(f, c), :] = values[q]
                ff[q, (f * 4 + c) * S : (f * 4 + c + 1) * S, :] = values[q]

        return emit

    def cot_emitter(layer_cot, gcot):
        def emit(f, c, inner, outer):
            for q in range(2):
                layer_cot[q, (f * 4 + c) * S : (f * 4 + c + 1) * S, :] = inner[q]
                gcot[q, plan.fb_rows(f, c, True), :] = outer[q]

        return emit

    def carry_packets(source, out, row0):
        def one(peer, carry):
            for axis in range(3):
                tile(out, peer, row0 + axis * 4)[...] = tile(source, peer, axis * 4)[...]
            return carry

        lax.fori_loop(0, peers, one, 0, unroll=4)

    def add_layers(through, layer_cot, total, sums, put, finish=None):
        own = plan.ff_at(layer_cot)
        for f in range(6):
            for c in range(4):
                for q in range(2):
                    added = sums[f * 2 + q][pl.ds((f % 2) * 4 + c, S, stride=8), :]
                    total[q, (f * 4 + c) * S : (f * 4 + c + 1) * S, :] = own(q, f, c) + added
        get = plan.slab_at(through)
        summed = plan.ff_at(total)
        for q in range(2):
            for x in range(E):
                for c in range(4):
                    put(q, x, c, get(q, x, c) + plan.spread(summed, q, x, c))
            if finish is not None:
                finish(q)

    def first_pack(send_s, parents_s, fields_r, guide_r, volume, layers, packets, fb):
        get = plan.native_at(fields_r.get())
        for x in range(E):
            for c in range(4):
                for q in range(2):
                    volume[q, (x * 4 + c) * S : (x * 4 + c + 1) * S, :] = get(q, x, c)
        layers_of(plan.slab_at(volume), fb, layers.ref)
        layers.send()
        plan.pack_faces(fb, send_s, packets)
        planes = guide_r.get()
        plan.pack_octants(
            lambda s, x, q: planes[q][plan.native_rows(s, x), :], parents_s, packets.ref, 48
        )
        packets.send(48, 16)

    state1, layers1, packets = run(
        first_pack,
        "first_pack",
        [send, parents],
        [Late(native_fields, native=True), Late(native_guidance, native=True)],
        [(plan.slab, None), (plan.ff, "late"), ((peers, 64, COL), "late")],
        [fb_scratch],
    )
    received1 = exchange(packets)

    def interior_first(levels_s, volume, guide_r, partial, kept, guide_slab, done, sems):
        copy = pltpu.make_async_copy(volume, kept, sems.at[0])
        copy.start()
        get = plan.native_at(guide_r.get())
        put = slab_put(guide_slab.ref)
        for x in range(E):
            for c in range(4):
                for q in range(2):
                    put(q, x, c, get(q, x, c))
        guide_slab.send()
        plan.interior(dyn_get(volume), levels_s, dyn_put(partial.ref))
        partial.send()
        done[...] = jnp.zeros(done.shape, f32)
        copy.wait()

    partial1, volume1, guide1, done1 = run(
        interior_first, "interior_first", [levels],
        [state1, Late(native_guidance, native=True)],
        [(plan.slab, "late"), (plan.slab, "raw"), (plan.slab, "late"), ((8, COL), None)],
        [pair_of_sems],
    )

    def first_flux(levels_s, send_s, table_s, layers, after, recv, half_r, back_r, gb, b_fb, packets,
                   planes, near, kinds, ff, rb):
        del after
        plan.ghosts(recv, table_s, planes, near, kinds, gb.ref, half_r, back_r)
        gb.send()
        layer = plan.ff_at(layers)
        boundary_fluxes(plan, layer, ghost_reader(gb.ref, layer, levels_s), flux_emitter(b_fb.ref, ff))
        b_fb.send()
        plan.pack_averages(plan.ff_at(ff), rb, send_s, packets, 0, half_r)

    ghosts1, fluxes1, packets = run(
        first_flux,
        "first_flux",
        [levels, send, table],
        [layers1, done1, received1, half, half_back],
        [(plan.fb, "late"), (plan.fb, "late"), ((peers, 3, 4, COL), None)],
        ghost_scratch + [vm(*plan.ff), vm(*plan.small)],
    )
    received2 = exchange(packets)

    def upward_second(levels_s, table_s, children_s, parents_s, guide_r, recv, back_r, up, cot_fb,
                      packets, cc):
        plan.upward(recv, 48, cc, children_s, parents_s, plan.slab_at(guide_r), slab_put(up.ref), back_r)
        up.send()
        corrected_cot_of(plan.slab_at(up.ref), levels_s, cot_fb.ref)
        cot_fb.send()
        plan.pack_quarters(cot_fb.ref, table_s, packets.ref, 0)
        packets.send()

    up2, corrcot2, quarters2 = run(
        upward_second,
        "upward_second",
        [levels, table, children, parents],
        [guide1, received1, half_back],
        [(plan.slab, "late"), (plan.fb, "late"), ((peers, 3, 4, COL), "late")],
        [vm((S + 1) * 32, COL)],
    )

    def first_update(levels_s, table_s, children_s, partial, b_fb, recv, quarters, half_r, updated,
                     packets, corr, cb):
        plan.corrected(b_fb, recv, 0, table_s, corr)
        finished(partial, corr, levels_s, slab_put(updated))
        plan.average_blocks(plan.slab_at(updated), cb, half_r)
        plan.pack_children(cb, children_s, packets, 0)
        carry_packets(quarters.get(), packets, 16)

    updated1, packets = run(
        first_update,
        "first_update",
        [levels, table, children],
        [partial1, fluxes1, received2, Late(quarters2), half],
        [(plan.slab, None), ((peers, 7, 4, COL), None)],
        [fb_scratch, vm(*plan.coarse)],
    )
    received3 = exchange(packets)

    def middle_pack(send_s, parents_s, updated, recv, volume, layers, packets, fb):
        volume[...] = updated[...]

        def store(s, x, q, value):
            volume[q, plan.slab_rows(s, x), :] = value

        plan.place_octants(recv, 0, parents_s, store)
        layers_of(plan.slab_at(volume), fb, layers.ref)
        layers.send()
        plan.pack_faces(fb, send_s, packets)

    volume2, layers2, packets = run(
        middle_pack,
        "middle_pack",
        [send, parents],
        [updated1, received3],
        [(plan.slab, None), (plan.ff, "late"), ((peers, 48, COL), "late")],
        [fb_scratch],
    )
    received4 = exchange(packets)

    def flux_cot_second(send_s, table_s, cot_fb, recv, back_r, flux_cot, kinds, *sums):
        flux_cot_of(recv, 16, cot_fb.get(), table_s, send_s, sums, kinds, flux_cot.ref, back_r)
        flux_cot.send()

    (fluxcot2,) = run(
        flux_cot_second,
        "flux_cot_second",
        [send, table],
        [Late(corrcot2), received3, half_back],
        [(plan.ff, "late")],
        [kind_scratch] + quarter_sums,
    )

    def interior_both(levels_s, volume, cot, partial, through, done):
        plan.interior(
            dyn_get(volume), levels_s, dyn_put(partial.ref), dyn_get(cot.get()), dyn_put(through.ref)
        )
        partial.send()
        through.send()
        done[...] = jnp.zeros(done.shape, f32)

    partial2, through2, done2 = run(
        interior_both, "interior_both", [levels], [volume2, Late(up2)],
        [(plan.slab, "late"), (plan.slab, "late"), ((8, COL), None)], [],
    )

    def second_pull(levels_s, table_s, layers, after, recv, flux_cot, half_r, back_r, gb, layer_cot,
                    packets, planes, near, kinds, gcot, *parts):
        del after
        plan.ghosts(recv, table_s, planes, near, kinds, gb.ref, half_r, back_r)
        gb.send()
        layer = plan.ff_at(layers)
        boundary_pull(
            plan, layer, ghost_reader(gb.ref, layer, levels_s), plan.ff_at(flux_cot.get()),
            cot_emitter(layer_cot.ref, gcot),
        )
        layer_cot.send()
        plan.pack_ghost_cot(gcot, table_s, planes, near, packets, parts, half_r, back_r)

    ghosts2, layercot2, packets = run(
        second_pull,
        "second_pull",
        [levels, table],
        [layers2, done2, received4, Late(fluxcot2), half, half_back],
        [(plan.fb, "late"), (plan.ff, "late"), ((peers, 48, COL), "late")],
        ghost_scratch + [fb_scratch] + cot_halves,
    )
    received5 = exchange(packets)

    def second_flux(levels_s, send_s, layers, gb, half_r, b_fb, packets, ff, rb):
        layer = plan.ff_at(layers.get())
        boundary_fluxes(plan, layer, ghost_reader(gb.get(), layer, levels_s), flux_emitter(b_fb.ref, ff))
        b_fb.send()
        plan.pack_averages(plan.ff_at(ff), rb, send_s, packets.ref, 0, half_r)
        packets.send()

    fluxes2, averages2 = run(
        second_flux,
        "second_flux",
        [levels, send],
        [Late(layers2), Late(ghosts2), half],
        [(plan.fb, "late"), ((peers, 3, 4, COL), "late")],
        [vm(*plan.ff), vm(*plan.small)],
    )

    def middle_cot(send_s, parents_s, through, layer_cot, recv, averages, inner, packets, total, *sums):
        plan.take_faces(recv, send_s, sums)
        carry_packets(averages.get(), packets, 16)
        add_layers(through.get(), layer_cot.get(), total, sums, slab_put(inner))
        plan.pack_octants(
            lambda s, x, q: inner[q, plan.slab_rows(s, x), :], parents_s, packets, 0
        )

    inner_cot, packets = run(
        middle_cot,
        "middle_cot",
        [send, parents],
        [Late(through2), Late(layercot2), received5, Late(averages2)],
        [(plan.slab, None), ((peers, 7, 4, COL), None)],
        [vm(*plan.ff)] + face_sums,
    )
    received6 = exchange(packets)

    def upward_first(levels_s, table_s, children_s, parents_s, inner, recv, back_r, up, cot_fb,
                     packets, cc):
        plan.upward(
            recv, 0, cc, children_s, parents_s, plan.slab_at(inner), slab_put(up.ref), back_r
        )
        up.send()
        corrected_cot_of(plan.slab_at(up.ref), levels_s, cot_fb.ref)
        cot_fb.send()
        plan.pack_quarters(cot_fb.ref, table_s, packets, 0)

    up1, corrcot1, packets = run(
        upward_first,
        "upward_first",
        [levels, table, children, parents],
        [inner_cot, received6, half_back],
        [(plan.slab, "late"), (plan.fb, "late"), ((peers, 3, 4, COL), None)],
        [vm((S + 1) * 32, COL)],
    )
    received7 = exchange(packets)

    def second_update(levels_s, table_s, partial, b_fb, recv, half_r, final, cb, corr, updated, n0,
                      n1, sems):
        plan.corrected(b_fb.get(), recv, 16, table_s, corr)
        planes = [n0, n1]
        put_slab = slab_put(updated)

        def put(q, x, c, value):
            put_slab(q, x, c, value)
            planes[q][pl.ds(c * E + x, S, stride=4 * E), :] = value

        finished(partial.get(), corr, levels_s, put)
        copies = native_copies(planes, final, sems, False)
        for copy in copies:
            copy.start()
        plan.average_blocks(plan.slab_at(updated), cb, half_r)
        for copy in copies:
            copy.wait()

    final_open, coarse2 = run(
        second_update,
        "second_update",
        [levels, table],
        [Late(partial2), Late(fluxes2), received6, half],
        [(plan.native, "raw"), (plan.coarse, None)],
        [fb_scratch, vm(*plan.slab)] + native_planes + [pair_of_sems],
    )

    def interior_back(levels_s, volume, cot, through):
        plan.interior(
            dyn_get(volume.get()), levels_s, None, dyn_get(cot.get()), dyn_put(through.ref)
        )
        through.send()

    (through1,) = run(
        interior_back, "interior_back", [levels], [Late(volume1), Late(up1)],
        [(plan.slab, "late")], [],
    )

    def first_pull(levels_s, send_s, table_s, children_s, layers, gb, cot_fb, recv, coarse, half_r,
                   back_r, layer_cot, packets, planes, near, kinds, flux_cot, gcot, *late):
        parts, sums = late[:2], late[2:]
        plan.pack_children(coarse, children_s, packets.ref, 48)
        packets.send(48, 16)
        flux_cot_of(recv, 0, cot_fb, table_s, send_s, sums, kinds, flux_cot, back_r)
        layer = plan.ff_at(layers)
        boundary_pull(
            plan, layer, ghost_reader(gb, layer, levels_s), plan.ff_at(flux_cot),
            cot_emitter(layer_cot.ref, gcot),
        )
        layer_cot.send()
        plan.pack_ghost_cot(gcot, table_s, planes, near, packets, parts, half_r, back_r)

    layercot1, packets = run(
        first_pull,
        "first_pull",
        [levels, send, table, children],
        [layers1, ghosts1, corrcot1, received7, coarse2, half, half_back],
        [(plan.ff, "late"), ((peers, 64, COL), "late")],
        ghost_scratch + [vm(*plan.ff), fb_scratch] + cot_halves + quarter_sums,
    )
    received8 = exchange(packets)

    def last_cot(send_s, parents_s, through, layer_cot, recv, open_r, gradient, final, total, n0, n1,
                 p0, p1, sems, slot_sems, *sums):
        del open_r
        placed = [p0, p1]

        def store(s, x, q, value):
            placed[q][plan.native_rows(s, x), :] = value

        plan.place_octants(recv, 48, parents_s, store)

        def each_covered(act):
            for s in range(S):

                def one(s=s):
                    rows = (s * 4 * E, 4 * E)
                    for copy in native_copies(placed, final, slot_sems.at[s], False, rows):
                        act(copy)

                pl.when(parents_s[s, 0] >= 0)(one)

        each_covered(lambda copy: copy.start())
        plan.take_faces(recv, send_s, sums)
        planes = [n0, n1]

        def put(q, x, c, value):
            planes[q][pl.ds(c * E + x, S, stride=4 * E), :] = value

        copies = native_copies(planes, gradient, sems, False)
        add_layers(
            through.get(), layer_cot.get(), total, sums, put, lambda q: copies[q].start()
        )
        for copy in copies:
            copy.wait()
        each_covered(lambda copy: copy.wait())

    gradient, final_fields = run(
        last_cot,
        "last_cot",
        [send, parents],
        [Late(through1), Late(layercot1), received8, Late(final_open, raw=True)],
        [(plan.native, "raw"), (plan.native, "raw")],
        [vm(*plan.ff)] + native_planes + native_planes
        + [pair_of_sems, pltpu.SemaphoreType.DMA((S, 2))] + face_sums,
        aliases={5: 1},
    )
    return (final_fields.reshape(fields.shape), gradient.reshape(fields.shape))


def solution(mesh):
    placed = (
        P("blk", None, None, None),
        P("blk", None, None, None),
        P("blk"),
        P("blk", None, None),
        P("blk", None, None),
        P("blk", None, None),
        P("blk", None),
        P("blk", None),
    )
    return jax.shard_map(
        on_device,
        mesh=mesh,
        in_specs=placed,
        out_specs=(P("blk", None, None, None), P("blk", None, None, None)),
        check_vma=False,
    )
```
